8 devices in a mesh: dp: 1 (over z), tp: 8 (over y, x, core).
Axes of the slice: x: 2, y: 2, z: 1, core: 2. Of those that a mesh axis runs over, the one named last changes fastest.
Arguments:
- x_in: bfloat16 [8, 64, 4096], P('dp', 'tp')
- seg_pos: int32 [8, 64], P('dp')
- conv_state: bfloat16 [2, 8, 3, 4096], P(None, 'dp', None, 'tp')
- lru_state: float32 [2, 8, 4096], P(None, 'dp', 'tp')
- k_cache: bfloat16 [8, 2048, 256], P('dp')
- v_cache: bfloat16 [8, 2048, 256], P('dp')
- slot_pos: int32 [8, 2048], P('dp')
- norm_scale: bfloat16 [6, 4096], replicated
- w_x: bfloat16 [2, 4096, 4096], P(None, None, 'tp')
- b_x: bfloat16 [2, 4096], P(None, 'tp')
- w_y: bfloat16 [2, 4096, 4096], P(None, None, 'tp')
- b_y: bfloat16 [2, 4096], P(None, 'tp')
- conv_w: bfloat16 [2, 4, 4096], P(None, None, 'tp')
- conv_b: bfloat16 [2, 4096], P(None, 'tp')
- w_a: bfloat16 [2, 16, 256, 256], P(None, 'tp')
- b_a: bfloat16 [2, 4096], P(None, 'tp')
- w_i: bfloat16 [2, 16, 256, 256], P(None, 'tp')
- b_i: bfloat16 [2, 4096], P(None, 'tp')
- a_param: float32 [2, 4096], P(None, 'tp')
- w_out: bfloat16 [2, 4096, 4096], P(None, 'tp')
- b_out: bfloat16 [2, 4096], replicated
- w_q: bfloat16 [4096, 4096], P(None, 'tp')
- w_k: bfloat16 [4096, 256], replicated
- w_v: bfloat16 [4096, 256], replicated
- w_o: bfloat16 [4096, 4096], P('tp')
- b_o: bfloat16 [4096], replicated
- w_1: bfloat16 [3, 4096, 12288], P(None, None, 'tp')
- b_1: bfloat16 [3, 12288], P(None, 'tp')
- w_2: bfloat16 [3, 4096, 12288], P(None, None, 'tp')
- b_2: bfloat16 [3, 12288], P(None, 'tp')
- w_d: bfloat16 [3, 12288, 4096], P(None, 'tp')
- b_d: bfloat16 [3, 4096], replicated
Outputs:
- output 1: bfloat16 [8, 64, 4096], P('dp', 'tp')
- output 2: bfloat16 [2, 8, 3, 4096], P(None, 'dp', None, 'tp')
- output 3: float32 [2, 8, 4096], P(None, 'dp', 'tp')
- output 4: bfloat16 [8, 2048, 256], P('dp')
- output 5: bfloat16 [8, 2048, 256], P('dp')
- output 6: int32 [8, 2048], P('dp')
All inputs are finite; a program needn't handle non-finite values.
Results may differ from the reference program's by a relative error of at most 0.02.
Values are sent between devices in bfloat16 or wider.
A program may use at most 1 GiB of HBM per device.

```python
import jax
import jax.numpy as jnp
from jax import lax

BATCH = 8
TOKENS = 64
D = 4096
L = 4096
HEADS = 16
FF = 12288
WINDOW = 2048
HEAD_DIM = 256
ROPE_DIM = 128
CONV_WIDTH = 4
GATE_BLOCK = L // HEADS


def normal_draw(key_in, shape_in, scale_in):
    return jax.random.normal(key_in, shape_in, jnp.float32) * scale_in


def draw_positions(pos_key):
    key_reset, key_lap, key_offset = jax.random.split(pos_key, 3)
    reset_at = jnp.minimum(jax.random.randint(key_reset, (BATCH,), TOKENS // 2, 2 * TOKENS), TOKENS)
    lap_count = jax.random.randint(key_lap, (BATCH,), 0, 3)
    offset_in = jax.random.randint(key_offset, (BATCH,), 0, WINDOW - TOKENS + 1)
    start_pos = lap_count * WINDOW + TOKENS - reset_at + offset_in
    token_idx = jnp.arange(TOKENS)[None, :]
    seg_pos = jnp.where(token_idx < reset_at[:, None], start_pos[:, None] + token_idx, token_idx - reset_at[:, None])
    slot_idx = jnp.arange(WINDOW)[None, :]
    last_pos = start_pos[:, None] - 1 - jnp.mod(start_pos[:, None] - 1 - slot_idx, WINDOW)
    slot_pos = jnp.where(last_pos >= 0, last_pos, -1)
    return seg_pos.astype(jnp.int32), slot_pos.astype(jnp.int32)


def setup_inputs(seed: int = 0, part: int = 0) -> dict:
    base_key = jax.random.key(seed)
    root_keys = jax.random.split(base_key, 2)
    own_keys = jax.random.split(jax.random.fold_in(root_keys[0], part), 8)
    weight_keys = jax.random.split(root_keys[1], 32)
    seg_pos, slot_pos = draw_positions(own_keys[0])
    seq_mean = normal_draw(own_keys[6], (BATCH, 1, HEAD_DIM), 1.0)
    q_width = HEADS * HEAD_DIM
    return {
        'x_in': normal_draw(own_keys[1], (BATCH, TOKENS, D), 1.0).astype(jnp.bfloat16),
        'seg_pos': seg_pos,
        'conv_state': normal_draw(own_keys[2], (2, BATCH, CONV_WIDTH - 1, L), 2.0).astype(jnp.bfloat16),
        'lru_state': normal_draw(own_keys[3], (2, BATCH, L), 1.0),
        'k_cache': normal_draw(own_keys[4], (BATCH, WINDOW, HEAD_DIM), 2.0).astype(jnp.bfloat16),
        'v_cache': (normal_draw(own_keys[5], (BATCH, WINDOW, HEAD_DIM), 1.0) + seq_mean).astype(jnp.bfloat16),
        'slot_pos': slot_pos,
        'norm_scale': normal_draw(weight_keys[0], (6, D), 0.3).astype(jnp.bfloat16),
        'w_x': normal_draw(weight_keys[1], (2, D, L), D ** -0.5).astype(jnp.bfloat16),
        'b_x': normal_draw(weight_keys[2], (2, L), 0.5).astype(jnp.bfloat16),
        'w_y': normal_draw(weight_keys[3], (2, D, L), D ** -0.5).astype(jnp.bfloat16),
        'b_y': normal_draw(weight_keys[4], (2, L), 0.5).astype(jnp.bfloat16),
        'conv_w': normal_draw(weight_keys[5], (2, CONV_WIDTH, L), 0.5).astype(jnp.bfloat16),
        'conv_b': normal_draw(weight_keys[6], (2, L), 0.3).astype(jnp.bfloat16),
        'w_a': normal_draw(weight_keys[7], (2, HEADS, GATE_BLOCK, GATE_BLOCK), GATE_BLOCK ** -0.5).astype(jnp.bfloat16),
        'b_a': normal_draw(weight_keys[8], (2, L), 1.0).astype(jnp.bfloat16),
        'w_i': normal_draw(weight_keys[9], (2, HEADS, GATE_BLOCK, GATE_BLOCK), GATE_BLOCK ** -0.5).astype(jnp.bfloat16),
        'b_i': normal_draw(weight_keys[10], (2, L), 0.5).astype(jnp.bfloat16),
        'a_param': jnp.log(jnp.expm1(jax.random.uniform(weight_keys[11], (2, L), jnp.float32, 1e-4, 1e-3))),
        'w_out': normal_draw(weight_keys[12], (2, L, D), L ** -0.5).astype(jnp.bfloat16),
        'b_out': normal_draw(weight_keys[13], (2, D), 0.3).astype(jnp.bfloat16),
        'w_q': normal_draw(weight_keys[14], (D, q_width), D ** -0.5).astype(jnp.bfloat16),
        'w_k': normal_draw(weight_keys[15], (D, HEAD_DIM), D ** -0.5).astype(jnp.bfloat16),
        'w_v': normal_draw(weight_keys[16], (D, HEAD_DIM), D ** -0.5).astype(jnp.bfloat16),
        'w_o': normal_draw(weight_keys[17], (q_width, D), q_width ** -0.5).astype(jnp.bfloat16),
        'b_o': normal_draw(weight_keys[18], (D,), 0.3).astype(jnp.bfloat16),
        'w_1': normal_draw(weight_keys[19], (3, D, FF), D ** -0.5).astype(jnp.bfloat16),
        'b_1': normal_draw(weight_keys[20], (3, FF), 0.5).astype(jnp.bfloat16),
        'w_2': normal_draw(weight_keys[21], (3, D, FF), D ** -0.5).astype(jnp.bfloat16),
        'b_2': normal_draw(weight_keys[22], (3, FF), 0.5).astype(jnp.bfloat16),
        'w_d': normal_draw(weight_keys[23], (3, FF, D), FF ** -0.5).astype(jnp.bfloat16),
        'b_d': normal_draw(weight_keys[24], (3, D), 0.3).astype(jnp.bfloat16),
    }


def rms_norm(hidden, norm_gain):
    hidden_f32 = hidden.astype(jnp.float32)
    inv_rms = lax.rsqrt(jnp.mean(hidden_f32 * hidden_f32, axis=-1, keepdims=True) + 1e-6)
    return (hidden_f32 * inv_rms * (1.0 + norm_gain.astype(jnp.float32))).astype(jnp.bfloat16)


def dense_proj(act_in, weight):
    flat_acts = act_in.reshape(-1, act_in.shape[-1])
    product = jnp.dot(flat_acts, weight, preferred_element_type=jnp.float32)
    return product.reshape(act_in.shape[:-1] + (weight.shape[-1],))


def residual_add(hidden, update, bias_row):
    return (hidden.astype(jnp.float32) + update.astype(jnp.float32) + bias_row.astype(jnp.float32)).astype(jnp.bfloat16)


def apply_rope(proj_f32, pos_exp):
    half_dim = ROPE_DIM // 2
    timescale = 10000.0 ** (2.0 * jnp.arange(half_dim).astype(jnp.float32) / ROPE_DIM)
    angle_rad = pos_exp.astype(jnp.float32) / timescale
    sin_a = jnp.sin(angle_rad)
    cos_a = jnp.cos(angle_rad)
    first_half = proj_f32[..., :half_dim]
    second_half = proj_f32[..., half_dim:ROPE_DIM]
    return jnp.concatenate([first_half * cos_a - second_half * sin_a, second_half * cos_a + first_half * sin_a, proj_f32[..., ROPE_DIM:]], axis=-1).astype(jnp.bfloat16)


def recurrent_block(normed, seg_pos, conv_prev, state_prev, w_x, b_x, w_y, b_y, conv_w, conv_b, w_a, b_a, w_i, b_i, a_param, w_out):
    gate_y = jax.nn.gelu(dense_proj(normed, w_y) + b_y.astype(jnp.float32), approximate=True).astype(jnp.bfloat16)
    branch_x = (dense_proj(normed, w_x) + b_x.astype(jnp.float32)).astype(jnp.bfloat16)
    padded = jnp.concatenate([conv_prev, branch_x], axis=1).astype(jnp.float32)
    conv_f32 = conv_b.astype(jnp.float32) + sum(padded[:, tap_idx:tap_idx + TOKENS] * conv_w[tap_idx].astype(jnp.float32) for tap_idx in range(CONV_WIDTH))
    conv_bf = conv_f32.astype(jnp.bfloat16)
    blocks = conv_bf.astype(jnp.float32).reshape(BATCH, TOKENS, HEADS, GATE_BLOCK)
    gate_r = jax.nn.sigmoid(jnp.einsum('bchi,hij->bchj', blocks, w_a.astype(jnp.float32)).reshape(BATCH, TOKENS, L) + b_a.astype(jnp.float32))
    gate_i = jax.nn.sigmoid(jnp.einsum('bchi,hij->bchj', blocks, w_i.astype(jnp.float32)).reshape(BATCH, TOKENS, L) + b_i.astype(jnp.float32))
    decay_a = jnp.exp(-8.0 * gate_r * jax.nn.softplus(a_param))
    is_reset = (seg_pos == 0)[:, :, None]
    multiplier = jnp.where(is_reset, 1.0, jnp.sqrt(1.0 - decay_a * decay_a))
    decay_a = jnp.where(is_reset, 0.0, decay_a)
    drive_in = conv_bf.astype(jnp.float32) * gate_i * multiplier

    def lru_step(h_carry, step_in):
        new_h = step_in[0] * h_carry + step_in[1]
        return new_h, new_h

    last_h, hidden_seq = lax.scan(lru_step, state_prev, (jnp.swapaxes(decay_a, 0, 1), jnp.swapaxes(drive_in, 0, 1)))
    hidden_seq = jnp.swapaxes(hidden_seq, 0, 1)
    mixed_hy = (hidden_seq * gate_y.astype(jnp.float32)).astype(jnp.bfloat16)
    return dense_proj(mixed_hy, w_out), branch_x[:, TOKENS - (CONV_WIDTH - 1):], last_h


def attention_block(normed, seg_pos, k_cache, v_cache, slot_pos, w_q, w_k, w_v, w_o):
    query_rot = apply_rope(dense_proj(normed, w_q).reshape(BATCH, TOKENS, HEADS, HEAD_DIM), seg_pos[:, :, None, None])
    key_new = apply_rope(dense_proj(normed, w_k), seg_pos[:, :, None])
    value_new = dense_proj(normed, w_v).astype(jnp.bfloat16)

    def one_sequence(seq_in):
        q_seq, k_seq, v_seq, k_old, v_old, slot_seq, pos_seq = seq_in
        doc_id = jnp.cumsum((pos_seq == 0).astype(jnp.int32))
        diff_old = pos_seq[:, None] - slot_seq[None, :]
        mask_old = (slot_seq[None, :] >= 0) & (diff_old >= 0) & (diff_old < WINDOW) & (doc_id[:, None] == 0)
        diff_new = pos_seq[:, None] - pos_seq[None, :]
        mask_new = (diff_new >= 0) & (diff_new < WINDOW) & (doc_id[:, None] == doc_id[None, :])

        def one_head(q_head):
            score_old = jnp.where(mask_old, jnp.dot(q_head, k_old.T, preferred_element_type=jnp.float32) / 16.0, -1e30)
            score_new = jnp.where(mask_new, jnp.dot(q_head, k_seq.T, preferred_element_type=jnp.float32) / 16.0, -1e30)
            row_max = jnp.maximum(score_old.max(axis=-1), score_new.max(axis=-1))[:, None]
            exp_old = jnp.exp(score_old - row_max)
            exp_new = jnp.exp(score_new - row_max)
            denom_sum = exp_old.sum(axis=-1, keepdims=True) + exp_new.sum(axis=-1, keepdims=True)
            prob_old = (exp_old / denom_sum).astype(jnp.bfloat16)
            prob_new = (exp_new / denom_sum).astype(jnp.bfloat16)
            head_out = jnp.dot(prob_old, v_old, preferred_element_type=jnp.float32) + jnp.dot(prob_new, v_seq, preferred_element_type=jnp.float32)
            return head_out.astype(jnp.bfloat16)

        return lax.map(one_head, jnp.swapaxes(q_seq, 0, 1))

    attn_out = lax.map(one_sequence, (query_rot, key_new, value_new, k_cache, v_cache, slot_pos, seg_pos))
    attn_out = jnp.swapaxes(attn_out, 1, 2).reshape(BATCH, TOKENS, HEADS * HEAD_DIM)
    attn_proj = dense_proj(attn_out, w_o)
    batch_idx = jnp.arange(BATCH)[:, None]
    slot_new = jnp.mod(seg_pos, WINDOW)
    k_out = k_cache.at[batch_idx, slot_new].set(key_new)
    v_out = v_cache.at[batch_idx, slot_new].set(value_new)
    slot_out = slot_pos.at[batch_idx, slot_new].set(seg_pos)
    return attn_proj, k_out, v_out, slot_out


def mlp_block(normed, w_1, b_1, w_2, b_2, w_d):
    gate_val = jax.nn.gelu(dense_proj(normed, w_1) + b_1.astype(jnp.float32), approximate=True)
    up_val = dense_proj(normed, w_2) + b_2.astype(jnp.float32)
    return dense_proj((gate_val * up_val).astype(jnp.bfloat16), w_d)


def reference(x_in, seg_pos, conv_state, lru_state, k_cache, v_cache, slot_pos, norm_scale, w_x, b_x, w_y, b_y, conv_w, conv_b, w_a, b_a, w_i, b_i, a_param, w_out, b_out, w_q, w_k, w_v, w_o, b_o, w_1, b_1, w_2, b_2, w_d, b_d):
    hidden = x_in
    conv_list = []
    lru_list = []
    for layer_idx in range(2):
        rec_out, conv_new, lru_new = recurrent_block(rms_norm(hidden, norm_scale[2 * layer_idx]), seg_pos, conv_state[layer_idx], lru_state[layer_idx], w_x[layer_idx], b_x[layer_idx], w_y[layer_idx], b_y[layer_idx], conv_w[layer_idx], conv_b[layer_idx], w_a[layer_idx], b_a[layer_idx], w_i[layer_idx], b_i[layer_idx], a_param[layer_idx], w_out[layer_idx])
        hidden = residual_add(hidden, rec_out, b_out[layer_idx])
        mlp_out = mlp_block(rms_norm(hidden, norm_scale[2 * layer_idx + 1]), w_1[layer_idx], b_1[layer_idx], w_2[layer_idx], b_2[layer_idx], w_d[layer_idx])
        hidden = residual_add(hidden, mlp_out, b_d[layer_idx])
        conv_list.append(conv_new)
        lru_list.append(lru_new)
    attn_proj, k_out, v_out, slot_out = attention_block(rms_norm(hidden, norm_scale[4]), seg_pos, k_cache, v_cache, slot_pos, w_q, w_k, w_v, w_o)
    hidden = residual_add(hidden, attn_proj, b_o)
    mlp_out = mlp_block(rms_norm(hidden, norm_scale[5]), w_1[2], b_1[2], w_2[2], b_2[2], w_d[2])
    hidden = residual_add(hidden, mlp_out, b_d[2])
    return (hidden, jnp.stack(conv_list), jnp.stack(lru_list), k_out, v_out, slot_out)
```

```python
import jax
import jax.numpy as jnp
from jax import lax
from jax.experimental import pallas as pl
from jax.experimental.pallas import tpu as pltpu
from jax.sharding import PartitionSpec as P

F32 = jnp.float32
BF16 = jnp.bfloat16
WINDOW = 2048
ROPE_DIM = 128
D = 4096
HALF_SEQ = 4
TOK = 8
SHARD = 32
ROWS = 256
COLS = 512
NBLK = D // COLS
PIECE = 16
NC = 4
NR = 4
WID = 256
HALVES = LAYERS = 2
SEQS = 8
SPAN = 96
NEG = -1e30

REC, MLP, ATT = 'rec', 'mlp', 'att'
SUBLAYERS = ((REC, 0), (MLP, 0), (REC, 1), (MLP, 1), (ATT, 0), (MLP, 2))

AG_OWN = ('x0', 'y1', 'x1', 'y0', 'so')
AG_STEPS = (
    (('x0', 'y1'), ('dy0', 'dx1', 'sx0', 'sy1')),
    (('x1', 'y0'), ('sx1', 'sy0')),
    (('dy0', 'dx1'), ('sd0', 'sd1')),
    (('so', 'sx0', 'sy1', 'sx1', 'sy0', 'sd0', 'sd1'), ()),
)
AG_STEP_OF = {name: i for i, (waits, _) in enumerate(AG_STEPS) for name in waits}
AG_ROWS = tuple(sum(SHARD if name == 'so' else PIECE for name in waits) for waits, _ in AG_STEPS)
RS_IN = ('x0', 'y1', 'x1', 'y0')
CHUNKS = 2
CBLK = NBLK // CHUNKS
RS_SEMS = 3 * CHUNKS + 1
RS_ORDER = ((0, 0), (1, 0), (0, 1), (1, 1), (2, 0), (2, 1))

UNITS = {REC: (2, 2.4, 2, 0.6), MLP: (6, 1.4, 8, 0.6), ATT: (6, 1.7, 2, 0.6)}
LINK_US, D2D_US, LINK_LATENCY, D2D_LATENCY = 2.81, 0.22, 1.9, 1.0


def link_of(name):
    if name[0] == 's':
        return 's'
    return 'x' if name in ('x0', 'x1', 'dx1', 'd0') else 'y'


def plan():
    free = dict.fromkeys('xys', 0.0)
    ends = {}
    now = 0.0

    def send(key, size):
        link = link_of(key[-1])
        rate, latency = (D2D_US, D2D_LATENCY) if link == 's' else (LINK_US, LINK_LATENCY)
        free[link] = max(now, free[link]) + size * rate
        ends[key] = free[link] + latency

    def own(h, k):
        for name in AG_OWN:
            send((h, k, 'g', name), 2 if name == 'so' else 1)

    def chain(h):
        steps = []
        for k, (kind, _) in enumerate(SUBLAYERS):
            n_col, _, n_row, _ = UNITS[kind]
            for i, (waits, sends) in enumerate(AG_STEPS):
                steps.append((('ag', i, 0, h, k), 0, [(h, k, 'g', w) for w in waits], [((h, k, 'g', w), 1) for w in sends], 0))
            for step, c in RS_ORDER:
                need = n_col + n_row * (c + 1) // CHUNKS if step == 0 else 0
                waits = ((), ('s3', 's1', 's2', 's0'), ('d0', 'd1'))[step]
                sends = (('s3', 's1', 's2', 's0'), ('d0', 'd1', 'x0', 'y1'), ('y0', 'x1'))[step]
                steps.append((('rs', step, c, h, k), need, [(h, k, c, w) for w in waits],
                              [((h, k, c, w), (2 if step == 0 else 1) / CHUNKS) for w in sends], 0.15))
            steps.append((('rs', 3, 0, h, k), 0, [(h, k, c, w) for c in range(CHUNKS) for w in RS_IN], [], 0.7))
        return steps

    waiting = [chain(0), chain(1)]
    computing = [(h, k) for k in range(len(SUBLAYERS)) for h in range(2)]
    unit, done, gathered, order = 0, {}, set(), []
    own(0, 0)
    own(1, 0)
    while waiting[0] or waiting[1]:
        heads = []
        for h in range(2):
            if waiting[h]:
                step = waiting[h][0]
                if done.get((h, step[0][-1]), 0) >= step[1]:
                    heads.append((max([ends[w] for w in step[2]], default=0.0), step[0][-1], h))
        ready = [(k, h) for t, k, h in heads if t <= now]
        if not ready and computing and computing[0] in gathered:
            h, k = computing[0]
            n_col, col_us, n_row, row_us = UNITS[SUBLAYERS[k][0]]
            now += col_us if unit < n_col else row_us
            order.append(('unit', h, k))
            unit += 1
            done[h, k] = unit
            if unit == n_col + n_row:
                computing.pop(0)
                unit = 0
            continue
        if ready:
            h = min(ready)[1]
        else:
            now, _, h = min(heads)
        name, _, _, sends, us = waiting[h].pop(0)
        k = name[-1]
        now += us
        for key, size in sends:
            send(key, size)
        if name[:2] == ('ag', 3):
            gathered.add((h, k))
        if name[:2] == ('rs', 3) and k + 1 < len(SUBLAYERS):
            own(h, k + 1)
        order.append(name)
    return order


class Ring:
    def __init__(self, depth, order, start):
        self.depth, self.start, self.at = depth, start, 0
        self.total = sum(n for _, n in order)
        self.runs = []
        g = 0
        for what, n in order:
            self.runs.append((what, g, n))
            g += n

    def prime(self):
        for what, g0, n in self.runs:
            for t in range(n):
                if g0 + t < self.depth:
                    self.start(what, t, g0 + t)

    def take(self, n):
        base = self.at
        self.at += n
        return base

    def slot(self, base, i):
        return (base + i) % self.depth

    def refill(self, base, n, i):
        ahead = base + self.depth
        slot = self.slot(base, i)
        for what, g0, m in self.runs:
            lo, hi = max(g0, ahead), min(g0 + m, ahead + n)
            if lo < hi:
                if isinstance(i, int):
                    if lo - ahead <= i < hi - ahead:
                        self.start(what, ahead - g0 + i, slot)
                else:
                    @pl.when((i >= lo - ahead) & (i < hi - ahead))
                    def _():
                        self.start(what, ahead - g0 + i, slot)


def loop(n, body):
    def step(i, carry):
        body(i, None)
        return carry

    lax.fori_loop(0, n, step, 0)


def sum_blocks(body):
    return lax.fori_loop(0, NBLK, body, jnp.zeros((SHARD, COLS), F32))


def row_sum(v):
    return jnp.sum(v, axis=-1, keepdims=True)


def row_max(v):
    return jnp.max(v, axis=-1, keepdims=True)


def run_ticks(i, ticks):
    for when, fn in ticks.items():
        if isinstance(i, int):
            if i == when:
                fn()
        else:
            pl.when(i == when)(fn)


def later(ticks, n):
    return {i - n: fn for i, fn in ticks.items()}


def mega(x_ref, norm_ref, bout_ref, bo_ref, bd_ref, by_ref, bx_ref, cw_ref, cb_ref, ba_ref, bi_ref, ap_ref, b1_ref, b2_ref,
         conv_ref, lru_ref, wa_ref, wi_ref, pos_ref, slot_ref, cos_ref, sin_ref,
         w_y, w_x, w_out, w_1, w_2, w_d, w_q, w_k, w_v, w_o, k_cache, v_cache,
         xo_ref, convo_ref, lruo_ref, ko_ref, vo_ref,
         nbuf, part, sibr, town, tbuf, dgr, xyr, xres, hbuf, qbuf, obuf, kvbuf, cring, rring,
         gain, bias, rvec, mvec, conv0, convf, poscol, posrow,
         ag_s, ag_r, rs_s, rs_r, csem, rsem, kvsem):
    me = lax.axis_index('tp')
    core = lax.rem(me, 2)
    xpos = lax.rem(me // 2, 2)
    ypos = me // 4
    sib = me + 1 - 2 * core
    xn = me + 2 - 4 * xpos
    yn = me + 4 - 8 * ypos
    dg = xn + 4 - 8 * ypos

    def start_c(what, t, slot):
        kind, l = what
        cols = pl.ds(t * WID if isinstance(t, int) else pl.multiple_of(t * WID, WID), WID)
        if kind == REC:
            srcs = w_y.at[l, :, cols], w_x.at[l, :, cols]
        elif kind == MLP:
            srcs = w_1.at[l, :, cols], w_2.at[l, :, cols]
        elif kind == 'q':
            srcs = w_q.at[:, pl.ds(0, WID)], w_q.at[:, pl.ds(WID, WID)]
        else:
            srcs = w_k, w_v
        for e, src in enumerate(srcs):
            pltpu.make_async_copy(src, cring.at[slot, e], csem.at[slot, e]).start()

    def wait_c(slot):
        for e, src in enumerate((w_k, w_v)):
            pltpu.make_async_copy(src, cring.at[slot, e], csem.at[slot, e]).wait()

    def start_r(what, t, slot):
        kind, l = what
        if kind == MLP:
            cols = pl.ds(t * COLS if isinstance(t, int) else pl.multiple_of(t * COLS, COLS), COLS)
            for e in range(3):
                pltpu.make_async_copy(w_d.at[l, pl.ds(e * 512, 512), cols], rring.at[slot, e], rsem.at[slot, e]).start()
        else:
            for e in range(4):
                c0 = t * 4 * COLS + e * COLS
                cols = pl.ds(c0 if isinstance(t, int) else pl.multiple_of(c0, COLS), COLS)
                src = w_out.at[l, :, cols] if kind == REC else w_o.at[:, cols]
                pltpu.make_async_copy(src, rring.at[slot, e], rsem.at[slot, e]).start()

    def wait_r(slot, n):
        for e in range(n):
            pltpu.make_async_copy(w_o.at[:, pl.ds(0, COLS)], rring.at[slot, e], rsem.at[slot, e]).wait()

    c_order, r_order = [], []
    for kind, l in SUBLAYERS:
        for _ in range(2):
            if kind == REC:
                c_order.append(((REC, l), 2))
                r_order.append(((REC, l), 2))
            elif kind == MLP:
                c_order.append(((MLP, l), 6))
                r_order.append(((MLP, l), 8))
            else:
                c_order += [(('q', 0), 1), (('kv', 0), 1)]
                r_order.append(((ATT, 0), 2))
    cw = Ring(NC, c_order, start_c)
    rw = Ring(NR, r_order, start_r)

    def kv_copies(seq, slot):
        return (pltpu.make_async_copy(k_cache.at[seq], kvbuf.at[slot, 0], kvsem.at[slot, 0]),
                pltpu.make_async_copy(v_cache.at[seq], kvbuf.at[slot, 1], kvsem.at[slot, 1]))

    def await_bytes(ref, sem):
        pltpu.make_async_copy(ref, ref, sem).wait()

    def rows_of(dev, p=None):
        if p is None:
            return pl.ds(pl.multiple_of(SHARD * dev, SHARD), SHARD)
        return pl.ds(pl.multiple_of(SHARD * dev + PIECE * p, PIECE), PIECE)

    def ag(h, name):
        p = None if name == 'so' else int(name[-1])
        origin = {'so': me, 'x': me, 'y': me, 'dy': xn, 'dx': yn, 'sx': xn, 'sy': yn, 'sd': dg}[name if name == 'so' else name[:-1]]
        target = sib if name[0] == 's' else xn if name in ('x0', 'x1', 'dx1') else yn
        ref = nbuf.at[h, rows_of(origin, p), :]
        return pltpu.make_async_remote_copy(src_ref=ref, dst_ref=ref, send_sem=ag_s.at[h], recv_sem=ag_r.at[h, AG_STEP_OF[name]],
                                            device_id={'tp': target}, device_id_type=pl.DeviceIdType.MESH)

    def ag0(h):
        for name in AG_OWN:
            ag(h, name).start()

    def ag_step(h, i):
        waits, sends = AG_STEPS[i]
        await_bytes(nbuf.at[h, pl.ds(0, AG_ROWS[i]), :], ag_r.at[h, i])
        for name in sends:
            ag(h, name).start()
        if i == 3:
            await_bytes(nbuf.at[h, pl.ds(0, sum(AG_ROWS)), :], ag_s.at[h])

    chip_rows = (me, xn, yn, dg)
    other_rows = (sib, xn + 1 - 2 * core, yn + 1 - 2 * core, dg + 1 - 2 * core)

    def rs_sem(name, c):
        if name in RS_IN:
            return RS_SEMS - 1
        return c * 3 + (0 if name == 's3' else 1 if name[0] == 's' else 2)

    def rs(h, name, c):
        p = int(name[1])
        cb = pl.ds(c * CBLK, CBLK)
        if name[0] == 's':
            src, dst, target = part.at[h, cb, rows_of(other_rows[p]), :], sibr.at[h, p, cb], sib
        elif name[0] == 'd':
            src, dst, target = tbuf.at[h, 2, p, cb], dgr.at[h, p, cb], (xn if p == 0 else yn)
        elif name[0] == 'x':
            src, dst, target = tbuf.at[h, 0, p, cb], xyr.at[h, 0, p, cb], xn
        else:
            src, dst, target = tbuf.at[h, 1, p, cb], xyr.at[h, 1, p, cb], yn
        return pltpu.make_async_remote_copy(src_ref=src, dst_ref=dst, send_sem=rs_s.at[h], recv_sem=rs_r.at[h, rs_sem(name, c)],
                                            device_id={'tp': target}, device_id_type=pl.DeviceIdType.MESH)

    def rs0(h, c):
        for p in (3, 1, 2, 0):
            rs(h, 's%d' % p, c).start()

    def rs1(h, c):
        cb = pl.ds(c * CBLK, CBLK)

        def some(p):
            def body(i, _):
                j = c * CBLK + i
                v = part[h, j, rows_of(chip_rows[p]), :].astype(F32) + sibr[h, p, j].astype(F32)
                if p == 0:
                    town[h, j] = v
                else:
                    v = v.astype(BF16)
                    tbuf[h, p - 1, 0, j] = v[:PIECE]
                    tbuf[h, p - 1, 1, j] = v[PIECE:]

            loop(CBLK, body)

        await_bytes(sibr.at[h, 3, cb], rs_r.at[h, rs_sem('s3', c)])
        some(3)
        rs(h, 'd0', c).start()
        rs(h, 'd1', c).start()
        await_bytes(sibr.at[h, pl.ds(0, 3), cb], rs_r.at[h, rs_sem('s0', c)])
        some(1)
        rs(h, 'x0', c).start()
        some(2)
        rs(h, 'y1', c).start()
        some(0)

    def rs2(h, c):
        await_bytes(dgr.at[h, :, pl.ds(c * CBLK, CBLK)], rs_r.at[h, rs_sem('d0', c)])

        def body(i, _):
            j = c * CBLK + i
            for to, p in ((1, 0), (0, 1)):
                tbuf[h, to, p, j] = (tbuf[h, to, p, j].astype(F32) + dgr[h, p, j].astype(F32)).astype(BF16)

        loop(CBLK, body)
        rs(h, 'y0', c).start()
        rs(h, 'x1', c).start()

    def blk(j):
        return pl.ds(pl.multiple_of(j * COLS, COLS), COLS)

    def normalise(h, k, square_sum):
        inv = lax.rsqrt(row_sum(square_sum) * (1.0 / D) + 1e-6)

        def body(j, _):
            nbuf[h, rows_of(me), blk(j)] = (xres[h, j].astype(F32) * inv * gain[k:k + 1, blk(j)]).astype(BF16)

        loop(NBLK, body)

    def first(h):
        def body(j, acc):
            v = x_ref[h * SHARD:(h + 1) * SHARD, blk(j)]
            xres[h, j] = v
            v = v.astype(F32)
            return acc + v * v

        normalise(h, 0, sum_blocks(body))
        ag0(h)

    def rs3(h, k):
        await_bytes(xyr.at[h], rs_r.at[h, RS_SEMS - 1])
        last = k == len(SUBLAYERS) - 1

        def body(j, acc):
            got = jnp.concatenate([xyr[h, 0, p, j].astype(F32) + xyr[h, 1, p, j].astype(F32) for p in range(2)], axis=0)
            v = xres[h, j].astype(F32) + (town[h, j] + got) + bias[k:k + 1, blk(j)]
            v = v.astype(BF16)
            if last:
                xo_ref[h * SHARD:(h + 1) * SHARD, blk(j)] = v
                return acc
            xres[h, j] = v
            v = v.astype(F32)
            return acc + v * v

        square_sum = sum_blocks(body)
        await_bytes(part.at[h, :, pl.ds(0, ROWS - SHARD), :], rs_s.at[h])
        if not last:
            normalise(h, k + 1, square_sum)
            ag0(h)

    def setup():
        for k, (ref, l) in enumerate(((bout_ref, 0), (bd_ref, 0), (bout_ref, 1), (bd_ref, 1), (bo_ref, 0), (bd_ref, 2))):
            bias[k:k + 1, :] = ref[...].astype(F32)[l:l + 1]
        rows = [(by_ref[...], 1), (bx_ref[...], 1)] + [(cw_ref[:, i], 1) for i in range(4)]
        rows += [(cb_ref[...], 1), (ba_ref[...], 1), (bi_ref[...], 1), (jax.nn.softplus(ap_ref[...]), -8.0)]
        for r, (v, scale) in enumerate(rows):
            v = v.astype(F32) * scale
            for l in range(LAYERS):
                for t in range(2):
                    rvec[l, t, r:r + 1, :] = v[l:l + 1, t * WID:(t + 1) * WID]
        for r, ref in enumerate((b1_ref, b2_ref)):
            v = ref[...].astype(F32)
            for m in range(3):
                for t in range(6):
                    mvec[m, t, r:r + 1, :] = v[m:m + 1, t * WID:(t + 1) * WID]
        conv0[...] = jnp.zeros_like(conv0)
        for l in range(LAYERS):
            for i in range(3):
                v = conv_ref[l, i].astype(F32)
                for q in range(SEQS):
                    conv0[l, q, 5 + i:6 + i, :] = v[q:q + 1]
        p = pos_ref[...]
        cols = jnp.concatenate([p, p], axis=1).T
        for q in range(SEQS):
            col = cols[:, q:q + 1]
            poscol[q] = col
            posrow[q // HALF_SEQ, :, q % HALF_SEQ] = col[:64].reshape(8, TOK, 1)

    def dot(a, b):
        return jnp.dot(a, b, preferred_element_type=F32)

    def store_part(h, j, v):
        part[h, j] = v.astype(BF16)

    def out_small(h, ticks):
        base = rw.take(2)

        def body(i, _):
            slot = rw.slot(base, i)
            wait_r(slot, 4)
            for e in range(4):
                store_part(h, i * 4 + e, dot(hbuf[:, 0:512], rring[slot, e]))
            rw.refill(base, 2, i)
            run_ticks(i, ticks)

        loop(2, body)

    def comp_rec(h, l, ticks):
        base = cw.take(2)

        def body(t, _):
            slot = cw.slot(base, t)
            wait_c(slot)
            vec = rvec[l, t]
            lanes = pl.ds(pl.multiple_of(t * WID, WID), WID)

            def row(r):
                return vec[r:r + 1, :]

            n = nbuf[h]
            gate_y = jax.nn.gelu(dot(n, cring[slot, 0]) + row(0), approximate=True).astype(BF16).astype(F32)
            u = (dot(n, cring[slot, 1]) + row(1)).astype(BF16).astype(F32)
            cw.refill(base, 2, t)
            u3 = u.reshape(SHARD, TOK, WID)
            for q in range(HALF_SEQ):
                for i in range(3):
                    convf[l, i, h * HALF_SEQ + q:h * HALF_SEQ + q + 1, lanes] = u3[SHARD - HALF_SEQ + q, 5 + i:6 + i, :]
            before = jnp.concatenate([conv0[l, h * HALF_SEQ:(h + 1) * HALF_SEQ, :, lanes], u3[:SHARD - HALF_SEQ]], axis=0)
            jj = lax.broadcasted_iota(jnp.int32, (SHARD, TOK, WID), 1)
            conv = u3 * row(5)
            for back in (1, 2, 3):
                shifted = jnp.where(jj >= back, pltpu.roll(u3, back, 1), pltpu.roll(before, back, 1))
                conv = conv + shifted * row(5 - back)
            conv = (conv + row(6)).reshape(ROWS, WID).astype(BF16)
            gate_r = jax.nn.sigmoid(dot(conv, wa_ref[l, t]) + row(7))
            gate_i = jax.nn.sigmoid(dot(conv, wi_ref[l, t]) + row(8))
            decay = jnp.exp(gate_r * row(9))
            fresh = posrow[h].reshape(ROWS, 1) == 0
            mult = jnp.where(fresh, 1.0, jnp.sqrt(1.0 - decay * decay))
            decay = jnp.where(fresh, 0.0, decay)
            drive = conv.astype(F32) * gate_i * mult
            a3 = decay.reshape(SHARD, TOK, WID)
            b3 = drive.reshape(SHARD, TOK, WID)
            for back in (1, 2, 4):
                b3 = b3 + a3 * jnp.where(jj >= back, pltpu.roll(b3, back, 1), 0.0)
                a3 = a3 * jnp.where(jj >= back, pltpu.roll(a3, back, 1), 1.0)
            held = lru_ref[l, :, lanes]
            carry = jnp.concatenate([held[q:q + 1].reshape(1, 1, WID) for q in range(h * HALF_SEQ, (h + 1) * HALF_SEQ)], axis=0)
            out = []
            for d in range(8):
                here = slice(d * HALF_SEQ, (d + 1) * HALF_SEQ)
                hs = b3[here] + a3[here] * carry
                carry = hs[:, TOK - 1:TOK, :]
                out.append(hs)
            for q in range(HALF_SEQ):
                lruo_ref[l, h * HALF_SEQ + q:h * HALF_SEQ + q + 1, lanes] = carry[q]
            hs = jnp.concatenate(out, axis=0).reshape(ROWS, WID)
            hbuf[:, lanes] = (hs * gate_y).astype(BF16)
            run_ticks(t, ticks)

        loop(2, body)
        out_small(h, later(ticks, 2))

    def comp_mlp(h, m, ticks):
        base = cw.take(6)

        def body(t, _):
            slot = cw.slot(base, t)
            wait_c(slot)
            n = nbuf[h]
            gate = jax.nn.gelu(dot(n, cring[slot, 0]) + mvec[m, t, 0:1, :], approximate=True)
            up = dot(n, cring[slot, 1]) + mvec[m, t, 1:2, :]
            hbuf[:, pl.ds(pl.multiple_of(t * WID, WID), WID)] = (gate * up).astype(BF16)
            cw.refill(base, 6, t)
            run_ticks(t, ticks)

        loop(6, body)
        base_r = rw.take(8)

        def body_r(j, _):
            slot = rw.slot(base_r, j)
            wait_r(slot, 3)
            store_part(h, j, dot(hbuf[:, 0:512], rring[slot, 0]) + dot(hbuf[:, 512:1024], rring[slot, 1])
                       + dot(hbuf[:, 1024:1536], rring[slot, 2]))
            rw.refill(base_r, 8, j)
            run_ticks(j, later(ticks, 6))

        loop(8, body_r)

    def comp_att(h, l, ticks):
        for c in kv_copies(h * HALF_SEQ, 0):
            c.start()
        def row_order(ref):
            v = ref[h * HALF_SEQ:(h + 1) * HALF_SEQ].reshape(HALF_SEQ, 8, TOK, ROPE_DIM)
            return jnp.concatenate([v[q, d] for d in range(8) for q in range(HALF_SEQ)], axis=0)

        cos, sin = row_order(cos_ref), row_order(sin_ref)

        def rope(v):
            r = v[:, :ROPE_DIM]
            return jnp.concatenate([r * cos + pltpu.roll(r, ROPE_DIM // 2, 1) * sin, v[:, ROPE_DIM:]], axis=1)

        def by_seq(v):
            v = v.reshape(8, HALF_SEQ, TOK, WID)
            return [v[:, s].reshape(64, WID).astype(BF16) for s in range(HALF_SEQ)]

        n = nbuf[h]
        base = cw.take(1)
        slot = cw.slot(base, 0)
        wait_c(slot)
        for e in range(2):
            for s, v in enumerate(by_seq(rope(dot(n, cring[slot, e])))):
                qbuf[s, e * 64:(e + 1) * 64, :] = v
        cw.refill(base, 1, 0)
        run_ticks(0, ticks)
        base = cw.take(1)
        slot = cw.slot(base, 0)
        wait_c(slot)
        for s, v in enumerate(by_seq(rope(dot(n, cring[slot, 0])))):
            ko_ref[h * HALF_SEQ + s] = v
        for s, v in enumerate(by_seq(dot(n, cring[slot, 1]))):
            vo_ref[h * HALF_SEQ + s] = v
        cw.refill(base, 1, 0)
        run_ticks(0, later(ticks, 1))

        def body(s, _):
            seq = h * HALF_SEQ + s
            slot = lax.rem(s, 2)
            for c in kv_copies(seq, slot):
                c.wait()

            @pl.when(s + 1 < HALF_SEQ)
            def _():
                for c in kv_copies(seq + 1, 1 - slot):
                    c.start()

            q = qbuf[s]
            trans = (((1,), (1,)), ((), ()))
            s_old = lax.dot_general(q, kvbuf[slot, 0], trans, preferred_element_type=F32) * 0.0625
            s_new = lax.dot_general(q, ko_ref[seq], trans, preferred_element_type=F32) * 0.0625
            held = slot_ref[pl.ds(seq, 1), :]
            pos = poscol[seq]
            index = lax.rem(lax.broadcasted_iota(jnp.int32, (128, 1), 0), 64)
            last = jnp.where(pos > index, pos, -1)
            s_old = jnp.where((held >= 0) & (held <= last) & (held > pos - WINDOW), s_old, NEG)
            other = lax.broadcasted_iota(jnp.int32, (128, 64), 1)
            s_new = jnp.where((other <= index) & (other >= index - pos), s_new, NEG)
            top = jnp.maximum(row_max(s_old), row_max(s_new))
            e_old = jnp.exp(s_old - top)
            e_new = jnp.exp(s_new - top)
            inv = 1.0 / (row_sum(e_old) + row_sum(e_new))
            o = dot((e_old * inv).astype(BF16), kvbuf[slot, 1]) + dot((e_new * inv).astype(BF16), vo_ref[seq])
            o = o.reshape(2, 8, TOK, WID)
            obuf[:, s, :, 0:WID] = o[0]
            obuf[:, s, :, WID:512] = o[1]
            run_ticks(s, later(ticks, 2))

        loop(HALF_SEQ, body)
        hbuf[:, 0:512] = obuf[...].reshape(ROWS, 512).astype(BF16)
        out_small(h, later(ticks, 6))

    comp = {REC: comp_rec, MLP: comp_mlp, ATT: comp_att}

    cw.prime()
    rw.prime()
    barrier = pltpu.get_barrier_semaphore()
    for other in (sib, xn, yn):
        pl.semaphore_signal(barrier, inc=1, device_id={'tp': other}, device_id_type=pl.DeviceIdType.MESH)
    pl.semaphore_wait(barrier, 3)

    gain[...] = 1.0 + norm_ref[...].astype(F32)
    first(0)
    first(1)
    setup()

    def act(name):
        kind, i, c, h, k = name
        if kind == 'ag':
            ag_step(h, i)
        elif i == 3:
            rs3(h, k)
        else:
            (rs0, rs1, rs2)[i](h, c)

    def act_all(names):
        for name in names:
            act(name)

    after, unit = {}, None
    count = {}
    for event in plan():
        if event[0] == 'unit':
            hk = event[1:]
            unit = hk, count.get(hk, 0)
            count[hk] = unit[1] + 1
        else:
            after.setdefault(unit, []).append(event)
    act_all(after[None])
    for k, (kind, l) in enumerate(SUBLAYERS):
        for h in range(HALVES):
            last = count[h, k] - 1
            ticks = {u: (lambda names=names: act_all(names)) for (hk, u), names in
                     ((key, v) for key, v in after.items() if key) if hk == (h, k) and u < last}
            comp[kind](h, l, ticks)
            act_all(after.get(((h, k), last), ()))
    convo_ref[...] = convf[...].astype(BF16)


def update(scal_ref, new_ref, k_cache, v_cache, kn_ref, vn_ref, ko, vo, buf, in_sem, out_sem):
    pairs = [(e, q) for q in range(SEQS) for e in range(2)]

    def copy_in(e, q):
        return pltpu.make_async_copy((k_cache, v_cache)[e].at[q], buf.at[e, q], in_sem.at[e, q])

    def copy_out(e, q):
        return pltpu.make_async_copy(buf.at[e, q], (ko, vo)[e].at[q], out_sem.at[e, q])

    for e, q in pairs:
        copy_in(e, q).start()
    for e, q in pairs:
        copy_in(e, q).wait()
        for start in (pl.multiple_of(scal_ref[q], 16), 0):
            rows = pl.ds(start, SPAN)
            hit = lax.broadcasted_iota(jnp.int32, (SPAN, 64), 0) + start == new_ref[q]
            put = jnp.dot(hit.astype(BF16), (kn_ref, vn_ref)[e][q], preferred_element_type=F32)
            any_hit = row_sum(hit.astype(F32)) > 0.5
            buf[e, q, rows, :] = jnp.where(any_hit, put, buf[e, q, rows, :].astype(F32)).astype(BF16)
        copy_out(e, q).start()
    for e, q in pairs:
        copy_out(e, q).wait()


def solution(mesh):
    def device_body(x_in, seg_pos, conv_state, lru_state, k_cache, v_cache, slot_pos, norm_scale, w_x, b_x, w_y, b_y, conv_w, conv_b, w_a, b_a, w_i, b_i, a_param, w_out, b_out, w_q, w_k, w_v, w_o, b_o, w_1, b_1, w_2, b_2, w_d, b_d):
        lane = lax.broadcasted_iota(jnp.int32, (1, 1, ROPE_DIM), 2)
        half_dim = ROPE_DIM // 2
        timescale = 10000.0 ** (2.0 * (lane % half_dim).astype(F32) / ROPE_DIM)
        angle = seg_pos[:, :, None].astype(F32) / timescale
        cos = jnp.cos(angle)
        sin = jnp.where(lane < half_dim, -jnp.sin(angle), jnp.sin(angle))

        vmem = pl.BlockSpec(memory_space=pltpu.VMEM)
        hbm = pl.BlockSpec(memory_space=pl.ANY)
        sds = jax.ShapeDtypeStruct
        fresh = sds((SEQS, 64, WID), BF16)
        x_out, conv_out, lru_out, k_new, v_new = pl.pallas_call(
            mega,
            out_shape=(sds((64, D), BF16), sds((LAYERS, 3, SEQS, 512), BF16), sds((LAYERS, SEQS, 512), F32), fresh, fresh),
            in_specs=[vmem] * 22 + [hbm] * 12,
            out_specs=[vmem] * 5,
            scratch_shapes=[
                pltpu.VMEM((HALVES, ROWS, D), BF16),
                pltpu.VMEM((HALVES, NBLK, ROWS, COLS), BF16),
                pltpu.VMEM((HALVES, 4, NBLK, SHARD, COLS), BF16),
                pltpu.VMEM((HALVES, NBLK, SHARD, COLS), F32),
                pltpu.VMEM((HALVES, 3, 2, NBLK, PIECE, COLS), BF16),
                pltpu.VMEM((HALVES, 2, NBLK, PIECE, COLS), BF16),
                pltpu.VMEM((HALVES, 2, 2, NBLK, PIECE, COLS), BF16),
                pltpu.VMEM((HALVES, NBLK, SHARD, COLS), BF16),
                pltpu.VMEM((ROWS, 1536), BF16),
                pltpu.VMEM((HALF_SEQ, 128, WID), BF16),
                pltpu.VMEM((8, HALF_SEQ, TOK, 512), F32),
                pltpu.VMEM((HALVES, 2, WINDOW, WID), BF16),
                pltpu.VMEM((NC, 2, D, WID), BF16),
                pltpu.VMEM((NR, 4, 512, COLS), BF16),
                pltpu.VMEM((6, D), F32),
                pltpu.VMEM((6, D), F32),
                pltpu.VMEM((LAYERS, 2, 16, WID), F32),
                pltpu.VMEM((3, 6, 8, WID), F32),
                pltpu.VMEM((LAYERS, SEQS, TOK, 512), F32),
                pltpu.VMEM((LAYERS, 3, SEQS, 512), F32),
                pltpu.VMEM((SEQS, 128, 1), jnp.int32),
                pltpu.VMEM((HALVES, 8, HALF_SEQ, TOK, 1), jnp.int32),
                pltpu.SemaphoreType.DMA((HALVES,)),
                pltpu.SemaphoreType.DMA((HALVES, len(AG_STEPS))),
                pltpu.SemaphoreType.DMA((HALVES,)),
                pltpu.SemaphoreType.DMA((HALVES, RS_SEMS)),
                pltpu.SemaphoreType.DMA((NC, 2)),
                pltpu.SemaphoreType.DMA((NR, 4)),
                pltpu.SemaphoreType.DMA((HALVES, 2)),
            ],
            compiler_params=pltpu.CompilerParams(collective_id=0, has_side_effects=True, vmem_limit_bytes=67043328),
            name='layers',
        )(x_in.reshape(64, D), norm_scale, b_out, b_o[None], b_d, b_y, b_x, conv_w, conv_b, b_a, b_i, a_param, b_1, b_2,
          conv_state.swapaxes(1, 2), lru_state, w_a, w_i, seg_pos, slot_pos, cos, sin,
          w_y, w_x, w_out, w_1, w_2, w_d, w_q, w_k, w_v, w_o, k_cache, v_cache)

        slot_new = seg_pos & (WINDOW - 1)
        window = jnp.minimum(slot_new[:, 0] // 16 * 16, WINDOW - SPAN)
        caches = [sds(k_cache.shape, BF16)] * 2
        k_out, v_out = pl.pallas_call(
            update,
            out_shape=caches,
            in_specs=[pl.BlockSpec(memory_space=pltpu.SMEM), vmem, hbm, hbm, vmem, vmem],
            out_specs=[hbm, hbm],
            scratch_shapes=[pltpu.VMEM((2, SEQS, WINDOW, WID), BF16)] + [pltpu.SemaphoreType.DMA((2, SEQS))] * 2,
            name='caches',
        )(window, slot_new[:, None, :], k_cache, v_cache, k_new, v_new)

        first, last = seg_pos[:, :1], seg_pos[:, 63:]
        count = jnp.where(last < 63, 63 - last, 64)
        slot = lax.broadcasted_iota(jnp.int32, (1, WINDOW), 1)
        ahead = (slot - first) & (WINDOW - 1)
        slot_out = jnp.where(ahead < count, first + ahead, jnp.where(slot < 64 - count, slot, slot_pos))
        return x_out.reshape(8, 8, D), conv_out.swapaxes(1, 2), lru_out, k_out, v_out, slot_out

    col_spec = P(None, None, 'tp')
    vec_spec = P(None, 'tp')
    row_spec = vec_spec
    x_spec, seq_spec, conv_spec, lru_spec = P('dp', 'tp'), P('dp'), P(None, 'dp', None, 'tp'), P(None, 'dp', 'tp')
    arg_specs = (x_spec, seq_spec, conv_spec, lru_spec, seq_spec, seq_spec, seq_spec, P(), col_spec, vec_spec, col_spec, vec_spec, col_spec, vec_spec, row_spec, vec_spec, row_spec, vec_spec, vec_spec, row_spec, P(), vec_spec, P(), P(), P('tp'), P(), col_spec, vec_spec, col_spec, vec_spec, row_spec, P())
    result_specs = (x_spec, conv_spec, lru_spec, seq_spec, seq_spec, seq_spec)
    return jax.shard_map(device_body, mesh=mesh, in_specs=arg_specs, out_specs=result_specs, check_vma=False)
```

```python
import jax
import jax.numpy as jnp
from jax import lax
from jax.experimental import pallas as pl
from jax.experimental.pallas import tpu as pltpu
from jax.sharding import PartitionSpec as P

F32 = jnp.float32
BF16 = jnp.bfloat16
WINDOW = 2048
ROPE_DIM = 128
D = 4096
HALF_SEQ = 4
TOK = 8
SHARD = 32
ROWS = 256
COLS = 512
NBLK = D // COLS
PIECE = 16
NC = 4
NR = 4
WID = 256
HALVES = LAYERS = 2
SEQS = 8
SPAN = 96
NEG = -1e30

REC, MLP, ATT = 'rec', 'mlp', 'att'
SUBLAYERS = ((REC, 0), (MLP, 0), (REC, 1), (MLP, 1), (ATT, 0), (MLP, 2))

UNITS = {REC: 4, MLP: 10, ATT: 8}
AG_OWN = ('x0', 'y1', 'x1', 'y0', 'so')
AG_STEPS = (
    (('x0', 'y1'), ('dy0', 'dx1', 'sx0', 'sy1')),
    (('x1', 'y0'), ('sx1', 'sy0')),
    (('dy0', 'dx1'), ('sd0', 'sd1')),
    (('so', 'sx0', 'sy1', 'sx1', 'sy0', 'sd0', 'sd1'), ()),
)
AG_STEP_OF = {name: i for i, (waits, _) in enumerate(AG_STEPS) for name in waits}
AG_ROWS = tuple(sum(SHARD if name == 'so' else PIECE for name in waits) for waits, _ in AG_STEPS)
RS_IN = ('x0', 'y1', 'x1', 'y0')
CHUNKS = 2
CBLK = NBLK // CHUNKS
RS_SEMS = 3 * CHUNKS + 1
RS_ORDER = ((0, 0), (1, 0), (0, 1), (1, 1), (2, 0), (2, 1))

PLAN = (
    'aabaa.b..bab.aab.aa..babaa.bbaabba...b....b.a..aababab..',
    'a..a....ab.b.ababba...ab.aaaaabbabbb.a..ba.bbaba.b..b..b',
    '....ba.aabbaab..a..a....ab..bbbaaba.b..b...b.a.aabbaab..',
    'a..a...a.bbbbaaba..b..b....ab.a.babaab........ba..bbbbab',
    'b',
)


def plan():
    def chain(h):
        if h:
            yield 'start', 0, 0, h, 0
        for k in range(len(SUBLAYERS)):
            for i in range(len(AG_STEPS)):
                yield 'ag', i, 0, h, k
            for step, c in RS_ORDER:
                yield 'rs', step, c, h, k
            yield 'rs', 3, 0, h, k

    ahead = {'a': chain(0), 'b': chain(1)}
    return [next(ahead[c]) if c in ahead else None for c in ''.join(PLAN)]


class Ring:
    def __init__(self, depth, order, start):
        self.depth, self.start, self.at = depth, start, 0
        self.total = sum(n for _, n in order)
        self.runs = []
        g = 0
        for what, n in order:
            self.runs.append((what, g, n))
            g += n

    def prime(self):
        for what, g0, n in self.runs:
            for t in range(n):
                if g0 + t < self.depth:
                    self.start(what, t, g0 + t)

    def take(self, n):
        base = self.at
        self.at += n
        return base

    def slot(self, base, i):
        return (base + i) % self.depth

    def refill(self, base, n, i):
        ahead = base + self.depth
        slot = self.slot(base, i)
        for what, g0, m in self.runs:
            lo, hi = max(g0, ahead), min(g0 + m, ahead + n)
            if lo < hi:
                if isinstance(i, int):
                    if lo - ahead <= i < hi - ahead:
                        self.start(what, ahead - g0 + i, slot)
                else:
                    @pl.when((i >= lo - ahead) & (i < hi - ahead))
                    def _():
                        self.start(what, ahead - g0 + i, slot)


def loop(n, body):
    def step(i, carry):
        body(i, None)
        return carry

    lax.fori_loop(0, n, step, 0)


def sum_blocks(body):
    return lax.fori_loop(0, NBLK, body, jnp.zeros((SHARD, COLS), F32))


def row_sum(v):
    return jnp.sum(v, axis=-1, keepdims=True)


def row_max(v):
    return jnp.max(v, axis=-1, keepdims=True)


def run_ticks(i, ticks):
    for when, fn in ticks.items():
        if isinstance(i, int):
            if i == when:
                fn()
        else:
            pl.when(i == when)(fn)


def later(ticks, n):
    return {i - n: fn for i, fn in ticks.items()}


def mega(x_ref, norm_ref, bout_ref, bo_ref, bd_ref, by_ref, bx_ref, cw_ref, cb_ref, ba_ref, bi_ref, ap_ref, b1_ref, b2_ref,
         conv_ref, lru_ref, wa_ref, wi_ref, pos_ref, slot_ref, cos_ref, sin_ref,
         w_y, w_x, w_out, w_1, w_2, w_d, w_q, w_k, w_v, w_o, k_cache, v_cache,
         xo_ref, convo_ref, lruo_ref, ko_ref, vo_ref,
         nbuf, part, sibr, town, tbuf, dgr, xyr, xres, hbuf, qbuf, obuf, kvbuf, cring, rring,
         gain, bias, rvec, mvec, conv0, convf, poscol, posrow,
         ag_s, ag_r, rs_s, rs_r, csem, rsem, kvsem):
    me = lax.axis_index('tp')
    core = lax.rem(me, 2)
    xpos = lax.rem(me // 2, 2)
    ypos = me // 4
    sib = me + 1 - 2 * core
    xn = me + 2 - 4 * xpos
    yn = me + 4 - 8 * ypos
    dg = xn + 4 - 8 * ypos

    def start_c(what, t, slot):
        kind, l = what
        cols = pl.ds(t * WID if isinstance(t, int) else pl.multiple_of(t * WID, WID), WID)
        if kind == REC:
            srcs = w_y.at[l, :, cols], w_x.at[l, :, cols]
        elif kind == MLP:
            srcs = w_1.at[l, :, cols], w_2.at[l, :, cols]
        elif kind == 'q':
            srcs = w_q.at[:, pl.ds(0, WID)], w_q.at[:, pl.ds(WID, WID)]
        else:
            srcs = w_k, w_v
        for e, src in enumerate(srcs):
            pltpu.make_async_copy(src, cring.at[slot, e], csem.at[slot, e]).start()

    def wait_c(slot):
        for e, src in enumerate((w_k, w_v)):
            pltpu.make_async_copy(src, cring.at[slot, e], csem.at[slot, e]).wait()

    def start_r(what, t, slot):
        kind, l = what
        if kind == MLP:
            cols = pl.ds(t * COLS if isinstance(t, int) else pl.multiple_of(t * COLS, COLS), COLS)
            for e in range(3):
                pltpu.make_async_copy(w_d.at[l, pl.ds(e * 512, 512), cols], rring.at[slot, e], rsem.at[slot, e]).start()
        else:
            for e in range(4):
                c0 = t * 4 * COLS + e * COLS
                cols = pl.ds(c0 if isinstance(t, int) else pl.multiple_of(c0, COLS), COLS)
                src = w_out.at[l, :, cols] if kind == REC else w_o.at[:, cols]
                pltpu.make_async_copy(src, rring.at[slot, e], rsem.at[slot, e]).start()

    def wait_r(slot, n):
        for e in range(n):
            pltpu.make_async_copy(w_o.at[:, pl.ds(0, COLS)], rring.at[slot, e], rsem.at[slot, e]).wait()

    c_order, r_order = [], []
    for kind, l in SUBLAYERS:
        for _ in range(2):
            if kind == REC:
                c_order.append(((REC, l), 2))
                r_order.append(((REC, l), 2))
            elif kind == MLP:
                c_order.append(((MLP, l), 6))
                r_order.append(((MLP, l), 8))
            else:
                c_order += [(('q', 0), 1), (('kv', 0), 1)]
                r_order.append(((ATT, 0), 2))
    cw = Ring(NC, c_order, start_c)
    rw = Ring(NR, r_order, start_r)

    def kv_copies(seq, slot):
        return (pltpu.make_async_copy(k_cache.at[seq], kvbuf.at[slot, 0], kvsem.at[slot, 0]),
                pltpu.make_async_copy(v_cache.at[seq], kvbuf.at[slot, 1], kvsem.at[slot, 1]))

    def await_bytes(ref, sem):
        pltpu.make_async_copy(ref, ref, sem).wait()

    def rows_of(dev, p=None):
        if p is None:
            return pl.ds(pl.multiple_of(SHARD * dev, SHARD), SHARD)
        return pl.ds(pl.multiple_of(SHARD * dev + PIECE * p, PIECE), PIECE)

    def ag(h, name):
        p = None if name == 'so' else int(name[-1])
        origin = {'so': me, 'x': me, 'y': me, 'dy': xn, 'dx': yn, 'sx': xn, 'sy': yn, 'sd': dg}[name if name == 'so' else name[:-1]]
        target = sib if name[0] == 's' else xn if name in ('x0', 'x1', 'dx1') else yn
        ref = nbuf.at[h, rows_of(origin, p), :]
        return pltpu.make_async_remote_copy(src_ref=ref, dst_ref=ref, send_sem=ag_s.at[h], recv_sem=ag_r.at[h, AG_STEP_OF[name]],
                                            device_id={'tp': target}, device_id_type=pl.DeviceIdType.MESH)

    def ag0(h):
        for name in AG_OWN:
            ag(h, name).start()

    def ag_step(h, i):
        waits, sends = AG_STEPS[i]
        await_bytes(nbuf.at[h, pl.ds(0, AG_ROWS[i]), :], ag_r.at[h, i])
        for name in sends:
            ag(h, name).start()
        if i == 3:
            await_bytes(nbuf.at[h, pl.ds(0, sum(AG_ROWS)), :], ag_s.at[h])

    chip_rows = (me, xn, yn, dg)
    other_rows = (sib, xn + 1 - 2 * core, yn + 1 - 2 * core, dg + 1 - 2 * core)

    def rs_sem(name, c):
        if name in RS_IN:
            return RS_SEMS - 1
        return c * 3 + (0 if name == 's3' else 1 if name[0] == 's' else 2)

    def rs(h, name, c):
        p = int(name[1])
        cb = pl.ds(c * CBLK, CBLK)
        if name[0] == 's':
            src, dst, target = part.at[h, cb, rows_of(other_rows[p]), :], sibr.at[h, p, cb], sib
        elif name[0] == 'd':
            src, dst, target = tbuf.at[h, 2, p, cb], dgr.at[h, p, cb], (xn if p == 0 else yn)
        elif name[0] == 'x':
            src, dst, target = tbuf.at[h, 0, p, cb], xyr.at[h, 0, p, cb], xn
        else:
            src, dst, target = tbuf.at[h, 1, p, cb], xyr.at[h, 1, p, cb], yn
        return pltpu.make_async_remote_copy(src_ref=src, dst_ref=dst, send_sem=rs_s.at[h], recv_sem=rs_r.at[h, rs_sem(name, c)],
                                            device_id={'tp': target}, device_id_type=pl.DeviceIdType.MESH)

    def rs0(h, c):
        for p in (3, 1, 2, 0):
            rs(h, 's%d' % p, c).start()

    def rs1(h, c):
        cb = pl.ds(c * CBLK, CBLK)

        def some(p):
            def body(i, _):
                j = c * CBLK + i
                v = part[h, j, rows_of(chip_rows[p]), :].astype(F32) + sibr[h, p, j].astype(F32)
                if p == 0:
                    town[h, j] = v
                else:
                    v = v.astype(BF16)
                    tbuf[h, p - 1, 0, j] = v[:PIECE]
                    tbuf[h, p - 1, 1, j] = v[PIECE:]

            loop(CBLK, body)

        await_bytes(sibr.at[h, 3, cb], rs_r.at[h, rs_sem('s3', c)])
        some(3)
        rs(h, 'd0', c).start()
        rs(h, 'd1', c).start()
        await_bytes(sibr.at[h, pl.ds(0, 3), cb], rs_r.at[h, rs_sem('s0', c)])
        some(1)
        rs(h, 'x0', c).start()
        some(2)
        rs(h, 'y1', c).start()
        some(0)

    def rs2(h, c):
        await_bytes(dgr.at[h, :, pl.ds(c * CBLK, CBLK)], rs_r.at[h, rs_sem('d0', c)])

        def body(i, _):
            j = c * CBLK + i
            for to, p in ((1, 0), (0, 1)):
                tbuf[h, to, p, j] = (tbuf[h, to, p, j].astype(F32) + dgr[h, p, j].astype(F32)).astype(BF16)

        loop(CBLK, body)
        rs(h, 'y0', c).start()
        rs(h, 'x1', c).start()

    def blk(j):
        return pl.ds(pl.multiple_of(j * COLS, COLS), COLS)

    def normalise(h, k, square_sum):
        inv = lax.rsqrt(row_sum(square_sum) * (1.0 / D) + 1e-6)

        def body(j, _):
            nbuf[h, rows_of(me), blk(j)] = (xres[h, j].astype(F32) * inv * gain[k:k + 1, blk(j)]).astype(BF16)

        loop(NBLK, body)

    def first(h):
        def body(j, acc):
            v = x_ref[h * SHARD:(h + 1) * SHARD, blk(j)]
            xres[h, j] = v
            v = v.astype(F32)
            return acc + v * v

        normalise(h, 0, sum_blocks(body))
        ag0(h)

    def rs3(h, k):
        await_bytes(xyr.at[h], rs_r.at[h, RS_SEMS - 1])
        last = k == len(SUBLAYERS) - 1

        def body(j, acc):
            got = jnp.concatenate([xyr[h, 0, p, j].astype(F32) + xyr[h, 1, p, j].astype(F32) for p in range(2)], axis=0)
            v = xres[h, j].astype(F32) + (town[h, j] + got) + bias[k:k + 1, blk(j)]
            v = v.astype(BF16)
            if last:
                xo_ref[h * SHARD:(h + 1) * SHARD, blk(j)] = v
                return acc
            xres[h, j] = v
            v = v.astype(F32)
            return acc + v * v

        square_sum = sum_blocks(body)
        await_bytes(part.at[h, :, pl.ds(0, ROWS - SHARD), :], rs_s.at[h])
        if not last:
            normalise(h, k + 1, square_sum)
            ag0(h)

    def setup():
        for k, (ref, l) in enumerate(((bout_ref, 0), (bd_ref, 0), (bout_ref, 1), (bd_ref, 1), (bo_ref, 0), (bd_ref, 2))):
            bias[k:k + 1, :] = ref[...].astype(F32)[l:l + 1]
        rows = [(by_ref[...], 1), (bx_ref[...], 1)] + [(cw_ref[:, i], 1) for i in range(4)]
        rows += [(cb_ref[...], 1), (ba_ref[...], 1), (bi_ref[...], 1), (jax.nn.softplus(ap_ref[...]), -8.0)]
        for r, (v, scale) in enumerate(rows):
            v = v.astype(F32) * scale
            for l in range(LAYERS):
                for t in range(2):
                    rvec[l, t, r:r + 1, :] = v[l:l + 1, t * WID:(t + 1) * WID]
        for r, ref in enumerate((b1_ref, b2_ref)):
            v = ref[...].astype(F32)
            for m in range(3):
                for t in range(6):
                    mvec[m, t, r:r + 1, :] = v[m:m + 1, t * WID:(t + 1) * WID]
        conv0[...] = jnp.zeros_like(conv0)
        for l in range(LAYERS):
            for i in range(3):
                v = conv_ref[l, i].astype(F32)
                for q in range(SEQS):
                    conv0[l, q, 5 + i:6 + i, :] = v[q:q + 1]
        p = pos_ref[...]
        cols = jnp.concatenate([p, p], axis=1).T
        for q in range(SEQS):
            col = cols[:, q:q + 1]
            poscol[q] = col
            posrow[q // HALF_SEQ, :, q % HALF_SEQ] = col[:64].reshape(8, TOK, 1)

    def dot(a, b):
        return jnp.dot(a, b, preferred_element_type=F32)

    def store_part(h, j, v):
        part[h, j] = v.astype(BF16)

    def out_small(h, ticks):
        base = rw.take(2)

        def body(i, _):
            slot = rw.slot(base, i)
            wait_r(slot, 4)
            for e in range(4):
                store_part(h, i * 4 + e, dot(hbuf[:, 0:512], rring[slot, e]))
            rw.refill(base, 2, i)
            run_ticks(i, ticks)

        loop(2, body)

    def comp_rec(h, l, ticks):
        base = cw.take(2)

        def body(t, _):
            slot = cw.slot(base, t)
            wait_c(slot)
            vec = rvec[l, t]
            lanes = pl.ds(pl.multiple_of(t * WID, WID), WID)

            def row(r):
                return vec[r:r + 1, :]

            n = nbuf[h]
            gate_y = jax.nn.gelu(dot(n, cring[slot, 0]) + row(0), approximate=True).astype(BF16).astype(F32)
            u = (dot(n, cring[slot, 1]) + row(1)).astype(BF16).astype(F32)
            cw.refill(base, 2, t)
            u3 = u.reshape(SHARD, TOK, WID)
            for q in range(HALF_SEQ):
                for i in range(3):
                    convf[l, i, h * HALF_SEQ + q:h * HALF_SEQ + q + 1, lanes] = u3[SHARD - HALF_SEQ + q, 5 + i:6 + i, :]
            before = jnp.concatenate([conv0[l, h * HALF_SEQ:(h + 1) * HALF_SEQ, :, lanes], u3[:SHARD - HALF_SEQ]], axis=0)
            jj = lax.broadcasted_iota(jnp.int32, (SHARD, TOK, WID), 1)
            conv = u3 * row(5)
            for back in (1, 2, 3):
                shifted = jnp.where(jj >= back, pltpu.roll(u3, back, 1), pltpu.roll(before, back, 1))
                conv = conv + shifted * row(5 - back)
            conv = (conv + row(6)).reshape(ROWS, WID).astype(BF16)
            gate_r = jax.nn.sigmoid(dot(conv, wa_ref[l, t]) + row(7))
            gate_i = jax.nn.sigmoid(dot(conv, wi_ref[l, t]) + row(8))
            decay = jnp.exp(gate_r * row(9))
            fresh = posrow[h].reshape(ROWS, 1) == 0
            mult = jnp.where(fresh, 1.0, jnp.sqrt(1.0 - decay * decay))
            decay = jnp.where(fresh, 0.0, decay)
            drive = conv.astype(F32) * gate_i * mult
            a3 = decay.reshape(SHARD, TOK, WID)
            b3 = drive.reshape(SHARD, TOK, WID)
            for back in (1, 2, 4):
                b3 = b3 + a3 * jnp.where(jj >= back, pltpu.roll(b3, back, 1), 0.0)
                a3 = a3 * jnp.where(jj >= back, pltpu.roll(a3, back, 1), 1.0)
            held = lru_ref[l, :, lanes]
            carry = jnp.concatenate([held[q:q + 1].reshape(1, 1, WID) for q in range(h * HALF_SEQ, (h + 1) * HALF_SEQ)], axis=0)
            out = []
            for d in range(8):
                here = slice(d * HALF_SEQ, (d + 1) * HALF_SEQ)
                hs = b3[here] + a3[here] * carry
                carry = hs[:, TOK - 1:TOK, :]
                out.append(hs)
            for q in range(HALF_SEQ):
                lruo_ref[l, h * HALF_SEQ + q:h * HALF_SEQ + q + 1, lanes] = carry[q]
            hs = jnp.concatenate(out, axis=0).reshape(ROWS, WID)
            hbuf[:, lanes] = (hs * gate_y).astype(BF16)
            run_ticks(t, ticks)

        loop(2, body)
        out_small(h, later(ticks, 2))

    def comp_mlp(h, m, ticks):
        base = cw.take(6)

        def body(t, _):
            slot = cw.slot(base, t)
            wait_c(slot)
            n = nbuf[h]
            gate = jax.nn.gelu(dot(n, cring[slot, 0]) + mvec[m, t, 0:1, :], approximate=True)
            up = dot(n, cring[slot, 1]) + mvec[m, t, 1:2, :]
            hbuf[:, pl.ds(pl.multiple_of(t * WID, WID), WID)] = (gate * up).astype(BF16)
            cw.refill(base, 6, t)
            run_ticks(t, ticks)

        loop(6, body)
        base_r = rw.take(8)

        def body_r(i, _):
            for e in range(2):
                wait_r(rw.slot(base_r, 2 * i + e), 3)
            for e in range(2):
                slot = rw.slot(base_r, 2 * i + e)
                store_part(h, 2 * i + e, dot(hbuf[:, 0:512], rring[slot, 0]) + dot(hbuf[:, 512:1024], rring[slot, 1])
                           + dot(hbuf[:, 1024:1536], rring[slot, 2]))
            for e in range(2):
                rw.refill(base_r, 8, 2 * i + e)
            run_ticks(i, later(ticks, 6))

        loop(4, body_r)

    def comp_att(h, l, ticks):
        for c in kv_copies(h * HALF_SEQ, 0):
            c.start()
        def row_order(ref):
            v = ref[h * HALF_SEQ:(h + 1) * HALF_SEQ].reshape(HALF_SEQ, 8, TOK, ROPE_DIM)
            return jnp.concatenate([v[q, d] for d in range(8) for q in range(HALF_SEQ)], axis=0)

        cos, sin = row_order(cos_ref), row_order(sin_ref)

        def rope(v):
            r = v[:, :ROPE_DIM]
            return jnp.concatenate([r * cos + pltpu.roll(r, ROPE_DIM // 2, 1) * sin, v[:, ROPE_DIM:]], axis=1)

        def by_seq(v):
            v = v.reshape(8, HALF_SEQ, TOK, WID)
            return [v[:, s].reshape(64, WID).astype(BF16) for s in range(HALF_SEQ)]

        n = nbuf[h]
        base = cw.take(1)
        slot = cw.slot(base, 0)
        wait_c(slot)
        for e in range(2):
            for s, v in enumerate(by_seq(rope(dot(n, cring[slot, e])))):
                qbuf[s, e * 64:(e + 1) * 64, :] = v
        cw.refill(base, 1, 0)
        run_ticks(0, ticks)
        base = cw.take(1)
        slot = cw.slot(base, 0)
        wait_c(slot)
        for s, v in enumerate(by_seq(rope(dot(n, cring[slot, 0])))):
            ko_ref[h * HALF_SEQ + s] = v
        for s, v in enumerate(by_seq(dot(n, cring[slot, 1]))):
            vo_ref[h * HALF_SEQ + s] = v
        cw.refill(base, 1, 0)
        run_ticks(0, later(ticks, 1))

        def body(s, _):
            seq = h * HALF_SEQ + s
            slot = lax.rem(s, 2)
            for c in kv_copies(seq, slot):
                c.wait()

            @pl.when(s + 1 < HALF_SEQ)
            def _():
                for c in kv_copies(seq + 1, 1 - slot):
                    c.start()

            q = qbuf[s]
            trans = (((1,), (1,)), ((), ()))
            s_old = lax.dot_general(q, kvbuf[slot, 0], trans, preferred_element_type=F32) * 0.0625
            s_new = lax.dot_general(q, ko_ref[seq], trans, preferred_element_type=F32) * 0.0625
            held = slot_ref[pl.ds(seq, 1), :]
            pos = poscol[seq]
            index = lax.rem(lax.broadcasted_iota(jnp.int32, (128, 1), 0), 64)
            last = jnp.where(pos > index, pos, -1)
            s_old = jnp.where((held >= 0) & (held <= last) & (held > pos - WINDOW), s_old, NEG)
            other = lax.broadcasted_iota(jnp.int32, (128, 64), 1)
            s_new = jnp.where((other <= index) & (other >= index - pos), s_new, NEG)
            top = jnp.maximum(row_max(s_old), row_max(s_new))
            e_old = jnp.exp(s_old - top)
            e_new = jnp.exp(s_new - top)
            inv = 1.0 / (row_sum(e_old) + row_sum(e_new))
            o = dot((e_old * inv).astype(BF16), kvbuf[slot, 1]) + dot((e_new * inv).astype(BF16), vo_ref[seq])
            o = o.reshape(2, 8, TOK, WID)
            obuf[:, s, :, 0:WID] = o[0]
            obuf[:, s, :, WID:512] = o[1]
            run_ticks(s, later(ticks, 2))

        loop(HALF_SEQ, body)
        hbuf[:, 0:512] = obuf[...].reshape(ROWS, 512).astype(BF16)
        out_small(h, later(ticks, 6))

    comp = {REC: comp_rec, MLP: comp_mlp, ATT: comp_att}

    cw.prime()
    rw.prime()
    barrier = pltpu.get_barrier_semaphore()
    for other in (sib, xn, yn):
        pl.semaphore_signal(barrier, inc=1, device_id={'tp': other}, device_id_type=pl.DeviceIdType.MESH)
    pl.semaphore_wait(barrier, 3)

    gain[...] = 1.0 + norm_ref[...].astype(F32)
    first(0)
    setup()

    def act(name):
        kind, i, c, h, k = name
        if kind == 'start':
            first(h)
        elif kind == 'ag':
            ag_step(h, i)
        elif i == 3:
            rs3(h, k)
        else:
            (rs0, rs1, rs2)[i](h, c)

    def act_all(names):
        for name in names:
            act(name)

    after, unit = {-1: []}, -1
    for event in plan():
        if event is None:
            unit += 1
            after[unit] = []
        else:
            after[unit].append(event)
    act_all(after[-1])
    base = 0
    for k, (kind, l) in enumerate(SUBLAYERS):
        for h in range(HALVES):
            last = base + UNITS[kind] - 1
            ticks = {u - base: (lambda names=after[u]: act_all(names)) for u in range(base, last) if after[u]}
            comp[kind](h, l, ticks)
            act_all(after[last])
            base = last + 1
    convo_ref[...] = convf[...].astype(BF16)


def update(scal_ref, new_ref, k_cache, v_cache, kn_ref, vn_ref, ko, vo, buf, in_sem, out_sem):
    pairs = [(e, q) for q in range(SEQS) for e in range(2)]

    def copy_in(e, q):
        return pltpu.make_async_copy((k_cache, v_cache)[e].at[q], buf.at[e, q], in_sem.at[e, q])

    def copy_out(e, q):
        return pltpu.make_async_copy(buf.at[e, q], (ko, vo)[e].at[q], out_sem.at[e, q])

    for e, q in pairs:
        copy_in(e, q).start()
    for e, q in pairs:
        copy_in(e, q).wait()
        for start in (pl.multiple_of(scal_ref[q], 16), 0):
            rows = pl.ds(start, SPAN)
            hit = lax.broadcasted_iota(jnp.int32, (SPAN, 64), 0) + start == new_ref[q]
            put = jnp.dot(hit.astype(BF16), (kn_ref, vn_ref)[e][q], preferred_element_type=F32)
            any_hit = row_sum(hit.astype(F32)) > 0.5
            buf[e, q, rows, :] = jnp.where(any_hit, put, buf[e, q, rows, :].astype(F32)).astype(BF16)
        copy_out(e, q).start()
    for e, q in pairs:
        copy_out(e, q).wait()


def solution(mesh):
    def device_body(x_in, seg_pos, conv_state, lru_state, k_cache, v_cache, slot_pos, norm_scale, w_x, b_x, w_y, b_y, conv_w, conv_b, w_a, b_a, w_i, b_i, a_param, w_out, b_out, w_q, w_k, w_v, w_o, b_o, w_1, b_1, w_2, b_2, w_d, b_d):
        lane = lax.broadcasted_iota(jnp.int32, (1, 1, ROPE_DIM), 2)
        half_dim = ROPE_DIM // 2
        timescale = 10000.0 ** (2.0 * (lane % half_dim).astype(F32) / ROPE_DIM)
        angle = seg_pos[:, :, None].astype(F32) / timescale
        cos = jnp.cos(angle)
        sin = jnp.where(lane < half_dim, -jnp.sin(angle), jnp.sin(angle))

        vmem = pl.BlockSpec(memory_space=pltpu.VMEM)
        hbm = pl.BlockSpec(memory_space=pl.ANY)
        sds = jax.ShapeDtypeStruct
        fresh = sds((SEQS, 64, WID), BF16)
        x_out, conv_out, lru_out, k_new, v_new = pl.pallas_call(
            mega,
            out_shape=(sds((64, D), BF16), sds((LAYERS, 3, SEQS, 512), BF16), sds((LAYERS, SEQS, 512), F32), fresh, fresh),
            in_specs=[vmem] * 22 + [hbm] * 12,
            out_specs=[vmem] * 5,
            scratch_shapes=[
                pltpu.VMEM((HALVES, ROWS, D), BF16),
                pltpu.VMEM((HALVES, NBLK, ROWS, COLS), BF16),
                pltpu.VMEM((HALVES, 4, NBLK, SHARD, COLS), BF16),
                pltpu.VMEM((HALVES, NBLK, SHARD, COLS), F32),
                pltpu.VMEM((HALVES, 3, 2, NBLK, PIECE, COLS), BF16),
                pltpu.VMEM((HALVES, 2, NBLK, PIECE, COLS), BF16),
                pltpu.VMEM((HALVES, 2, 2, NBLK, PIECE, COLS), BF16),
                pltpu.VMEM((HALVES, NBLK, SHARD, COLS), BF16),
                pltpu.VMEM((ROWS, 1536), BF16),
                pltpu.VMEM((HALF_SEQ, 128, WID), BF16),
                pltpu.VMEM((8, HALF_SEQ, TOK, 512), F32),
                pltpu.VMEM((HALVES, 2, WINDOW, WID), BF16),
                pltpu.VMEM((NC, 2, D, WID), BF16),
                pltpu.VMEM((NR, 4, 512, COLS), BF16),
                pltpu.VMEM((6, D), F32),
                pltpu.VMEM((6, D), F32),
                pltpu.VMEM((LAYERS, 2, 16, WID), F32),
                pltpu.VMEM((3, 6, 8, WID), F32),
                pltpu.VMEM((LAYERS, SEQS, TOK, 512), F32),
                pltpu.VMEM((LAYERS, 3, SEQS, 512), F32),
                pltpu.VMEM((SEQS, 128, 1), jnp.int32),
                pltpu.VMEM((HALVES, 8, HALF_SEQ, TOK, 1), jnp.int32),
                pltpu.SemaphoreType.DMA((HALVES,)),
                pltpu.SemaphoreType.DMA((HALVES, len(AG_STEPS))),
                pltpu.SemaphoreType.DMA((HALVES,)),
                pltpu.SemaphoreType.DMA((HALVES, RS_SEMS)),
                pltpu.SemaphoreType.DMA((NC, 2)),
                pltpu.SemaphoreType.DMA((NR, 4)),
                pltpu.SemaphoreType.DMA((HALVES, 2)),
            ],
            compiler_params=pltpu.CompilerParams(collective_id=0, has_side_effects=True, vmem_limit_bytes=67043328),
            name='layers',
        )(x_in.reshape(64, D), norm_scale, b_out, b_o[None], b_d, b_y, b_x, conv_w, conv_b, b_a, b_i, a_param, b_1, b_2,
          conv_state.swapaxes(1, 2), lru_state, w_a, w_i, seg_pos, slot_pos, cos, sin,
          w_y, w_x, w_out, w_1, w_2, w_d, w_q, w_k, w_v, w_o, k_cache, v_cache)

        slot_new = seg_pos & (WINDOW - 1)
        window = jnp.minimum(slot_new[:, 0] // 16 * 16, WINDOW - SPAN)
        caches = [sds(k_cache.shape, BF16)] * 2
        k_out, v_out = pl.pallas_call(
            update,
            out_shape=caches,
            in_specs=[pl.BlockSpec(memory_space=pltpu.SMEM), vmem, hbm, hbm, vmem, vmem],
            out_specs=[hbm, hbm],
            scratch_shapes=[pltpu.VMEM((2, SEQS, WINDOW, WID), BF16)] + [pltpu.SemaphoreType.DMA((2, SEQS))] * 2,
            name='caches',
        )(window, slot_new[:, None, :], k_cache, v_cache, k_new, v_new)

        first, last = seg_pos[:, :1], seg_pos[:, 63:]
        count = jnp.where(last < 63, 63 - last, 64)
        slot = lax.broadcasted_iota(jnp.int32, (1, WINDOW), 1)
        ahead = (slot - first) & (WINDOW - 1)
        slot_out = jnp.where(ahead < count, first + ahead, jnp.where(slot < 64 - count, slot, slot_pos))
        return x_out.reshape(8, 8, D), conv_out.swapaxes(1, 2), lru_out, k_out, v_out, slot_out

    col_spec = P(None, None, 'tp')
    vec_spec = P(None, 'tp')
    row_spec = vec_spec
    x_spec, seq_spec, conv_spec, lru_spec = P('dp', 'tp'), P('dp'), P(None, 'dp', None, 'tp'), P(None, 'dp', 'tp')
    arg_specs = (x_spec, seq_spec, conv_spec, lru_spec, seq_spec, seq_spec, seq_spec, P(), col_spec, vec_spec, col_spec, vec_spec, col_spec, vec_spec, row_spec, vec_spec, row_spec, vec_spec, vec_spec, row_spec, P(), vec_spec, P(), P(), P('tp'), P(), col_spec, vec_spec, col_spec, vec_spec, row_spec, P())
    result_specs = (x_spec, conv_spec, lru_spec, seq_spec, seq_spec, seq_spec)
    return jax.shard_map(device_body, mesh=mesh, in_specs=arg_specs, out_specs=result_specs, check_vma=False)
```

```python
import jax
import jax.numpy as jnp
from jax import lax
from jax.experimental import pallas as pl
from jax.experimental.pallas import tpu as pltpu
from jax.sharding import PartitionSpec as P

F32 = jnp.float32
BF16 = jnp.bfloat16
WINDOW = 2048
ROPE_DIM = 128
D = 4096
HALF_SEQ = 4
TOK = 8
SHARD = 32
ROWS = 256
COLS = 512
NBLK = D // COLS
PIECE = 16
NC = 4
NR = 4
WID = 256
HALVES = LAYERS = 2
SEQS = 8
SPAN = 96
NEG = -1e30

REC, MLP, ATT = 'rec', 'mlp', 'att'
SUBLAYERS = ((REC, 0), (MLP, 0), (REC, 1), (MLP, 1), (ATT, 0), (MLP, 2))

UNITS = {REC: 4, MLP: 10, ATT: 8}
STEPS = (('ag', 1, 0), ('ag', 2, 0), ('ag', 1, 1), ('ag', 2, 1), ('ag', 3, 0), ('ag', 3, 1), ('ag', 4, 0),
         ('rs', 0, 0), ('rs', 1, 0), ('rs', 0, 1), ('rs', 1, 1), ('rs', 2, 0), ('rs', 2, 1), ('rs', 3, 0), ('rs', 3, 1))
HALF_BLK = NBLK // 2

PLAN = (
    'aaaaabaa...ab.bbaabbabb.a.a.baa.bbaaaabaaab..b.b..b..b.a',
    'bb..aabbbab..a..a.a..a.ab..bbaabaaaab.bb.b.a.bbaabbabbba',
    '.aa.a.b.aabbabaaaab..b.b..b.b.b.ab..aabbbab..a..a.a..a.b',
    '.a.bbaabaaaab...bb..b..ab.bbaababbb.a..a.a.a..baa.bbaaba',
    'aab..b.b..b.b..abb.b.baabab........ba..bbabaabbbb',
)


def plan():
    def chain(h):
        if h:
            yield 'start', 0, 0, h, 0
        for k in range(len(SUBLAYERS)):
            for step in STEPS:
                yield *step, h, k

    ahead = {'a': chain(0), 'b': chain(1)}
    return [next(ahead[c]) if c in ahead else None for c in ''.join(PLAN)]


class Ring:
    def __init__(self, depth, order, start):
        self.depth, self.start, self.at = depth, start, 0
        self.total = sum(n for _, n in order)
        self.runs = []
        g = 0
        for what, n in order:
            self.runs.append((what, g, n))
            g += n

    def prime(self):
        for what, g0, n in self.runs:
            for t in range(n):
                if g0 + t < self.depth:
                    self.start(what, t, g0 + t)

    def take(self, n):
        base = self.at
        self.at += n
        return base

    def slot(self, base, i):
        return (base + i) % self.depth

    def refill(self, base, n, i):
        ahead = base + self.depth
        slot = self.slot(base, i)
        for what, g0, m in self.runs:
            lo, hi = max(g0, ahead), min(g0 + m, ahead + n)
            if lo < hi:
                if isinstance(i, int):
                    if lo - ahead <= i < hi - ahead:
                        self.start(what, ahead - g0 + i, slot)
                else:
                    @pl.when((i >= lo - ahead) & (i < hi - ahead))
                    def _():
                        self.start(what, ahead - g0 + i, slot)


def loop(n, body):
    def step(i, carry):
        body(i, None)
        return carry

    lax.fori_loop(0, n, step, 0)


def sum_blocks(body):
    return lax.fori_loop(0, NBLK, body, jnp.zeros((PIECE, COLS), F32))


def row_sum(v):
    return jnp.sum(v, axis=-1, keepdims=True)


def row_max(v):
    return jnp.max(v, axis=-1, keepdims=True)


def run_ticks(i, ticks):
    for when, fn in ticks.items():
        if isinstance(i, int):
            if i == when:
                fn()
        else:
            pl.when(i == when)(fn)


def later(ticks, n):
    return {i - n: fn for i, fn in ticks.items()}


def mega(x_ref, norm_ref, bout_ref, bo_ref, bd_ref, by_ref, bx_ref, cw_ref, cb_ref, ba_ref, bi_ref, ap_ref, b1_ref, b2_ref,
         conv_ref, lru_ref, wa_ref, wi_ref, pos_ref, slot_ref, cos_ref, sin_ref,
         w_y, w_x, w_out, w_1, w_2, w_d, w_q, w_k, w_v, w_o, k_cache, v_cache,
         xo_ref, convo_ref, lruo_ref, ko_ref, vo_ref,
         nbuf, part, sibr, town, tbuf, dgr, xyr, xres, hbuf, qbuf, obuf, kvbuf, cring, rring,
         gain, bias, rvec, mvec, conv0, convf, poscol, posrow,
         ag_s, ag_r, rs_s, rs_r, csem, rsem, kvsem):
    me = lax.axis_index('tp')
    core = lax.rem(me, 2)
    xpos = lax.rem(me // 2, 2)
    ypos = me // 4
    sib = me + 1 - 2 * core
    xn = me + 2 - 4 * xpos
    yn = me + 4 - 8 * ypos
    dg = xn + 4 - 8 * ypos

    def start_c(what, t, slot):
        kind, l = what
        cols = pl.ds(t * WID if isinstance(t, int) else pl.multiple_of(t * WID, WID), WID)
        if kind == REC:
            srcs = w_y.at[l, :, cols], w_x.at[l, :, cols]
        elif kind == MLP:
            srcs = w_1.at[l, :, cols], w_2.at[l, :, cols]
        elif kind == 'q':
            srcs = w_q.at[:, pl.ds(0, WID)], w_q.at[:, pl.ds(WID, WID)]
        else:
            srcs = w_k, w_v
        for e, src in enumerate(srcs):
            pltpu.make_async_copy(src, cring.at[slot, e], csem.at[slot, e]).start()

    def wait_c(slot):
        for e, src in enumerate((w_k, w_v)):
            pltpu.make_async_copy(src, cring.at[slot, e], csem.at[slot, e]).wait()

    def start_r(what, t, slot):
        kind, l = what
        if kind == MLP:
            cols = pl.ds(t * COLS if isinstance(t, int) else pl.multiple_of(t * COLS, COLS), COLS)
            for e in range(3):
                pltpu.make_async_copy(w_d.at[l, pl.ds(e * 512, 512), cols], rring.at[slot, e], rsem.at[slot, e]).start()
        else:
            for e in range(4):
                c0 = t * 4 * COLS + e * COLS
                cols = pl.ds(c0 if isinstance(t, int) else pl.multiple_of(c0, COLS), COLS)
                src = w_out.at[l, :, cols] if kind == REC else w_o.at[:, cols]
                pltpu.make_async_copy(src, rring.at[slot, e], rsem.at[slot, e]).start()

    def wait_r(slot, n):
        for e in range(n):
            pltpu.make_async_copy(w_o.at[:, pl.ds(0, COLS)], rring.at[slot, e], rsem.at[slot, e]).wait()

    c_order, r_order = [], []
    for kind, l in SUBLAYERS:
        for _ in range(2):
            if kind == REC:
                c_order.append(((REC, l), 2))
                r_order.append(((REC, l), 2))
            elif kind == MLP:
                c_order.append(((MLP, l), 6))
                r_order.append(((MLP, l), 8))
            else:
                c_order += [(('q', 0), 1), (('kv', 0), 1)]
                r_order.append(((ATT, 0), 2))
    cw = Ring(NC, c_order, start_c)
    rw = Ring(NR, r_order, start_r)

    def kv_copies(seq, slot):
        return (pltpu.make_async_copy(k_cache.at[seq], kvbuf.at[slot, 0], kvsem.at[slot, 0]),
                pltpu.make_async_copy(v_cache.at[seq], kvbuf.at[slot, 1], kvsem.at[slot, 1]))

    def await_bytes(ref, sem):
        pltpu.make_async_copy(ref, ref, sem).wait()

    def rows_of(dev, p=None):
        if p is None:
            return pl.ds(pl.multiple_of(SHARD * dev, SHARD), SHARD)
        return pl.ds(pl.multiple_of(SHARD * dev + PIECE * p, PIECE), PIECE)

    def ag(h, what, r, part=None):
        origin = {'x': me, 'y': me, 'so': me, 'dy': xn, 'dx': yn, 'sx': xn, 'sy': yn, 'sd': dg}[what]
        target = sib if what[0] == 's' else xn if what[-1] == 'x' else yn
        sem = 6 if part is None else 4 + r if what[0] == 'd' else 2 * r + (part if what == 'x' else 1 - part)
        ref = nbuf.at[h, rows_of(origin, r), :] if part is None else nbuf.at[h, rows_of(origin, r), pl.ds(part * D // 2, D // 2)]
        pltpu.make_async_remote_copy(src_ref=ref, dst_ref=ref, send_sem=ag_s.at[h], recv_sem=ag_r.at[h, sem],
                                     device_id={'tp': target}, device_id_type=pl.DeviceIdType.MESH).start()

    def ag_own(h, r):
        ag(h, 'x', r, 0)
        ag(h, 'y', r, 1)
        ag(h, 'x', r, 1)
        ag(h, 'y', r, 0)
        ag(h, 'so', r)

    def ag_step(h, i, r):
        sem = (2 * r, 2 * r + 1, 4 + r, 6)[i - 1]
        await_bytes(nbuf.at[h, pl.ds(0, 8 * PIECE if i == 4 else PIECE), :], ag_r.at[h, sem])
        if i == 1:
            ag(h, 'dy', r, 0)
            ag(h, 'dx', r, 1)
        elif i == 2:
            ag(h, 'sx', r)
            ag(h, 'sy', r)
        elif i == 3:
            ag(h, 'sd', r)
        else:
            await_bytes(nbuf.at[h, pl.ds(0, ROWS - SHARD), :], ag_s.at[h])

    chip_rows = (me, xn, yn, dg)
    other_rows = (sib, xn + 1 - 2 * core, yn + 1 - 2 * core, dg + 1 - 2 * core)

    def remote(h, src, dst, sem, target):
        pltpu.make_async_remote_copy(src_ref=src, dst_ref=dst, send_sem=rs_s.at[h], recv_sem=rs_r.at[h, sem],
                                     device_id={'tp': target}, device_id_type=pl.DeviceIdType.MESH).start()

    def half_blks(c):
        return pl.ds(c * HALF_BLK, HALF_BLK)

    def rs(h, what, r, c):
        cb = half_blks(c)
        if what == 'd':
            remote(h, tbuf.at[h, 2, r, cb], dgr.at[h, r, cb], 2 + r, yn if c else xn)
        else:
            to = 0 if what == 'x' else 1
            remote(h, tbuf.at[h, to, r, cb], xyr.at[h, to, r, cb], 4 + r, yn if to else xn)

    def rs0(h, c):
        cb = half_blks(c)
        for p in (3, 1, 2, 0):
            remote(h, part.at[h, cb, rows_of(other_rows[p]), :], sibr.at[h, p, cb], c, sib)

    def rs1(h, c):
        await_bytes(sibr.at[h, :, half_blks(c)], rs_r.at[h, c])

        def body(i, _):
            j = c * HALF_BLK + i
            for p in range(4):
                v = part[h, j, rows_of(chip_rows[p]), :].astype(F32) + sibr[h, p, j].astype(F32)
                if p == 0:
                    town[h, j] = v
                else:
                    v = v.astype(BF16)
                    tbuf[h, p - 1, 0, j] = v[:PIECE]
                    tbuf[h, p - 1, 1, j] = v[PIECE:]

        loop(HALF_BLK, body)
        if c == 1:
            rs(h, 'd', 0, 0)
            rs(h, 'd', 0, 1)
            rs(h, 'x', 0, 0)
            rs(h, 'y', 0, 1)
            rs(h, 'd', 1, 0)
            rs(h, 'd', 1, 1)

    def rs2(h, r):
        await_bytes(dgr.at[h, r], rs_r.at[h, 2 + r])

        def body(i, _):
            for to, j in ((1, i), (0, HALF_BLK + i)):
                tbuf[h, to, r, j] = (tbuf[h, to, r, j].astype(F32) + dgr[h, r, j].astype(F32)).astype(BF16)

        loop(HALF_BLK, body)
        rs(h, 'x', r, 1)
        rs(h, 'y', r, 0)
        if r == 0:
            rs(h, 'x', 1, 0)
            rs(h, 'y', 1, 1)

    def blk(j):
        return pl.ds(pl.multiple_of(j * COLS, COLS), COLS)

    def normalise(h, k, r, square_sum):
        inv = lax.rsqrt(row_sum(square_sum) * (1.0 / D) + 1e-6)

        def body(j, _):
            nbuf[h, rows_of(me, r), blk(j)] = (xres[h, r, j].astype(F32) * inv * gain[k:k + 1, blk(j)]).astype(BF16)

        loop(NBLK, body)
        ag_own(h, r)

    def first(h):
        for r in range(2):
            def body(j, acc):
                row = h * SHARD + r * PIECE
                v = x_ref[row:row + PIECE, blk(j)]
                xres[h, r, j] = v
                v = v.astype(F32)
                return acc + v * v

            normalise(h, 0, r, sum_blocks(body))

    def rs3(h, k, r):
        await_bytes(xyr.at[h, :, r], rs_r.at[h, 4 + r])
        last = k == len(SUBLAYERS) - 1
        here = slice(r * PIECE, (r + 1) * PIECE)

        def body(j, acc):
            got = xyr[h, 0, r, j].astype(F32) + xyr[h, 1, r, j].astype(F32)
            v = xres[h, r, j].astype(F32) + (town[h, j, here] + got) + bias[k:k + 1, blk(j)]
            v = v.astype(BF16)
            if last:
                row = h * SHARD + r * PIECE
                xo_ref[row:row + PIECE, blk(j)] = v
                return acc
            xres[h, r, j] = v
            v = v.astype(F32)
            return acc + v * v

        square_sum = sum_blocks(body)
        if r == 1:
            await_bytes(part.at[h, :, pl.ds(0, ROWS - SHARD), :], rs_s.at[h])
        if not last:
            normalise(h, k + 1, r, square_sum)

    def setup():
        for k, (ref, l) in enumerate(((bout_ref, 0), (bd_ref, 0), (bout_ref, 1), (bd_ref, 1), (bo_ref, 0), (bd_ref, 2))):
            bias[k:k + 1, :] = ref[...].astype(F32)[l:l + 1]
        rows = [(by_ref[...], 1), (bx_ref[...], 1)] + [(cw_ref[:, i], 1) for i in range(4)]
        rows += [(cb_ref[...], 1), (ba_ref[...], 1), (bi_ref[...], 1), (jax.nn.softplus(ap_ref[...]), -8.0)]
        for r, (v, scale) in enumerate(rows):
            v = v.astype(F32) * scale
            for l in range(LAYERS):
                for t in range(2):
                    rvec[l, t, r:r + 1, :] = v[l:l + 1, t * WID:(t + 1) * WID]
        for r, ref in enumerate((b1_ref, b2_ref)):
            v = ref[...].astype(F32)
            for m in range(3):
                for t in range(6):
                    mvec[m, t, r:r + 1, :] = v[m:m + 1, t * WID:(t + 1) * WID]
        conv0[...] = jnp.zeros_like(conv0)
        for l in range(LAYERS):
            for i in range(3):
                v = conv_ref[l, i].astype(F32)
                for q in range(SEQS):
                    conv0[l, q, 5 + i:6 + i, :] = v[q:q + 1]
        p = pos_ref[...]
        cols = jnp.concatenate([p, p], axis=1).T
        for q in range(SEQS):
            col = cols[:, q:q + 1]
            poscol[q] = col
            posrow[q // HALF_SEQ, :, q % HALF_SEQ] = col[:64].reshape(8, TOK, 1)

    def dot(a, b):
        return jnp.dot(a, b, preferred_element_type=F32)

    def store_part(h, j, v):
        part[h, j] = v.astype(BF16)

    def out_small(h, ticks):
        base = rw.take(2)

        def body(i, _):
            slot = rw.slot(base, i)
            wait_r(slot, 4)
            for e in range(4):
                store_part(h, i * 4 + e, dot(hbuf[:, 0:512], rring[slot, e]))
            rw.refill(base, 2, i)
            run_ticks(i, ticks)

        loop(2, body)

    def comp_rec(h, l, ticks):
        base = cw.take(2)

        def body(t, _):
            slot = cw.slot(base, t)
            wait_c(slot)
            vec = rvec[l, t]
            lanes = pl.ds(pl.multiple_of(t * WID, WID), WID)

            def row(r):
                return vec[r:r + 1, :]

            n = nbuf[h]
            gate_y = jax.nn.gelu(dot(n, cring[slot, 0]) + row(0), approximate=True).astype(BF16).astype(F32)
            u = (dot(n, cring[slot, 1]) + row(1)).astype(BF16).astype(F32)
            cw.refill(base, 2, t)
            u3 = u.reshape(SHARD, TOK, WID)
            for q in range(HALF_SEQ):
                for i in range(3):
                    convf[l, i, h * HALF_SEQ + q:h * HALF_SEQ + q + 1, lanes] = u3[SHARD - HALF_SEQ + q, 5 + i:6 + i, :]
            before = jnp.concatenate([conv0[l, h * HALF_SEQ:(h + 1) * HALF_SEQ, :, lanes], u3[:SHARD - HALF_SEQ]], axis=0)
            jj = lax.broadcasted_iota(jnp.int32, (SHARD, TOK, WID), 1)
            conv = u3 * row(5)
            for back in (1, 2, 3):
                shifted = jnp.where(jj >= back, pltpu.roll(u3, back, 1), pltpu.roll(before, back, 1))
                conv = conv + shifted * row(5 - back)
            conv = (conv + row(6)).reshape(ROWS, WID).astype(BF16)
            gate_r = jax.nn.sigmoid(dot(conv, wa_ref[l, t]) + row(7))
            gate_i = jax.nn.sigmoid(dot(conv, wi_ref[l, t]) + row(8))
            decay = jnp.exp(gate_r * row(9))
            fresh = posrow[h].reshape(ROWS, 1) == 0
            mult = jnp.where(fresh, 1.0, jnp.sqrt(1.0 - decay * decay))
            decay = jnp.where(fresh, 0.0, decay)
            drive = conv.astype(F32) * gate_i * mult
            a3 = decay.reshape(SHARD, TOK, WID)
            b3 = drive.reshape(SHARD, TOK, WID)
            for back in (1, 2, 4):
                b3 = b3 + a3 * jnp.where(jj >= back, pltpu.roll(b3, back, 1), 0.0)
                a3 = a3 * jnp.where(jj >= back, pltpu.roll(a3, back, 1), 1.0)
            held = lru_ref[l, :, lanes]
            carry = jnp.concatenate([held[q:q + 1].reshape(1, 1, WID) for q in range(h * HALF_SEQ, (h + 1) * HALF_SEQ)], axis=0)
            out = []
            for d in range(8):
                here = slice(d * HALF_SEQ, (d + 1) * HALF_SEQ)
                hs = b3[here] + a3[here] * carry
                carry = hs[:, TOK - 1:TOK, :]
                out.append(hs)
            for q in range(HALF_SEQ):
                lruo_ref[l, h * HALF_SEQ + q:h * HALF_SEQ + q + 1, lanes] = carry[q]
            hs = jnp.concatenate(out, axis=0).reshape(ROWS, WID)
            hbuf[:, lanes] = (hs * gate_y).astype(BF16)
            run_ticks(t, ticks)

        loop(2, body)
        out_small(h, later(ticks, 2))

    def comp_mlp(h, m, ticks):
        base = cw.take(6)

        def body(t, _):
            slot = cw.slot(base, t)
            wait_c(slot)
            n = nbuf[h]
            gate = jax.nn.gelu(dot(n, cring[slot, 0]) + mvec[m, t, 0:1, :], approximate=True)
            up = dot(n, cring[slot, 1]) + mvec[m, t, 1:2, :]
            hbuf[:, pl.ds(pl.multiple_of(t * WID, WID), WID)] = (gate * up).astype(BF16)
            cw.refill(base, 6, t)
            run_ticks(t, ticks)

        loop(6, body)
        base_r = rw.take(8)

        def body_r(i, _):
            for e in range(2):
                wait_r(rw.slot(base_r, 2 * i + e), 3)
            for e in range(2):
                slot = rw.slot(base_r, 2 * i + e)
                store_part(h, 2 * i + e, dot(hbuf[:, 0:512], rring[slot, 0]) + dot(hbuf[:, 512:1024], rring[slot, 1])
                           + dot(hbuf[:, 1024:1536], rring[slot, 2]))
            for e in range(2):
                rw.refill(base_r, 8, 2 * i + e)
            run_ticks(i, later(ticks, 6))

        loop(4, body_r)

    def comp_att(h, l, ticks):
        for c in kv_copies(h * HALF_SEQ, 0):
            c.start()
        def row_order(ref):
            v = ref[h * HALF_SEQ:(h + 1) * HALF_SEQ].reshape(HALF_SEQ, 8, TOK, ROPE_DIM)
            return jnp.concatenate([v[q, d] for d in range(8) for q in range(HALF_SEQ)], axis=0)

        cos, sin = row_order(cos_ref), row_order(sin_ref)

        def rope(v):
            r = v[:, :ROPE_DIM]
            return jnp.concatenate([r * cos + pltpu.roll(r, ROPE_DIM // 2, 1) * sin, v[:, ROPE_DIM:]], axis=1)

        def by_seq(v):
            v = v.reshape(8, HALF_SEQ, TOK, WID)
            return [v[:, s].reshape(64, WID).astype(BF16) for s in range(HALF_SEQ)]

        n = nbuf[h]
        base = cw.take(1)
        slot = cw.slot(base, 0)
        wait_c(slot)
        for e in range(2):
            for s, v in enumerate(by_seq(rope(dot(n, cring[slot, e])))):
                qbuf[s, e * 64:(e + 1) * 64, :] = v
        cw.refill(base, 1, 0)
        run_ticks(0, ticks)
        base = cw.take(1)
        slot = cw.slot(base, 0)
        wait_c(slot)
        for s, v in enumerate(by_seq(rope(dot(n, cring[slot, 0])))):
            ko_ref[h * HALF_SEQ + s] = v
        for s, v in enumerate(by_seq(dot(n, cring[slot, 1]))):
            vo_ref[h * HALF_SEQ + s] = v
        cw.refill(base, 1, 0)
        run_ticks(0, later(ticks, 1))

        def body(s, _):
            seq = h * HALF_SEQ + s
            slot = lax.rem(s, 2)
            for c in kv_copies(seq, slot):
                c.wait()

            @pl.when(s + 1 < HALF_SEQ)
            def _():
                for c in kv_copies(seq + 1, 1 - slot):
                    c.start()

            q = qbuf[s]
            trans = (((1,), (1,)), ((), ()))
            s_old = lax.dot_general(q, kvbuf[slot, 0], trans, preferred_element_type=F32) * 0.0625
            s_new = lax.dot_general(q, ko_ref[seq], trans, preferred_element_type=F32) * 0.0625
            held = slot_ref[pl.ds(seq, 1), :]
            pos = poscol[seq]
            index = lax.rem(lax.broadcasted_iota(jnp.int32, (128, 1), 0), 64)
            last = jnp.where(pos > index, pos, -1)
            s_old = jnp.where((held >= 0) & (held <= last) & (held > pos - WINDOW), s_old, NEG)
            other = lax.broadcasted_iota(jnp.int32, (128, 64), 1)
            s_new = jnp.where((other <= index) & (other >= index - pos), s_new, NEG)
            top = jnp.maximum(row_max(s_old), row_max(s_new))
            e_old = jnp.exp(s_old - top)
            e_new = jnp.exp(s_new - top)
            inv = 1.0 / (row_sum(e_old) + row_sum(e_new))
            o = dot((e_old * inv).astype(BF16), kvbuf[slot, 1]) + dot((e_new * inv).astype(BF16), vo_ref[seq])
            o = o.reshape(2, 8, TOK, WID)
            obuf[:, s, :, 0:WID] = o[0]
            obuf[:, s, :, WID:512] = o[1]
            run_ticks(s, later(ticks, 2))

        loop(HALF_SEQ, body)
        hbuf[:, 0:512] = obuf[...].reshape(ROWS, 512).astype(BF16)
        out_small(h, later(ticks, 6))

    comp = {REC: comp_rec, MLP: comp_mlp, ATT: comp_att}

    cw.prime()
    rw.prime()
    barrier = pltpu.get_barrier_semaphore()
    for other in (sib, xn, yn):
        pl.semaphore_signal(barrier, inc=1, device_id={'tp': other}, device_id_type=pl.DeviceIdType.MESH)
    pl.semaphore_wait(barrier, 3)

    gain[...] = 1.0 + norm_ref[...].astype(F32)
    first(0)
    setup()

    def act(name):
        kind, i, c, h, k = name
        if kind == 'start':
            first(h)
        elif kind == 'ag':
            ag_step(h, i, c)
        elif i == 3:
            rs3(h, k, c)
        else:
            (rs0, rs1, rs2)[i](h, c)

    def act_all(names):
        for name in names:
            act(name)

    after, unit = {-1: []}, -1
    for event in plan():
        if event is None:
            unit += 1
            after[unit] = []
        else:
            after[unit].append(event)
    act_all(after[-1])
    base = 0
    for k, (kind, l) in enumerate(SUBLAYERS):
        for h in range(HALVES):
            last = base + UNITS[kind] - 1
            ticks = {u - base: (lambda names=after[u]: act_all(names)) for u in range(base, last) if after[u]}
            comp[kind](h, l, ticks)
            act_all(after[last])
            base = last + 1
    convo_ref[...] = convf[...].astype(BF16)


def update(scal_ref, new_ref, k_cache, v_cache, kn_ref, vn_ref, ko, vo, buf, in_sem, out_sem):
    pairs = [(e, q) for q in range(SEQS) for e in range(2)]

    def copy_in(e, q):
        return pltpu.make_async_copy((k_cache, v_cache)[e].at[q], buf.at[e, q], in_sem.at[e, q])

    def copy_out(e, q):
        return pltpu.make_async_copy(buf.at[e, q], (ko, vo)[e].at[q], out_sem.at[e, q])

    for e, q in pairs:
        copy_in(e, q).start()
    for e, q in pairs:
        copy_in(e, q).wait()
        for start in (pl.multiple_of(scal_ref[q], 16), 0):
            rows = pl.ds(start, SPAN)
            hit = lax.broadcasted_iota(jnp.int32, (SPAN, 64), 0) + start == new_ref[q]
            put = jnp.dot(hit.astype(BF16), (kn_ref, vn_ref)[e][q], preferred_element_type=F32)
            any_hit = row_sum(hit.astype(F32)) > 0.5
            buf[e, q, rows, :] = jnp.where(any_hit, put, buf[e, q, rows, :].astype(F32)).astype(BF16)
        copy_out(e, q).start()
    for e, q in pairs:
        copy_out(e, q).wait()


def solution(mesh):
    def device_body(x_in, seg_pos, conv_state, lru_state, k_cache, v_cache, slot_pos, norm_scale, w_x, b_x, w_y, b_y, conv_w, conv_b, w_a, b_a, w_i, b_i, a_param, w_out, b_out, w_q, w_k, w_v, w_o, b_o, w_1, b_1, w_2, b_2, w_d, b_d):
        lane = lax.broadcasted_iota(jnp.int32, (1, 1, ROPE_DIM), 2)
        half_dim = ROPE_DIM // 2
        timescale = 10000.0 ** (2.0 * (lane % half_dim).astype(F32) / ROPE_DIM)
        angle = seg_pos[:, :, None].astype(F32) / timescale
        cos = jnp.cos(angle)
        sin = jnp.where(lane < half_dim, -jnp.sin(angle), jnp.sin(angle))

        vmem = pl.BlockSpec(memory_space=pltpu.VMEM)
        hbm = pl.BlockSpec(memory_space=pl.ANY)
        sds = jax.ShapeDtypeStruct
        fresh = sds((SEQS, 64, WID), BF16)
        x_out, conv_out, lru_out, k_new, v_new = pl.pallas_call(
            mega,
            out_shape=(sds((64, D), BF16), sds((LAYERS, 3, SEQS, 512), BF16), sds((LAYERS, SEQS, 512), F32), fresh, fresh),
            in_specs=[vmem] * 22 + [hbm] * 12,
            out_specs=[vmem] * 5,
            scratch_shapes=[
                pltpu.VMEM((HALVES, ROWS, D), BF16),
                pltpu.VMEM((HALVES, NBLK, ROWS, COLS), BF16),
                pltpu.VMEM((HALVES, 4, NBLK, SHARD, COLS), BF16),
                pltpu.VMEM((HALVES, NBLK, SHARD, COLS), F32),
                pltpu.VMEM((HALVES, 3, 2, NBLK, PIECE, COLS), BF16),
                pltpu.VMEM((HALVES, 2, NBLK, PIECE, COLS), BF16),
                pltpu.VMEM((HALVES, 2, 2, NBLK, PIECE, COLS), BF16),
                pltpu.VMEM((HALVES, 2, NBLK, PIECE, COLS), BF16),
                pltpu.VMEM((ROWS, 1536), BF16),
                pltpu.VMEM((HALF_SEQ, 128, WID), BF16),
                pltpu.VMEM((8, HALF_SEQ, TOK, 512), F32),
                pltpu.VMEM((HALVES, 2, WINDOW, WID), BF16),
                pltpu.VMEM((NC, 2, D, WID), BF16),
                pltpu.VMEM((NR, 4, 512, COLS), BF16),
                pltpu.VMEM((6, D), F32),
                pltpu.VMEM((6, D), F32),
                pltpu.VMEM((LAYERS, 2, 16, WID), F32),
                pltpu.VMEM((3, 6, 8, WID), F32),
                pltpu.VMEM((LAYERS, SEQS, TOK, 512), F32),
                pltpu.VMEM((LAYERS, 3, SEQS, 512), F32),
                pltpu.VMEM((SEQS, 128, 1), jnp.int32),
                pltpu.VMEM((HALVES, 8, HALF_SEQ, TOK, 1), jnp.int32),
                pltpu.SemaphoreType.DMA((HALVES,)),
                pltpu.SemaphoreType.DMA((HALVES, 7)),
                pltpu.SemaphoreType.DMA((HALVES,)),
                pltpu.SemaphoreType.DMA((HALVES, 6)),
                pltpu.SemaphoreType.DMA((NC, 2)),
                pltpu.SemaphoreType.DMA((NR, 4)),
                pltpu.SemaphoreType.DMA((HALVES, 2)),
            ],
            compiler_params=pltpu.CompilerParams(collective_id=0, has_side_effects=True, vmem_limit_bytes=67043328),
            name='layers',
        )(x_in.reshape(64, D), norm_scale, b_out, b_o[None], b_d, b_y, b_x, conv_w, conv_b, b_a, b_i, a_param, b_1, b_2,
          conv_state.swapaxes(1, 2), lru_state, w_a, w_i, seg_pos, slot_pos, cos, sin,
          w_y, w_x, w_out, w_1, w_2, w_d, w_q, w_k, w_v, w_o, k_cache, v_cache)

        slot_new = seg_pos & (WINDOW - 1)
        window = jnp.minimum(slot_new[:, 0] // 16 * 16, WINDOW - SPAN)
        caches = [sds(k_cache.shape, BF16)] * 2
        k_out, v_out = pl.pallas_call(
            update,
            out_shape=caches,
            in_specs=[pl.BlockSpec(memory_space=pltpu.SMEM), vmem, hbm, hbm, vmem, vmem],
            out_specs=[hbm, hbm],
            scratch_shapes=[pltpu.VMEM((2, SEQS, WINDOW, WID), BF16)] + [pltpu.SemaphoreType.DMA((2, SEQS))] * 2,
            name='caches',
        )(window, slot_new[:, None, :], k_cache, v_cache, k_new, v_new)

        first, last = seg_pos[:, :1], seg_pos[:, 63:]
        count = jnp.where(last < 63, 63 - last, 64)
        slot = lax.broadcasted_iota(jnp.int32, (1, WINDOW), 1)
        ahead = (slot - first) & (WINDOW - 1)
        slot_out = jnp.where(ahead < count, first + ahead, jnp.where(slot < 64 - count, slot, slot_pos))
        return x_out.reshape(8, 8, D), conv_out.swapaxes(1, 2), lru_out, k_out, v_out, slot_out

    col_spec = P(None, None, 'tp')
    vec_spec = P(None, 'tp')
    row_spec = vec_spec
    x_spec, seq_spec, conv_spec, lru_spec = P('dp', 'tp'), P('dp'), P(None, 'dp', None, 'tp'), P(None, 'dp', 'tp')
    arg_specs = (x_spec, seq_spec, conv_spec, lru_spec, seq_spec, seq_spec, seq_spec, P(), col_spec, vec_spec, col_spec, vec_spec, col_spec, vec_spec, row_spec, vec_spec, row_spec, vec_spec, vec_spec, row_spec, P(), vec_spec, P(), P(), P('tp'), P(), col_spec, vec_spec, col_spec, vec_spec, row_spec, P())
    result_specs = (x_spec, conv_spec, lru_spec, seq_spec, seq_spec, seq_spec)
    return jax.shard_map(device_body, mesh=mesh, in_specs=arg_specs, out_specs=result_specs, check_vma=False)
```

```python
import jax
import jax.numpy as jnp
from jax import lax
from jax.experimental import pallas as pl
from jax.experimental.pallas import tpu as pltpu
from jax.sharding import PartitionSpec as P

F32 = jnp.float32
BF16 = jnp.bfloat16
WINDOW = 2048
ROPE_DIM = 128
D = 4096
HALF_SEQ = 4
TOK = 8
SHARD = 32
ROWS = 256
COLS = 512
NBLK = D // COLS
PIECE = 16
NC = 4
NR = 4
WID = 256
HALVES = LAYERS = 2
SEQS = 8
SPAN = 96
NEG = -1e30

REC, MLP, ATT = 'rec', 'mlp', 'att'
SUBLAYERS = ((REC, 0), (MLP, 0), (REC, 1), (MLP, 1), (ATT, 0), (MLP, 2))

UNITS = {REC: 4, MLP: 10, ATT: 8}
STEPS = (('ag', 1, 0), ('ag', 2, 0), ('ag', 1, 1), ('ag', 2, 1), ('ag', 3, 0), ('ag', 3, 1), ('ag', 4, 0),
         ('rs', 0, 0), ('rs', 1, 0), ('rs', 0, 1), ('rs', 1, 1), ('rs', 2, 0), ('rs', 2, 1), ('rs', 3, 0), ('rs', 3, 1))
HALF_BLK = NBLK // 2

PLAN = (
    'aaaaabaa...ab.bbaabbabb.a.a.baa.bbaaaabaaab..b.b..b..b.a',
    'bb..aabbbab..a..a.a..a.ab..bbaabaaaab.bb.b.a.bbaabbabbba',
    '.aa.a.b.aabbabaaaab..b.b..b.b.b.ab..aabbbab..a..a.a..a.b',
    '.a.bbaabaaaab...bb..b..ab.bbaababbb.a..a.a.a..baa.bbaaba',
    'aab..b.b..b.b..abb.b.baabab........ba..bbabaabbbb',
)


def plan():
    def chain(h):
        if h:
            yield 'start', 0, 0, h, 0
        for k in range(len(SUBLAYERS)):
            for step in STEPS:
                yield *step, h, k

    ahead = {'a': chain(0), 'b': chain(1)}
    return [next(ahead[c]) if c in ahead else None for c in ''.join(PLAN)]


class Ring:
    def __init__(self, depth, order, start):
        self.depth, self.start, self.at = depth, start, 0
        self.total = sum(n for _, n in order)
        self.runs = []
        g = 0
        for what, n in order:
            self.runs.append((what, g, n))
            g += n

    def prime(self):
        for what, g0, n in self.runs:
            for t in range(n):
                if g0 + t < self.depth:
                    self.start(what, t, g0 + t)

    def take(self, n):
        base = self.at
        self.at += n
        return base

    def slot(self, base, i):
        return (base + i) % self.depth

    def refill(self, base, n, i):
        ahead = base + self.depth
        slot = self.slot(base, i)
        for what, g0, m in self.runs:
            lo, hi = max(g0, ahead), min(g0 + m, ahead + n)
            if lo < hi:
                if isinstance(i, int):
                    if lo - ahead <= i < hi - ahead:
                        self.start(what, ahead - g0 + i, slot)
                else:
                    @pl.when((i >= lo - ahead) & (i < hi - ahead))
                    def _():
                        self.start(what, ahead - g0 + i, slot)


def loop(n, body):
    def step(i, carry):
        body(i, None)
        return carry

    lax.fori_loop(0, n, step, 0)


def sum_blocks(body):
    return lax.fori_loop(0, NBLK, body, jnp.zeros((PIECE, COLS), F32))


def row_sum(v):
    return jnp.sum(v, axis=-1, keepdims=True)


def row_max(v):
    return jnp.max(v, axis=-1, keepdims=True)


def run_ticks(i, ticks):
    for when, fn in ticks.items():
        if isinstance(i, int):
            if i == when:
                fn()
        else:
            pl.when(i == when)(fn)


def later(ticks, n):
    return {i - n: fn for i, fn in ticks.items()}


def mega(x_ref, norm_ref, bout_ref, bo_ref, bd_ref, by_ref, bx_ref, cw_ref, cb_ref, ba_ref, bi_ref, ap_ref, b1_ref, b2_ref,
         conv_ref, lru_ref, wa_ref, wi_ref, pos_ref, slot_ref, cos_ref, sin_ref,
         w_y, w_x, w_out, w_1, w_2, w_d, w_q, w_k, w_v, w_o, k_cache, v_cache,
         xo_ref, convo_ref, lruo_ref, ko_ref, vo_ref,
         nbuf, part, sibr, town, tbuf, dgr, xyr, xres, hbuf, qbuf, obuf, kvbuf, cring, rring,
         gain, bias, rvec, mvec, conv0, convf, poscol, posrow,
         ag_s, ag_r, rs_s, rs_r, csem, rsem, kvsem):
    me = lax.axis_index('tp')
    core = lax.rem(me, 2)
    xpos = lax.rem(me // 2, 2)
    ypos = me // 4
    sib = me + 1 - 2 * core
    xn = me + 2 - 4 * xpos
    yn = me + 4 - 8 * ypos
    dg = xn + 4 - 8 * ypos

    def start_c(what, t, slot):
        kind, l = what
        cols = pl.ds(t * WID if isinstance(t, int) else pl.multiple_of(t * WID, WID), WID)
        if kind == REC:
            srcs = w_y.at[l, :, cols], w_x.at[l, :, cols]
        elif kind == MLP:
            srcs = w_1.at[l, :, cols], w_2.at[l, :, cols]
        elif kind == 'q':
            srcs = w_q.at[:, pl.ds(0, WID)], w_q.at[:, pl.ds(WID, WID)]
        else:
            srcs = w_k, w_v
        for e, src in enumerate(srcs):
            pltpu.make_async_copy(src, cring.at[slot, e], csem.at[slot, e]).start()

    def wait_c(slot):
        for e, src in enumerate((w_k, w_v)):
            pltpu.make_async_copy(src, cring.at[slot, e], csem.at[slot, e]).wait()

    def start_r(what, t, slot):
        kind, l = what
        if kind == MLP:
            cols = pl.ds(t * COLS if isinstance(t, int) else pl.multiple_of(t * COLS, COLS), COLS)
            for e in range(3):
                pltpu.make_async_copy(w_d.at[l, pl.ds(e * 512, 512), cols], rring.at[slot, e], rsem.at[slot, e]).start()
        else:
            for e in range(4):
                c0 = t * 4 * COLS + e * COLS
                cols = pl.ds(c0 if isinstance(t, int) else pl.multiple_of(c0, COLS), COLS)
                src = w_out.at[l, :, cols] if kind == REC else w_o.at[:, cols]
                pltpu.make_async_copy(src, rring.at[slot, e], rsem.at[slot, e]).start()

    def wait_r(slot, n):
        for e in range(n):
            pltpu.make_async_copy(w_o.at[:, pl.ds(0, COLS)], rring.at[slot, e], rsem.at[slot, e]).wait()

    c_order, r_order = [], []
    for kind, l in SUBLAYERS:
        for _ in range(2):
            if kind == REC:
                c_order.append(((REC, l), 2))
                r_order.append(((REC, l), 2))
            elif kind == MLP:
                c_order.append(((MLP, l), 6))
                r_order.append(((MLP, l), 8))
            else:
                c_order += [(('q', 0), 1), (('kv', 0), 1)]
                r_order.append(((ATT, 0), 2))
    cw = Ring(NC, c_order, start_c)
    rw = Ring(NR, r_order, start_r)

    def kv_copies(seq, slot):
        return (pltpu.make_async_copy(k_cache.at[seq], kvbuf.at[slot, 0], kvsem.at[slot, 0]),
                pltpu.make_async_copy(v_cache.at[seq], kvbuf.at[slot, 1], kvsem.at[slot, 1]))

    def await_bytes(ref, sem):
        pltpu.make_async_copy(ref, ref, sem).wait()

    def rows_of(dev, p=None):
        if p is None:
            return pl.ds(pl.multiple_of(SHARD * dev, SHARD), SHARD)
        return pl.ds(pl.multiple_of(SHARD * dev + PIECE * p, PIECE), PIECE)

    def ag(h, what, r, part=None):
        origin = {'x': me, 'y': me, 'so': me, 'dy': xn, 'dx': yn, 'sx': xn, 'sy': yn, 'sd': dg}[what]
        target = sib if what[0] == 's' else xn if what[-1] == 'x' else yn
        sem = 6 if part is None else 4 + r if what[0] == 'd' else 2 * r + (part if what == 'x' else 1 - part)
        ref = nbuf.at[h, rows_of(origin, r), :] if part is None else nbuf.at[h, rows_of(origin, r), pl.ds(part * D // 2, D // 2)]
        pltpu.make_async_remote_copy(src_ref=ref, dst_ref=ref, send_sem=ag_s.at[h], recv_sem=ag_r.at[h, sem],
                                     device_id={'tp': target}, device_id_type=pl.DeviceIdType.MESH).start()

    def ag_own(h, r):
        ag(h, 'x', r, 0)
        ag(h, 'y', r, 1)
        ag(h, 'x', r, 1)
        ag(h, 'y', r, 0)
        ag(h, 'so', r)

    def ag_step(h, i, r):
        sem = (2 * r, 2 * r + 1, 4 + r, 6)[i - 1]
        await_bytes(nbuf.at[h, pl.ds(0, 8 * PIECE if i == 4 else PIECE), :], ag_r.at[h, sem])
        if i == 1:
            ag(h, 'dy', r, 0)
            ag(h, 'dx', r, 1)
        elif i == 2:
            ag(h, 'sx', r)
            ag(h, 'sy', r)
        elif i == 3:
            ag(h, 'sd', r)
        else:
            await_bytes(nbuf.at[h, pl.ds(0, ROWS - SHARD), :], ag_s.at[h])

    chip_rows = (me, xn, yn, dg)
    other_rows = (sib, xn + 1 - 2 * core, yn + 1 - 2 * core, dg + 1 - 2 * core)

    def remote(h, src, dst, sem, target):
        pltpu.make_async_remote_copy(src_ref=src, dst_ref=dst, send_sem=rs_s.at[h], recv_sem=rs_r.at[h, sem],
                                     device_id={'tp': target}, device_id_type=pl.DeviceIdType.MESH).start()

    def half_blks(c):
        return pl.ds(c * HALF_BLK, HALF_BLK)

    def rs(h, what, r, c):
        cb = half_blks(c)
        if what == 'd':
            remote(h, tbuf.at[h, 2, r, cb], dgr.at[h, r, cb], 2 + r, yn if c else xn)
        else:
            to = 0 if what == 'x' else 1
            remote(h, tbuf.at[h, to, r, cb], xyr.at[h, to, r, cb], 4 + r, yn if to else xn)

    def rs0(h, c):
        cb = half_blks(c)
        for p in (3, 1, 2, 0):
            remote(h, part.at[h, cb, rows_of(other_rows[p]), :], sibr.at[h, p, cb], c, sib)

    def rs1(h, c):
        await_bytes(sibr.at[h, :, half_blks(c)], rs_r.at[h, c])

        def body(i, _):
            j = c * HALF_BLK + i
            for p in range(4):
                v = part[h, j, rows_of(chip_rows[p]), :].astype(F32) + sibr[h, p, j].astype(F32)
                if p == 0:
                    town[h, j] = v
                else:
                    v = v.astype(BF16)
                    tbuf[h, p - 1, 0, j] = v[:PIECE]
                    tbuf[h, p - 1, 1, j] = v[PIECE:]

        loop(HALF_BLK, body)
        if c == 1:
            rs(h, 'd', 0, 0)
            rs(h, 'd', 0, 1)
            rs(h, 'x', 0, 0)
            rs(h, 'y', 0, 1)
            rs(h, 'd', 1, 0)
            rs(h, 'd', 1, 1)

    def rs2(h, r):
        await_bytes(dgr.at[h, r], rs_r.at[h, 2 + r])

        def body(i, _):
            for to, j in ((1, i), (0, HALF_BLK + i)):
                tbuf[h, to, r, j] = (tbuf[h, to, r, j].astype(F32) + dgr[h, r, j].astype(F32)).astype(BF16)

        loop(HALF_BLK, body)
        rs(h, 'x', r, 1)
        rs(h, 'y', r, 0)
        if r == 0:
            rs(h, 'x', 1, 0)
            rs(h, 'y', 1, 1)

    def blk(j):
        return pl.ds(pl.multiple_of(j * COLS, COLS), COLS)

    def normalise(h, k, r, square_sum):
        inv = lax.rsqrt(row_sum(square_sum) * (1.0 / D) + 1e-6)

        def body(j, _):
            nbuf[h, rows_of(me, r), blk(j)] = (xres[h, r, j].astype(F32) * inv * gain[k:k + 1, blk(j)]).astype(BF16)

        loop(NBLK, body)
        ag_own(h, r)

    def first(h):
        for r in range(2):
            def body(j, acc):
                row = h * SHARD + r * PIECE
                v = x_ref[row:row + PIECE, blk(j)]
                xres[h, r, j] = v
                v = v.astype(F32)
                return acc + v * v

            normalise(h, 0, r, sum_blocks(body))

    def rs3(h, k, r):
        await_bytes(xyr.at[h, :, r], rs_r.at[h, 4 + r])
        last = k == len(SUBLAYERS) - 1
        here = slice(r * PIECE, (r + 1) * PIECE)

        def body(j, acc):
            got = xyr[h, 0, r, j].astype(F32) + xyr[h, 1, r, j].astype(F32)
            v = xres[h, r, j].astype(F32) + (town[h, j, here] + got) + bias[k:k + 1, blk(j)]
            v = v.astype(BF16)
            if last:
                row = h * SHARD + r * PIECE
                xo_ref[row:row + PIECE, blk(j)] = v
                return acc
            xres[h, r, j] = v
            v = v.astype(F32)
            return acc + v * v

        square_sum = sum_blocks(body)
        if r == 1:
            await_bytes(part.at[h, :, pl.ds(0, ROWS - SHARD), :], rs_s.at[h])
        if not last:
            normalise(h, k + 1, r, square_sum)

    def setup():
        for k, (ref, l) in enumerate(((bout_ref, 0), (bd_ref, 0), (bout_ref, 1), (bd_ref, 1), (bo_ref, None), (bd_ref, 2))):
            v = ref[...].astype(F32)
            bias[k:k + 1, :] = v.reshape(1, D) if l is None else v[l:l + 1]
        rows = [(by_ref[...], 1), (bx_ref[...], 1)] + [(cw_ref[:, i], 1) for i in range(4)]
        rows += [(cb_ref[...], 1), (ba_ref[...], 1), (bi_ref[...], 1), (jax.nn.softplus(ap_ref[...]), -8.0)]
        for r, (v, scale) in enumerate(rows):
            v = v.astype(F32) * scale
            for l in range(LAYERS):
                for t in range(2):
                    rvec[l, t, r:r + 1, :] = v[l:l + 1, t * WID:(t + 1) * WID]
        for r, ref in enumerate((b1_ref, b2_ref)):
            v = ref[...].astype(F32)
            for m in range(3):
                for t in range(6):
                    mvec[m, t, r:r + 1, :] = v[m:m + 1, t * WID:(t + 1) * WID]
        conv0[...] = jnp.zeros_like(conv0)
        for l in range(LAYERS):
            for i in range(3):
                v = conv_ref[l, i].astype(F32)
                for q in range(SEQS):
                    conv0[l, q, 5 + i:6 + i, :] = v[q:q + 1]
        p = pos_ref[...]
        cols = jnp.concatenate([p, p], axis=1).T
        for q in range(SEQS):
            col = cols[:, q:q + 1]
            poscol[q] = col
            posrow[q // HALF_SEQ, :, q % HALF_SEQ] = col[:64].reshape(8, TOK, 1)

    def dot(a, b):
        return jnp.dot(a, b, preferred_element_type=F32)

    def store_part(h, j, v):
        part[h, j] = v.astype(BF16)

    def out_small(h, ticks):
        base = rw.take(2)

        def body(i, _):
            slot = rw.slot(base, i)
            wait_r(slot, 4)
            for e in range(4):
                store_part(h, i * 4 + e, dot(hbuf[:, 0:512], rring[slot, e]))
            rw.refill(base, 2, i)
            run_ticks(i, ticks)

        loop(2, body)

    def comp_rec(h, l, ticks):
        base = cw.take(2)

        def body(t, _):
            slot = cw.slot(base, t)
            wait_c(slot)
            vec = rvec[l, t]
            lanes = pl.ds(pl.multiple_of(t * WID, WID), WID)

            def row(r):
                return vec[r:r + 1, :]

            n = nbuf[h]
            gate_y = jax.nn.gelu(dot(n, cring[slot, 0]) + row(0), approximate=True).astype(BF16).astype(F32)
            u = (dot(n, cring[slot, 1]) + row(1)).astype(BF16).astype(F32)
            cw.refill(base, 2, t)
            u3 = u.reshape(SHARD, TOK, WID)
            for q in range(HALF_SEQ):
                for i in range(3):
                    convf[l, i, h * HALF_SEQ + q:h * HALF_SEQ + q + 1, lanes] = u3[SHARD - HALF_SEQ + q, 5 + i:6 + i, :]
            before = jnp.concatenate([conv0[l, h * HALF_SEQ:(h + 1) * HALF_SEQ, :, lanes], u3[:SHARD - HALF_SEQ]], axis=0)
            jj = lax.broadcasted_iota(jnp.int32, (SHARD, TOK, WID), 1)
            conv = u3 * row(5)
            for back in (1, 2, 3):
                shifted = jnp.where(jj >= back, pltpu.roll(u3, back, 1), pltpu.roll(before, back, 1))
                conv = conv + shifted * row(5 - back)
            conv = (conv + row(6)).reshape(ROWS, WID).astype(BF16)
            gate_r = jax.nn.sigmoid(dot(conv, wa_ref[l, t]) + row(7))
            gate_i = jax.nn.sigmoid(dot(conv, wi_ref[l, t]) + row(8))
            decay = jnp.exp(gate_r * row(9))
            fresh = posrow[h].reshape(ROWS, 1) == 0
            mult = jnp.where(fresh, 1.0, jnp.sqrt(1.0 - decay * decay))
            decay = jnp.where(fresh, 0.0, decay)
            drive = conv.astype(F32) * gate_i * mult
            a3 = decay.reshape(SHARD, TOK, WID)
            b3 = drive.reshape(SHARD, TOK, WID)
            for back in (1, 2, 4):
                b3 = b3 + a3 * jnp.where(jj >= back, pltpu.roll(b3, back, 1), 0.0)
                a3 = a3 * jnp.where(jj >= back, pltpu.roll(a3, back, 1), 1.0)
            held = lru_ref[l, :, lanes]
            carry = jnp.concatenate([held[q:q + 1].reshape(1, 1, WID) for q in range(h * HALF_SEQ, (h + 1) * HALF_SEQ)], axis=0)
            out = []
            for d in range(8):
                here = slice(d * HALF_SEQ, (d + 1) * HALF_SEQ)
                hs = b3[here] + a3[here] * carry
                carry = hs[:, TOK - 1:TOK, :]
                out.append(hs)
            for q in range(HALF_SEQ):
                lruo_ref[l, h * HALF_SEQ + q:h * HALF_SEQ + q + 1, lanes] = carry[q]
            hs = jnp.concatenate(out, axis=0).reshape(ROWS, WID)
            hbuf[:, lanes] = (hs * gate_y).astype(BF16)
            run_ticks(t, ticks)

        loop(2, body)
        out_small(h, later(ticks, 2))

    def comp_mlp(h, m, ticks):
        base = cw.take(6)

        def body(t, _):
            slot = cw.slot(base, t)
            wait_c(slot)
            n = nbuf[h]
            gate = jax.nn.gelu(dot(n, cring[slot, 0]) + mvec[m, t, 0:1, :], approximate=True)
            up = dot(n, cring[slot, 1]) + mvec[m, t, 1:2, :]
            hbuf[:, pl.ds(pl.multiple_of(t * WID, WID), WID)] = (gate * up).astype(BF16)
            cw.refill(base, 6, t)
            run_ticks(t, ticks)

        loop(6, body)
        base_r = rw.take(8)

        def body_r(i, _):
            for e in range(2):
                wait_r(rw.slot(base_r, 2 * i + e), 3)
            for e in range(2):
                slot = rw.slot(base_r, 2 * i + e)
                store_part(h, 2 * i + e, dot(hbuf[:, 0:512], rring[slot, 0]) + dot(hbuf[:, 512:1024], rring[slot, 1])
                           + dot(hbuf[:, 1024:1536], rring[slot, 2]))
            for e in range(2):
                rw.refill(base_r, 8, 2 * i + e)
            run_ticks(i, later(ticks, 6))

        loop(4, body_r)

    def comp_att(h, l, ticks):
        for c in kv_copies(h * HALF_SEQ, 0):
            c.start()
        def row_order(ref):
            v = ref[h * HALF_SEQ:(h + 1) * HALF_SEQ].reshape(HALF_SEQ, 8, TOK, ROPE_DIM)
            return jnp.concatenate([v[q, d] for d in range(8) for q in range(HALF_SEQ)], axis=0)

        cos, sin = row_order(cos_ref), row_order(sin_ref)

        def rope(v):
            r = v[:, :ROPE_DIM]
            return jnp.concatenate([r * cos + pltpu.roll(r, ROPE_DIM // 2, 1) * sin, v[:, ROPE_DIM:]], axis=1)

        def by_seq(v):
            v = v.reshape(8, HALF_SEQ, TOK, WID)
            return [v[:, s].reshape(64, WID).astype(BF16) for s in range(HALF_SEQ)]

        n = nbuf[h]
        base = cw.take(1)
        slot = cw.slot(base, 0)
        wait_c(slot)
        for e in range(2):
            for s, v in enumerate(by_seq(rope(dot(n, cring[slot, e])))):
                qbuf[s, e * 64:(e + 1) * 64, :] = v
        cw.refill(base, 1, 0)
        run_ticks(0, ticks)
        base = cw.take(1)
        slot = cw.slot(base, 0)
        wait_c(slot)
        for s, v in enumerate(by_seq(rope(dot(n, cring[slot, 0])))):
            ko_ref[h * HALF_SEQ + s] = v
        for s, v in enumerate(by_seq(dot(n, cring[slot, 1]))):
            vo_ref[h * HALF_SEQ + s] = v
        cw.refill(base, 1, 0)
        run_ticks(0, later(ticks, 1))

        def body(s, _):
            seq = h * HALF_SEQ + s
            slot = lax.rem(s, 2)
            for c in kv_copies(seq, slot):
                c.wait()

            @pl.when(s + 1 < HALF_SEQ)
            def _():
                for c in kv_copies(seq + 1, 1 - slot):
                    c.start()

            q = qbuf[s]
            trans = (((1,), (1,)), ((), ()))
            s_old = lax.dot_general(q, kvbuf[slot, 0], trans, preferred_element_type=F32) * 0.0625
            s_new = lax.dot_general(q, ko_ref[seq], trans, preferred_element_type=F32) * 0.0625
            held = slot_ref[pl.ds(seq, 1), :]
            pos = poscol[seq]
            index = lax.rem(lax.broadcasted_iota(jnp.int32, (128, 1), 0), 64)
            last = jnp.where(pos > index, pos, -1)
            s_old = jnp.where((held >= 0) & (held <= last) & (held > pos - WINDOW), s_old, NEG)
            other = lax.broadcasted_iota(jnp.int32, (128, 64), 1)
            s_new = jnp.where((other <= index) & (other >= index - pos), s_new, NEG)
            top = jnp.maximum(row_max(s_old), row_max(s_new))
            e_old = jnp.exp(s_old - top)
            e_new = jnp.exp(s_new - top)
            inv = 1.0 / (row_sum(e_old) + row_sum(e_new))
            o = dot((e_old * inv).astype(BF16), kvbuf[slot, 1]) + dot((e_new * inv).astype(BF16), vo_ref[seq])
            o = o.reshape(2, 8, TOK, WID)
            obuf[:, s, :, 0:WID] = o[0]
            obuf[:, s, :, WID:512] = o[1]
            run_ticks(s, later(ticks, 2))

        loop(HALF_SEQ, body)
        hbuf[:, 0:512] = obuf[...].reshape(ROWS, 512).astype(BF16)
        out_small(h, later(ticks, 6))

    comp = {REC: comp_rec, MLP: comp_mlp, ATT: comp_att}

    cw.prime()
    rw.prime()
    barrier = pltpu.get_barrier_semaphore()
    for other in (sib, xn, yn):
        pl.semaphore_signal(barrier, inc=1, device_id={'tp': other}, device_id_type=pl.DeviceIdType.MESH)
    pl.semaphore_wait(barrier, 3)

    gain[...] = 1.0 + norm_ref[...].astype(F32)
    first(0)
    setup()

    def act(name):
        kind, i, c, h, k = name
        if kind == 'start':
            first(h)
        elif kind == 'ag':
            ag_step(h, i, c)
        elif i == 3:
            rs3(h, k, c)
        else:
            (rs0, rs1, rs2)[i](h, c)

    def act_all(names):
        for name in names:
            act(name)

    after, unit = {-1: []}, -1
    for event in plan():
        if event is None:
            unit += 1
            after[unit] = []
        else:
            after[unit].append(event)
    act_all(after[-1])
    base = 0
    for k, (kind, l) in enumerate(SUBLAYERS):
        for h in range(HALVES):
            last = base + UNITS[kind] - 1
            ticks = {u - base: (lambda names=after[u]: act_all(names)) for u in range(base, last) if after[u]}
            comp[kind](h, l, ticks)
            act_all(after[last])
            base = last + 1
    convo_ref[...] = convf[...].astype(BF16)


def finish(pos_s, pos_ref, slot_ref, k_cache, v_cache, kn_ref, vn_ref, x_ref, conv_ref, lru_ref,
           ko, vo, so_ref, xo_ref, convo_ref, lruo_ref, buf, in_sem, out_sem):
    pairs = [(e, q) for q in range(SEQS) for e in range(2)]

    def copy_in(e, q):
        return pltpu.make_async_copy((k_cache, v_cache)[e].at[q], buf.at[e, q], in_sem.at[e, q])

    def copy_out(e, q):
        return pltpu.make_async_copy(buf.at[e, q], (ko, vo)[e].at[q], out_sem.at[e, q])

    for e, q in pairs:
        copy_in(e, q).start()
    xo_ref[...] = x_ref[...]
    convo_ref[...] = conv_ref[...]
    lruo_ref[...] = lru_ref[...]
    begin, last = pos_ref[:, 0:1], pos_ref[:, 63:64]
    count = jnp.where(last < 63, 63 - last, 64)
    slot = lax.broadcasted_iota(jnp.int32, (SEQS, WINDOW), 1)
    ahead = (slot - begin) & (WINDOW - 1)
    so_ref[...] = jnp.where(ahead < count, begin + ahead, jnp.where(slot < 64 - count, slot, slot_ref[...]))
    for q in range(SEQS):
        first_row = pl.multiple_of(jnp.minimum((pos_s[q, 0] & (WINDOW - 1)) // PIECE * PIECE, WINDOW - SPAN), PIECE)
        new_slots = pos_ref[q:q + 1, :] & (WINDOW - 1)
        for e in range(2):
            copy_in(e, q).wait()
        for start in (first_row, 0):
            rows = pl.ds(start, SPAN)
            hit = lax.broadcasted_iota(jnp.int32, (SPAN, 64), 0) + start == new_slots
            any_hit = row_sum(hit.astype(F32)) > 0.5
            for e, ref in enumerate((kn_ref, vn_ref)):
                put = jnp.dot(hit.astype(BF16), ref[q], preferred_element_type=F32)
                buf[e, q, rows, :] = jnp.where(any_hit, put, buf[e, q, rows, :].astype(F32)).astype(BF16)
        for e in range(2):
            copy_out(e, q).start()
    for e, q in pairs:
        copy_out(e, q).wait()


def solution(mesh):
    def device_body(x_in, seg_pos, conv_state, lru_state, k_cache, v_cache, slot_pos, norm_scale, w_x, b_x, w_y, b_y, conv_w, conv_b, w_a, b_a, w_i, b_i, a_param, w_out, b_out, w_q, w_k, w_v, w_o, b_o, w_1, b_1, w_2, b_2, w_d, b_d):
        lane = lax.broadcasted_iota(jnp.int32, (1, 1, ROPE_DIM), 2)
        half_dim = ROPE_DIM // 2
        timescale = 10000.0 ** (2.0 * (lane % half_dim).astype(F32) / ROPE_DIM)
        angle = seg_pos[:, :, None].astype(F32) / timescale
        cos = jnp.cos(angle)
        sin = jnp.where(lane < half_dim, -jnp.sin(angle), jnp.sin(angle))

        vmem = pl.BlockSpec(memory_space=pltpu.VMEM)
        hbm = pl.BlockSpec(memory_space=pl.ANY)
        sds = jax.ShapeDtypeStruct
        fresh = sds((SEQS, 64, WID), BF16)
        x_out, conv_out, lru_out, k_new, v_new = pl.pallas_call(
            mega,
            out_shape=(sds((64, D), BF16), sds((LAYERS, 3, SEQS, 512), BF16), sds((LAYERS, SEQS, 512), F32), fresh, fresh),
            in_specs=[vmem] * 22 + [hbm] * 12,
            out_specs=[vmem] * 5,
            scratch_shapes=[
                pltpu.VMEM((HALVES, ROWS, D), BF16),
                pltpu.VMEM((HALVES, NBLK, ROWS, COLS), BF16),
                pltpu.VMEM((HALVES, 4, NBLK, SHARD, COLS), BF16),
                pltpu.VMEM((HALVES, NBLK, SHARD, COLS), F32),
                pltpu.VMEM((HALVES, 3, 2, NBLK, PIECE, COLS), BF16),
                pltpu.VMEM((HALVES, 2, NBLK, PIECE, COLS), BF16),
                pltpu.VMEM((HALVES, 2, 2, NBLK, PIECE, COLS), BF16),
                pltpu.VMEM((HALVES, 2, NBLK, PIECE, COLS), BF16),
                pltpu.VMEM((ROWS, 1536), BF16),
                pltpu.VMEM((HALF_SEQ, 128, WID), BF16),
                pltpu.VMEM((8, HALF_SEQ, TOK, 512), F32),
                pltpu.VMEM((HALVES, 2, WINDOW, WID), BF16),
                pltpu.VMEM((NC, 2, D, WID), BF16),
                pltpu.VMEM((NR, 4, 512, COLS), BF16),
                pltpu.VMEM((6, D), F32),
                pltpu.VMEM((6, D), F32),
                pltpu.VMEM((LAYERS, 2, 16, WID), F32),
                pltpu.VMEM((3, 6, 8, WID), F32),
                pltpu.VMEM((LAYERS, SEQS, TOK, 512), F32),
                pltpu.VMEM((LAYERS, 3, SEQS, 512), F32),
                pltpu.VMEM((SEQS, 128, 1), jnp.int32),
                pltpu.VMEM((HALVES, 8, HALF_SEQ, TOK, 1), jnp.int32),
                pltpu.SemaphoreType.DMA((HALVES,)),
                pltpu.SemaphoreType.DMA((HALVES, 7)),
                pltpu.SemaphoreType.DMA((HALVES,)),
                pltpu.SemaphoreType.DMA((HALVES, 6)),
                pltpu.SemaphoreType.DMA((NC, 2)),
                pltpu.SemaphoreType.DMA((NR, 4)),
                pltpu.SemaphoreType.DMA((HALVES, 2)),
            ],
            compiler_params=pltpu.CompilerParams(collective_id=0, has_side_effects=True, vmem_limit_bytes=67043328),
            name='layers',
        )(x_in.reshape(64, D), norm_scale, b_out, b_o, b_d, b_y, b_x, conv_w, conv_b, b_a, b_i, a_param, b_1, b_2,
          conv_state.swapaxes(1, 2), lru_state, w_a, w_i, seg_pos, slot_pos, cos, sin,
          w_y, w_x, w_out, w_1, w_2, w_d, w_q, w_k, w_v, w_o, k_cache, v_cache)

        k_out, v_out, slot_out, x_out, conv_out, lru_out = pl.pallas_call(
            finish,
            out_shape=[sds(v.shape, v.dtype) for v in (k_cache, v_cache, slot_pos, x_out, conv_out, lru_out)],
            in_specs=[pl.BlockSpec(memory_space=pltpu.SMEM), vmem, vmem, hbm, hbm] + [vmem] * 5,
            out_specs=[hbm, hbm] + [vmem] * 4,
            scratch_shapes=[pltpu.VMEM((2, SEQS, WINDOW, WID), BF16)] + [pltpu.SemaphoreType.DMA((2, SEQS))] * 2,
            name='caches',
        )(seg_pos, seg_pos, slot_pos, k_cache, v_cache, k_new, v_new, x_out, conv_out, lru_out)
        return x_out.reshape(SEQS, TOK, D), conv_out.swapaxes(1, 2), lru_out, k_out, v_out, slot_out

    col_spec = P(None, None, 'tp')
    vec_spec = P(None, 'tp')
    row_spec = vec_spec
    x_spec, seq_spec, conv_spec, lru_spec = P('dp', 'tp'), P('dp'), P(None, 'dp', None, 'tp'), P(None, 'dp', 'tp')
    arg_specs = (x_spec, seq_spec, conv_spec, lru_spec, seq_spec, seq_spec, seq_spec, P(), col_spec, vec_spec, col_spec, vec_spec, col_spec, vec_spec, row_spec, vec_spec, row_spec, vec_spec, vec_spec, row_spec, P(), vec_spec, P(), P(), P('tp'), P(), col_spec, vec_spec, col_spec, vec_spec, row_spec, P())
    result_specs = (x_spec, conv_spec, lru_spec, seq_spec, seq_spec, seq_spec)
    return jax.shard_map(device_body, mesh=mesh, in_specs=arg_specs, out_specs=result_specs, check_vma=False)
```

```python
import jax
import jax.numpy as jnp
from jax import lax
from jax.experimental import pallas as pl
from jax.experimental.pallas import tpu as pltpu
from jax.sharding import PartitionSpec as P

F32 = jnp.float32
BF16 = jnp.bfloat16
WINDOW = 2048
ROPE_DIM = 128
D = 4096
HALF_SEQ = 4
TOK = 8
SHARD = 32
ROWS = 256
COLS = 512
NBLK = D // COLS
PIECE = 16
NC = 4
NR = 4
WID = 256
HALVES = LAYERS = 2
SEQS = 8
TOKENS = 64
BIG = 1 << 30
SPAN = 96
NEG = -1e30

REC, MLP, ATT = 'rec', 'mlp', 'att'
SUBLAYERS = ((REC, 0), (MLP, 0), (REC, 1), (MLP, 1), (ATT, 0), (MLP, 2))

UNITS = {REC: 4, MLP: 10, ATT: 8}
STEPS = (('ag', 1, 0), ('ag', 2, 0), ('ag', 1, 1), ('ag', 2, 1), ('ag', 3, 0), ('ag', 3, 1), ('ag', 4, 0),
         ('rs', 0, 0), ('rs', 1, 0), ('rs', 0, 1), ('rs', 1, 1), ('rs', 2, 0), ('rs', 2, 1), ('rs', 3, 0), ('rs', 3, 1))
HALF_BLK = NBLK // 2

PLAN = (
    'aaaaabaa...ab.bbaabbabb.a.a.baa.bbaaaabaaab..b.b..b..b.a',
    'bb..aabbbab..a..a.a..a.ab..bbaabaaaab.bb.b.a.bbaabbabbba',
    '.aa.a.b.aabbabaaaab..b.b..b.b.b.ab..aabbbab..a..a.a..a.b',
    '.a.bbaabaaaab...bb..b..ab.bbaababbb.a..a.a.a..baa.bbaaba',
    'aab..b.b..b.b..abb.b.baabab........ba..bbabaabbbb',
)


def plan():
    def chain(h):
        if h:
            yield 'start', 0, 0, h, 0
        for k in range(len(SUBLAYERS)):
            for step in STEPS:
                yield *step, h, k

    ahead = {'a': chain(0), 'b': chain(1)}
    return [next(ahead[c]) if c in ahead else None for c in ''.join(PLAN)]


class Ring:
    def __init__(self, depth, order, start):
        self.depth, self.start, self.at = depth, start, 0
        self.total = sum(n for _, n in order)
        self.runs = []
        g = 0
        for what, n in order:
            self.runs.append((what, g, n))
            g += n

    def prime(self):
        for what, g0, n in self.runs:
            for t in range(n):
                if g0 + t < self.depth:
                    self.start(what, t, g0 + t)

    def take(self, n):
        base = self.at
        self.at += n
        return base

    def slot(self, base, i):
        return (base + i) % self.depth

    def refill(self, base, n, i):
        ahead = base + self.depth
        slot = self.slot(base, i)
        for what, g0, m in self.runs:
            lo, hi = max(g0, ahead), min(g0 + m, ahead + n)
            if lo < hi:
                if isinstance(i, int):
                    if lo - ahead <= i < hi - ahead:
                        self.start(what, ahead - g0 + i, slot)
                else:
                    @pl.when((i >= lo - ahead) & (i < hi - ahead))
                    def _():
                        self.start(what, ahead - g0 + i, slot)


def loop(n, body):
    def step(i, carry):
        body(i, None)
        return carry

    lax.fori_loop(0, n, step, 0)


def sum_blocks(body):
    return lax.fori_loop(0, NBLK, body, jnp.zeros((PIECE, COLS), F32))


def row_sum(v):
    return jnp.sum(v, axis=-1, keepdims=True)


def row_max(v):
    return jnp.max(v, axis=-1, keepdims=True)


def run_ticks(i, ticks):
    for when, fn in ticks.items():
        if isinstance(i, int):
            if i == when:
                fn()
        else:
            pl.when(i == when)(fn)


def later(ticks, n):
    return {i - n: fn for i, fn in ticks.items()}


def mega(x_ref, norm_ref, bout_ref, bo_ref, bd_ref, by_ref, bx_ref, cw_ref, cb_ref, ba_ref, bi_ref, ap_ref, b1_ref, b2_ref,
         conv_ref, lru_ref, wa_ref, wi_ref, pos_ref, slot_ref, scale_ref,
         w_y, w_x, w_out, w_1, w_2, w_d, w_q, w_k, w_v, w_o, k_cache, v_cache,
         xo_ref, convo_ref, lruo_ref, ko_ref, vo_ref,
         nbuf, part, sibr, town, tbuf, dgr, xyr, xres, hbuf, qbuf, obuf, kvbuf, cring, rring,
         gain, bias, rvec, mvec, conv0, convf, poscol, posrow, costab, sintab,
         ag_s, ag_r, rs_s, rs_r, csem, rsem, kvsem):
    me = lax.axis_index('tp')
    core = lax.rem(me, 2)
    xpos = lax.rem(me // 2, 2)
    ypos = me // 4
    sib = me + 1 - 2 * core
    xn = me + 2 - 4 * xpos
    yn = me + 4 - 8 * ypos
    dg = xn + 4 - 8 * ypos

    def start_c(what, t, slot):
        kind, l = what
        cols = pl.ds(t * WID if isinstance(t, int) else pl.multiple_of(t * WID, WID), WID)
        if kind == REC:
            srcs = w_y.at[l, :, cols], w_x.at[l, :, cols]
        elif kind == MLP:
            srcs = w_1.at[l, :, cols], w_2.at[l, :, cols]
        elif kind == 'q':
            srcs = w_q.at[:, pl.ds(0, WID)], w_q.at[:, pl.ds(WID, WID)]
        else:
            srcs = w_k, w_v
        for e, src in enumerate(srcs):
            pltpu.make_async_copy(src, cring.at[slot, e], csem.at[slot, e]).start()

    def wait_c(slot):
        for e, src in enumerate((w_k, w_v)):
            pltpu.make_async_copy(src, cring.at[slot, e], csem.at[slot, e]).wait()

    def start_r(what, t, slot):
        kind, l = what
        if kind == MLP:
            cols = pl.ds(t * COLS if isinstance(t, int) else pl.multiple_of(t * COLS, COLS), COLS)
            for e in range(3):
                pltpu.make_async_copy(w_d.at[l, pl.ds(e * 512, 512), cols], rring.at[slot, e], rsem.at[slot, e]).start()
        else:
            for e in range(4):
                c0 = t * 4 * COLS + e * COLS
                cols = pl.ds(c0 if isinstance(t, int) else pl.multiple_of(c0, COLS), COLS)
                src = w_out.at[l, :, cols] if kind == REC else w_o.at[:, cols]
                pltpu.make_async_copy(src, rring.at[slot, e], rsem.at[slot, e]).start()

    def wait_r(slot, n):
        for e in range(n):
            pltpu.make_async_copy(w_o.at[:, pl.ds(0, COLS)], rring.at[slot, e], rsem.at[slot, e]).wait()

    c_order, r_order = [], []
    for kind, l in SUBLAYERS:
        for _ in range(2):
            if kind == REC:
                c_order.append(((REC, l), 2))
                r_order.append(((REC, l), 2))
            elif kind == MLP:
                c_order.append(((MLP, l), 6))
                r_order.append(((MLP, l), 8))
            else:
                c_order += [(('q', 0), 1), (('kv', 0), 1)]
                r_order.append(((ATT, 0), 2))
    cw = Ring(NC, c_order, start_c)
    rw = Ring(NR, r_order, start_r)

    def kv_copies(seq, slot):
        return (pltpu.make_async_copy(k_cache.at[seq], kvbuf.at[slot, 0], kvsem.at[slot, 0]),
                pltpu.make_async_copy(v_cache.at[seq], kvbuf.at[slot, 1], kvsem.at[slot, 1]))

    def await_bytes(ref, sem):
        pltpu.make_async_copy(ref, ref, sem).wait()

    def rows_of(dev, p=None):
        if p is None:
            return pl.ds(pl.multiple_of(SHARD * dev, SHARD), SHARD)
        return pl.ds(pl.multiple_of(SHARD * dev + PIECE * p, PIECE), PIECE)

    def ag(h, what, r, part=None):
        origin = {'x': me, 'y': me, 'so': me, 'dy': xn, 'dx': yn, 'sx': xn, 'sy': yn, 'sd': dg}[what]
        target = sib if what[0] == 's' else xn if what[-1] == 'x' else yn
        sem = 6 if part is None else 4 + r if what[0] == 'd' else 2 * r + (part if what == 'x' else 1 - part)
        ref = nbuf.at[h, rows_of(origin, r), :] if part is None else nbuf.at[h, rows_of(origin, r), pl.ds(part * D // 2, D // 2)]
        pltpu.make_async_remote_copy(src_ref=ref, dst_ref=ref, send_sem=ag_s.at[h], recv_sem=ag_r.at[h, sem],
                                     device_id={'tp': target}, device_id_type=pl.DeviceIdType.MESH).start()

    def ag_own(h, r):
        ag(h, 'x', r, 0)
        ag(h, 'y', r, 1)
        ag(h, 'x', r, 1)
        ag(h, 'y', r, 0)
        ag(h, 'so', r)

    def ag_step(h, i, r):
        sem = (2 * r, 2 * r + 1, 4 + r, 6)[i - 1]
        await_bytes(nbuf.at[h, pl.ds(0, 8 * PIECE if i == 4 else PIECE), :], ag_r.at[h, sem])
        if i == 1:
            ag(h, 'dy', r, 0)
            ag(h, 'dx', r, 1)
        elif i == 2:
            ag(h, 'sx', r)
            ag(h, 'sy', r)
        elif i == 3:
            ag(h, 'sd', r)
        else:
            await_bytes(nbuf.at[h, pl.ds(0, ROWS - SHARD), :], ag_s.at[h])

    chip_rows = (me, xn, yn, dg)
    other_rows = (sib, xn + 1 - 2 * core, yn + 1 - 2 * core, dg + 1 - 2 * core)

    def remote(h, src, dst, sem, target):
        pltpu.make_async_remote_copy(src_ref=src, dst_ref=dst, send_sem=rs_s.at[h], recv_sem=rs_r.at[h, sem],
                                     device_id={'tp': target}, device_id_type=pl.DeviceIdType.MESH).start()

    def half_blks(c):
        return pl.ds(c * HALF_BLK, HALF_BLK)

    def rs(h, what, r, c):
        cb = half_blks(c)
        if what == 'd':
            remote(h, tbuf.at[h, 2, r, cb], dgr.at[h, r, cb], 2 + r, yn if c else xn)
        else:
            to = 0 if what == 'x' else 1
            remote(h, tbuf.at[h, to, r, cb], xyr.at[h, to, r, cb], 4 + r, yn if to else xn)

    def rs0(h, c):
        cb = half_blks(c)
        for p in (3, 1, 2, 0):
            remote(h, part.at[h, cb, rows_of(other_rows[p]), :], sibr.at[h, p, cb], 6 + c if p == 3 else c, sib)

    def rs1(h, c):
        cb = half_blks(c)

        def add_up(kinds):
            def body(i, _):
                j = c * HALF_BLK + i
                for p in kinds:
                    v = part[h, j, rows_of(chip_rows[p]), :].astype(F32) + sibr[h, p, j].astype(F32)
                    if p == 0:
                        town[h, j] = v
                    else:
                        v = v.astype(BF16)
                        tbuf[h, p - 1, 0, j] = v[:PIECE]
                        tbuf[h, p - 1, 1, j] = v[PIECE:]

            loop(HALF_BLK, body)

        await_bytes(sibr.at[h, 3, cb], rs_r.at[h, 6 + c])
        add_up((3,))
        if c == 1:
            rs(h, 'd', 0, 0)
            rs(h, 'd', 0, 1)
        await_bytes(sibr.at[h, pl.ds(0, 3), cb], rs_r.at[h, c])
        add_up((1, 2, 0))
        if c == 1:
            rs(h, 'x', 0, 0)
            rs(h, 'y', 0, 1)
            rs(h, 'd', 1, 0)
            rs(h, 'd', 1, 1)

    def rs2(h, r):
        await_bytes(dgr.at[h, r], rs_r.at[h, 2 + r])

        def body(i, _):
            for to, j in ((1, i), (0, HALF_BLK + i)):
                tbuf[h, to, r, j] = (tbuf[h, to, r, j].astype(F32) + dgr[h, r, j].astype(F32)).astype(BF16)

        loop(HALF_BLK, body)
        rs(h, 'x', r, 1)
        rs(h, 'y', r, 0)
        if r == 0:
            rs(h, 'x', 1, 0)
            rs(h, 'y', 1, 1)

    def blk(j):
        return pl.ds(pl.multiple_of(j * COLS, COLS), COLS)

    def normalise(h, k, r, square_sum):
        inv = lax.rsqrt(row_sum(square_sum) * (1.0 / D) + 1e-6)

        def body(j, _):
            nbuf[h, rows_of(me, r), blk(j)] = (xres[h, r, j].astype(F32) * inv * gain[k:k + 1, blk(j)]).astype(BF16)

        loop(NBLK, body)
        ag_own(h, r)

    def first(h):
        for r in range(2):
            def body(j, acc):
                row = h * SHARD + r * PIECE
                v = x_ref[row:row + PIECE, blk(j)]
                xres[h, r, j] = v
                v = v.astype(F32)
                return acc + v * v

            normalise(h, 0, r, sum_blocks(body))

    def rs3(h, k, r):
        await_bytes(xyr.at[h, :, r], rs_r.at[h, 4 + r])
        last = k == len(SUBLAYERS) - 1
        here = slice(r * PIECE, (r + 1) * PIECE)

        def body(j, acc):
            got = xyr[h, 0, r, j].astype(F32) + xyr[h, 1, r, j].astype(F32)
            v = xres[h, r, j].astype(F32) + (town[h, j, here] + got) + bias[k:k + 1, blk(j)]
            v = v.astype(BF16)
            if last:
                row = h * SHARD + r * PIECE
                xo_ref[row:row + PIECE, blk(j)] = v
                return acc
            xres[h, r, j] = v
            v = v.astype(F32)
            return acc + v * v

        square_sum = sum_blocks(body)
        if r == 1:
            await_bytes(part.at[h, :, pl.ds(0, ROWS - SHARD), :], rs_s.at[h])
        if not last:
            normalise(h, k + 1, r, square_sum)

    def setup():
        for k, (ref, l) in enumerate(((bout_ref, 0), (bd_ref, 0), (bout_ref, 1), (bd_ref, 1), (bo_ref, None), (bd_ref, 2))):
            v = ref[...].astype(F32)
            bias[k:k + 1, :] = v.reshape(1, D) if l is None else v[l:l + 1]
        rows = [(by_ref[...], 1), (bx_ref[...], 1)] + [(cw_ref[:, i], 1) for i in range(4)]
        rows += [(cb_ref[...], 1), (ba_ref[...], 1), (bi_ref[...], 1), (jax.nn.softplus(ap_ref[...]), -8.0)]
        for r, (v, scale) in enumerate(rows):
            v = v.astype(F32) * scale
            for l in range(LAYERS):
                for t in range(2):
                    rvec[l, t, r:r + 1, :] = v[l:l + 1, t * WID:(t + 1) * WID]
        for r, ref in enumerate((b1_ref, b2_ref)):
            v = ref[...].astype(F32)
            for m in range(3):
                for t in range(6):
                    mvec[m, t, r:r + 1, :] = v[m:m + 1, t * WID:(t + 1) * WID]
        conv0[...] = jnp.zeros_like(conv0)
        for l in range(LAYERS):
            for i in range(3):
                v = conv_ref[l, i].astype(F32)
                for q in range(SEQS):
                    conv0[l, q, 5 + i:6 + i, :] = v[q:q + 1]
        p = pos_ref[...]
        cols = jnp.concatenate([p, p], axis=1).T
        for q in range(SEQS):
            col = cols[:, q:q + 1]
            poscol[q] = col[:TOKENS]
            posrow[q // HALF_SEQ, :, q % HALF_SEQ] = col[:TOKENS].reshape(8, TOK, 1)
        lane = lax.broadcasted_iota(jnp.int32, (1, ROPE_DIM), 1)
        for h in range(HALVES):
            angle = posrow[h].reshape(ROWS, 1).astype(F32) / scale_ref[...]
            costab[h] = jnp.cos(angle)
            sine = jnp.sin(angle)
            sintab[h] = jnp.where(lane < ROPE_DIM // 2, -sine, sine)

    def dot(a, b):
        return jnp.dot(a, b, preferred_element_type=F32)

    def store_part(h, j, v):
        part[h, j] = v.astype(BF16)

    def out_small(h, ticks):
        base = rw.take(2)

        def body(i, _):
            slot = rw.slot(base, i)
            wait_r(slot, 4)
            for e in range(4):
                store_part(h, i * 4 + e, dot(hbuf[:, 0:512], rring[slot, e]))
            rw.refill(base, 2, i)
            run_ticks(i, ticks)

        loop(2, body)

    def comp_rec(h, l, ticks):
        base = cw.take(2)

        def body(t, _):
            slot = cw.slot(base, t)
            wait_c(slot)
            vec = rvec[l, t]
            lanes = pl.ds(pl.multiple_of(t * WID, WID), WID)

            def row(r):
                return vec[r:r + 1, :]

            n = nbuf[h]
            gate_y = jax.nn.gelu(dot(n, cring[slot, 0]) + row(0), approximate=True).astype(BF16).astype(F32)
            u = (dot(n, cring[slot, 1]) + row(1)).astype(BF16).astype(F32)
            cw.refill(base, 2, t)
            u3 = u.reshape(SHARD, TOK, WID)
            for q in range(HALF_SEQ):
                for i in range(3):
                    convf[l, i, h * HALF_SEQ + q:h * HALF_SEQ + q + 1, lanes] = u3[SHARD - HALF_SEQ + q, 5 + i:6 + i, :]
            before = jnp.concatenate([conv0[l, h * HALF_SEQ:(h + 1) * HALF_SEQ, :, lanes], u3[:SHARD - HALF_SEQ]], axis=0)
            jj = lax.broadcasted_iota(jnp.int32, (SHARD, TOK, WID), 1)
            conv = u3 * row(5)
            for back in (1, 2, 3):
                shifted = jnp.where(jj >= back, pltpu.roll(u3, back, 1), pltpu.roll(before, back, 1))
                conv = conv + shifted * row(5 - back)
            conv = (conv + row(6)).reshape(ROWS, WID).astype(BF16)
            gate_r = jax.nn.sigmoid(dot(conv, wa_ref[l, t]) + row(7))
            gate_i = jax.nn.sigmoid(dot(conv, wi_ref[l, t]) + row(8))
            decay = jnp.exp(gate_r * row(9))
            fresh = posrow[h].reshape(ROWS, 1) == 0
            mult = jnp.where(fresh, 1.0, jnp.sqrt(1.0 - decay * decay))
            decay = jnp.where(fresh, 0.0, decay)
            drive = conv.astype(F32) * gate_i * mult
            a3 = decay.reshape(SHARD, TOK, WID)
            b3 = drive.reshape(SHARD, TOK, WID)
            for back in (1, 2, 4):
                b3 = b3 + a3 * jnp.where(jj >= back, pltpu.roll(b3, back, 1), 0.0)
                a3 = a3 * jnp.where(jj >= back, pltpu.roll(a3, back, 1), 1.0)
            held = lru_ref[l, :, lanes]
            carry = jnp.concatenate([held[q:q + 1].reshape(1, 1, WID) for q in range(h * HALF_SEQ, (h + 1) * HALF_SEQ)], axis=0)
            out = []
            for d in range(8):
                here = slice(d * HALF_SEQ, (d + 1) * HALF_SEQ)
                hs = b3[here] + a3[here] * carry
                carry = hs[:, TOK - 1:TOK, :]
                out.append(hs)
            for q in range(HALF_SEQ):
                lruo_ref[l, h * HALF_SEQ + q:h * HALF_SEQ + q + 1, lanes] = carry[q]
            hs = jnp.concatenate(out, axis=0).reshape(ROWS, WID)
            hbuf[:, lanes] = (hs * gate_y).astype(BF16)
            run_ticks(t, ticks)

        loop(2, body)
        out_small(h, later(ticks, 2))

    def comp_mlp(h, m, ticks):
        base = cw.take(6)

        def body(t, _):
            slot = cw.slot(base, t)
            wait_c(slot)
            n = nbuf[h]
            gate = jax.nn.gelu(dot(n, cring[slot, 0]) + mvec[m, t, 0:1, :], approximate=True)
            up = dot(n, cring[slot, 1]) + mvec[m, t, 1:2, :]
            hbuf[:, pl.ds(pl.multiple_of(t * WID, WID), WID)] = (gate * up).astype(BF16)
            cw.refill(base, 6, t)
            run_ticks(t, ticks)

        loop(6, body)
        base_r = rw.take(8)

        def body_r(i, _):
            for e in range(2):
                wait_r(rw.slot(base_r, 2 * i + e), 3)
            for e in range(2):
                slot = rw.slot(base_r, 2 * i + e)
                store_part(h, 2 * i + e, dot(hbuf[:, 0:512], rring[slot, 0]) + dot(hbuf[:, 512:1024], rring[slot, 1])
                           + dot(hbuf[:, 1024:1536], rring[slot, 2]))
            for e in range(2):
                rw.refill(base_r, 8, 2 * i + e)
            run_ticks(i, later(ticks, 6))

        loop(4, body_r)

    def comp_att(h, l, ticks):
        for c in kv_copies(h * HALF_SEQ, 0):
            c.start()
        cos, sin = costab[h], sintab[h]

        def rope(v):
            r = v[:, :ROPE_DIM]
            return jnp.concatenate([r * cos + pltpu.roll(r, ROPE_DIM // 2, 1) * sin, v[:, ROPE_DIM:]], axis=1)

        def by_seq(v):
            v = v.reshape(8, HALF_SEQ, TOK, WID)
            return [v[:, s].reshape(TOKENS, WID).astype(BF16) for s in range(HALF_SEQ)]

        n = nbuf[h]
        base = cw.take(1)
        slot = cw.slot(base, 0)
        wait_c(slot)
        for e in range(2):
            for s, v in enumerate(by_seq(rope(dot(n, cring[slot, e])) * 0.0625)):
                qbuf[s, e * TOKENS:(e + 1) * TOKENS, :] = v
        cw.refill(base, 1, 0)
        run_ticks(0, ticks)
        base = cw.take(1)
        slot = cw.slot(base, 0)
        wait_c(slot)
        for s, v in enumerate(by_seq(rope(dot(n, cring[slot, 0])))):
            ko_ref[h * HALF_SEQ + s] = v
        for s, v in enumerate(by_seq(dot(n, cring[slot, 1]))):
            vo_ref[h * HALF_SEQ + s] = v
        cw.refill(base, 1, 0)
        run_ticks(0, later(ticks, 1))

        def body(s, _):
            seq = h * HALF_SEQ + s
            slot = lax.rem(s, 2)
            for c in kv_copies(seq, slot):
                c.wait()

            @pl.when(s + 1 < HALF_SEQ)
            def _():
                for c in kv_copies(seq + 1, 1 - slot):
                    c.start()

            q = qbuf[s]
            trans = (((1,), (1,)), ((), ()))
            s_old = lax.dot_general(q, kvbuf[slot, 0], trans, preferred_element_type=F32)
            s_new = lax.dot_general(q, ko_ref[seq], trans, preferred_element_type=F32)
            held = slot_ref[pl.ds(seq, 1), :]
            held = jnp.where(held >= 0, held, BIG)
            pos = poscol[seq]
            index = lax.broadcasted_iota(jnp.int32, (TOKENS, 1), 0)
            last = jnp.where(pos > index, pos, -1)
            seen = (held <= last) & (held > pos - WINDOW)
            s_old = jnp.where(seen[None], s_old.reshape(2, TOKENS, WINDOW), NEG).reshape(128, WINDOW)
            other = lax.broadcasted_iota(jnp.int32, (TOKENS, TOKENS), 1)
            seen = (other <= index) & (other >= index - pos)
            s_new = jnp.where(seen[None], s_new.reshape(2, TOKENS, TOKENS), NEG).reshape(128, TOKENS)
            top = jnp.maximum(row_max(s_old), row_max(s_new))
            e_old = jnp.exp(s_old - top)
            e_new = jnp.exp(s_new - top)
            inv = 1.0 / (row_sum(e_old) + row_sum(e_new))
            o = dot((e_old * inv).astype(BF16), kvbuf[slot, 1]) + dot((e_new * inv).astype(BF16), vo_ref[seq])
            o = o.reshape(2, 8, TOK, WID)
            obuf[:, s, :, 0:WID] = o[0]
            obuf[:, s, :, WID:512] = o[1]
            run_ticks(s, later(ticks, 2))

        loop(HALF_SEQ, body)
        hbuf[:, 0:512] = obuf[...].reshape(ROWS, 512).astype(BF16)
        out_small(h, later(ticks, 6))

    comp = {REC: comp_rec, MLP: comp_mlp, ATT: comp_att}

    cw.prime()
    rw.prime()
    barrier = pltpu.get_barrier_semaphore()
    for other in (sib, xn, yn):
        pl.semaphore_signal(barrier, inc=1, device_id={'tp': other}, device_id_type=pl.DeviceIdType.MESH)
    pl.semaphore_wait(barrier, 3)

    gain[...] = 1.0 + norm_ref[...].astype(F32)
    first(0)
    setup()

    def act(name):
        kind, i, c, h, k = name
        if kind == 'start':
            first(h)
        elif kind == 'ag':
            ag_step(h, i, c)
        elif i == 3:
            rs3(h, k, c)
        else:
            (rs0, rs1, rs2)[i](h, c)

    def act_all(names):
        for name in names:
            act(name)

    after, unit = {-1: []}, -1
    for event in plan():
        if event is None:
            unit += 1
            after[unit] = []
        else:
            after[unit].append(event)
    act_all(after[-1])
    base = 0
    for k, (kind, l) in enumerate(SUBLAYERS):
        for h in range(HALVES):
            last = base + UNITS[kind] - 1
            ticks = {u - base: (lambda names=after[u]: act_all(names)) for u in range(base, last) if after[u]}
            comp[kind](h, l, ticks)
            act_all(after[last])
            base = last + 1
    convo_ref[...] = convf[...].astype(BF16)


def finish(pos_s, pos_ref, slot_ref, k_cache, v_cache, kn_ref, vn_ref, x_ref, conv_ref, lru_ref,
           ko, vo, so_ref, xo_ref, convo_ref, lruo_ref, buf, xbuf, cbuf, lbuf, in_sem, out_sem, small_in, small_out):
    pairs = [(e, q) for q in range(SEQS) for e in range(2)]

    def copy_in(e, q):
        return pltpu.make_async_copy((k_cache, v_cache)[e].at[q], buf.at[e, q], in_sem.at[e, q])

    def copy_out(e, q):
        return pltpu.make_async_copy(buf.at[e, q], (ko, vo)[e].at[q], out_sem.at[e, q])

    for e, q in pairs:
        copy_in(e, q).start()
    small = ((x_ref, xbuf, xo_ref), (conv_ref, cbuf, convo_ref), (lru_ref, lbuf, lruo_ref))
    for i, (src, mid, _) in enumerate(small):
        pltpu.make_async_copy(src, mid, small_in.at[i]).start()
    begin, last = pos_ref[:, 0:1], pos_ref[:, 63:TOKENS]
    count = jnp.where(last < 63, 63 - last, TOKENS)
    slot = lax.broadcasted_iota(jnp.int32, (SEQS, WINDOW), 1)
    ahead = (slot - begin) & (WINDOW - 1)
    so_ref[...] = jnp.where(ahead < count, begin + ahead, jnp.where(slot < TOKENS - count, slot, slot_ref[...]))
    for i, (src, mid, dst) in enumerate(small):
        pltpu.make_async_copy(src, mid, small_in.at[i]).wait()
        pltpu.make_async_copy(mid, dst, small_out.at[i]).start()
    for q in range(SEQS):
        first_row = pl.multiple_of(jnp.minimum((pos_s[q, 0] & (WINDOW - 1)) // PIECE * PIECE, WINDOW - SPAN), PIECE)
        new_slots = pos_ref[q:q + 1, :] & (WINDOW - 1)
        for e in range(2):
            copy_in(e, q).wait()
        for start in (first_row, 0):
            rows = pl.ds(start, SPAN)
            hit = lax.broadcasted_iota(jnp.int32, (SPAN, TOKENS), 0) + start == new_slots
            any_hit = row_sum(hit.astype(F32)) > 0.5
            for e, ref in enumerate((kn_ref, vn_ref)):
                put = jnp.dot(hit.astype(BF16), ref[q], preferred_element_type=F32)
                buf[e, q, rows, :] = jnp.where(any_hit, put, buf[e, q, rows, :].astype(F32)).astype(BF16)
        for e in range(2):
            copy_out(e, q).start()
    for e, q in pairs:
        copy_out(e, q).wait()
    for i, (_, mid, dst) in enumerate(small):
        pltpu.make_async_copy(mid, dst, small_out.at[i]).wait()


def solution(mesh):
    def device_body(x_in, seg_pos, conv_state, lru_state, k_cache, v_cache, slot_pos, norm_scale, w_x, b_x, w_y, b_y, conv_w, conv_b, w_a, b_a, w_i, b_i, a_param, w_out, b_out, w_q, w_k, w_v, w_o, b_o, w_1, b_1, w_2, b_2, w_d, b_d):
        half_dim = ROPE_DIM // 2
        timescale = 10000.0 ** (2.0 * (jnp.arange(ROPE_DIM) % half_dim).astype(F32) / ROPE_DIM)

        vmem = pl.BlockSpec(memory_space=pltpu.VMEM)
        hbm = pl.BlockSpec(memory_space=pl.ANY)
        sds = jax.ShapeDtypeStruct
        fresh = sds((SEQS, TOKENS, WID), BF16)
        x_out, conv_out, lru_out, k_new, v_new = pl.pallas_call(
            mega,
            out_shape=(sds((TOKENS, D), BF16), sds((LAYERS, 3, SEQS, 512), BF16), sds((LAYERS, SEQS, 512), F32), fresh, fresh),
            in_specs=[vmem] * 21 + [hbm] * 12,
            out_specs=[vmem] * 5,
            scratch_shapes=[
                pltpu.VMEM((HALVES, ROWS, D), BF16),
                pltpu.VMEM((HALVES, NBLK, ROWS, COLS), BF16),
                pltpu.VMEM((HALVES, 4, NBLK, SHARD, COLS), BF16),
                pltpu.VMEM((HALVES, NBLK, SHARD, COLS), F32),
                pltpu.VMEM((HALVES, 3, 2, NBLK, PIECE, COLS), BF16),
                pltpu.VMEM((HALVES, 2, NBLK, PIECE, COLS), BF16),
                pltpu.VMEM((HALVES, 2, 2, NBLK, PIECE, COLS), BF16),
                pltpu.VMEM((HALVES, 2, NBLK, PIECE, COLS), BF16),
                pltpu.VMEM((ROWS, 1536), BF16),
                pltpu.VMEM((HALF_SEQ, 128, WID), BF16),
                pltpu.VMEM((8, HALF_SEQ, TOK, 512), F32),
                pltpu.VMEM((HALVES, 2, WINDOW, WID), BF16),
                pltpu.VMEM((NC, 2, D, WID), BF16),
                pltpu.VMEM((NR, 4, 512, COLS), BF16),
                pltpu.VMEM((6, D), F32),
                pltpu.VMEM((6, D), F32),
                pltpu.VMEM((LAYERS, 2, 16, WID), F32),
                pltpu.VMEM((3, 6, 8, WID), F32),
                pltpu.VMEM((LAYERS, SEQS, TOK, 512), F32),
                pltpu.VMEM((LAYERS, 3, SEQS, 512), F32),
                pltpu.VMEM((SEQS, TOKENS, 1), jnp.int32),
                pltpu.VMEM((HALVES, 8, HALF_SEQ, TOK, 1), jnp.int32),
                pltpu.VMEM((HALVES, ROWS, ROPE_DIM), F32),
                pltpu.VMEM((HALVES, ROWS, ROPE_DIM), F32),
                pltpu.SemaphoreType.DMA((HALVES,)),
                pltpu.SemaphoreType.DMA((HALVES, 7)),
                pltpu.SemaphoreType.DMA((HALVES,)),
                pltpu.SemaphoreType.DMA((HALVES, 8)),
                pltpu.SemaphoreType.DMA((NC, 2)),
                pltpu.SemaphoreType.DMA((NR, 4)),
                pltpu.SemaphoreType.DMA((HALVES, 2)),
            ],
            compiler_params=pltpu.CompilerParams(collective_id=0, has_side_effects=True, vmem_limit_bytes=67043328),
            name='layers',
        )(x_in.reshape(TOKENS, D), norm_scale, b_out, b_o, b_d, b_y, b_x, conv_w, conv_b, b_a, b_i, a_param, b_1, b_2,
          conv_state.swapaxes(1, 2), lru_state, w_a, w_i, seg_pos, slot_pos, timescale[None],
          w_y, w_x, w_out, w_1, w_2, w_d, w_q, w_k, w_v, w_o, k_cache, v_cache)

        k_out, v_out, slot_out, x_out, conv_out, lru_out = pl.pallas_call(
            finish,
            out_shape=[sds(v.shape, v.dtype) for v in (k_cache, v_cache, slot_pos, x_out, conv_out, lru_out)],
            in_specs=[pl.BlockSpec(memory_space=pltpu.SMEM), vmem, vmem, hbm, hbm, vmem, vmem] + [hbm] * 3,
            out_specs=[hbm, hbm, vmem] + [hbm] * 3,
            scratch_shapes=[pltpu.VMEM((2, SEQS, WINDOW, WID), BF16)] + [pltpu.VMEM(v.shape, v.dtype) for v in (x_out, conv_out, lru_out)]
            + [pltpu.SemaphoreType.DMA((2, SEQS))] * 2 + [pltpu.SemaphoreType.DMA((3,))] * 2,
            name='caches',
        )(seg_pos, seg_pos, slot_pos, k_cache, v_cache, k_new, v_new, x_out, conv_out, lru_out)
        return x_out.reshape(SEQS, TOK, D), conv_out.swapaxes(1, 2), lru_out, k_out, v_out, slot_out

    col_spec = P(None, None, 'tp')
    vec_spec = P(None, 'tp')
    row_spec = vec_spec
    x_spec, seq_spec, conv_spec, lru_spec = P('dp', 'tp'), P('dp'), P(None, 'dp', None, 'tp'), P(None, 'dp', 'tp')
    arg_specs = (x_spec, seq_spec, conv_spec, lru_spec, seq_spec, seq_spec, seq_spec, P(), col_spec, vec_spec, col_spec, vec_spec, col_spec, vec_spec, row_spec, vec_spec, row_spec, vec_spec, vec_spec, row_spec, P(), vec_spec, P(), P(), P('tp'), P(), col_spec, vec_spec, col_spec, vec_spec, row_spec, P())
    result_specs = (x_spec, conv_spec, lru_spec, seq_spec, seq_spec, seq_spec)
    return jax.shard_map(device_body, mesh=mesh, in_specs=arg_specs, out_specs=result_specs, check_vma=False)
```

```python
import jax
import jax.numpy as jnp
from jax import lax
from jax.experimental import pallas as pl
from jax.experimental.pallas import tpu as pltpu
from jax.sharding import PartitionSpec as P

F32 = jnp.float32
BF16 = jnp.bfloat16
WINDOW = 2048
ROPE_DIM = 128
D = 4096
HALF_SEQ = 4
TOK = 8
SHARD = 32
ROWS = 256
COLS = 512
NBLK = D // COLS
PIECE = 16
NC = 4
NR = 4
WID = 256
HALVES = LAYERS = 2
SEQS = 8
TOKENS = 64
BIG = 1 << 30
SPAN = 96
NEG = -1e30

REC, MLP, ATT = 'rec', 'mlp', 'att'
SUBLAYERS = ((REC, 0), (MLP, 0), (REC, 1), (MLP, 1), (ATT, 0), (MLP, 2))

UNITS = {REC: 4, MLP: 10, ATT: 8}
STEPS = (('ag', 1, 0), ('ag', 2, 0), ('ag', 1, 1), ('ag', 2, 1), ('ag', 3, 0), ('ag', 3, 1), ('ag', 4, 0),
         ('rs', 0, 0), ('rs', 1, 0), ('rs', 0, 1), ('rs', 1, 1), ('rs', 2, 0), ('rs', 2, 1), ('rs', 3, 0), ('rs', 3, 1))
HALF_BLK = NBLK // 2

PLAN = (
    'aaaaabaa...abb.bbaababba.aa.a.abba.babaaaab..b.b..b..b.a',
    'b.b.aabbabb.a..a.a..a.a.b.a.abbbaaaab.bb.bb.a.baabbabbab',
    '.aa.a.ba.abababaaab..b.b..b.b..a.bb.aabbabb.a..a.a..a..b',
    'a.a.abbabaaab...bb..b..abb.baaabbbba...aa..a..b.aaabbbaa',
    'aab..b.b..b..b.abb.b.ababab....a....ba..bbbbababb',
)


def plan():
    def chain(h):
        if h:
            yield 'start', 0, 0, h, 0
        for k in range(len(SUBLAYERS)):
            for step in STEPS:
                yield *step, h, k

    ahead = {'a': chain(0), 'b': chain(1)}
    return [next(ahead[c]) if c in ahead else None for c in ''.join(PLAN)]


class Ring:
    def __init__(self, depth, order, start):
        self.depth, self.start, self.at = depth, start, 0
        self.total = sum(n for _, n in order)
        self.runs = []
        g = 0
        for what, n in order:
            self.runs.append((what, g, n))
            g += n

    def prime(self):
        for what, g0, n in self.runs:
            for t in range(n):
                if g0 + t < self.depth:
                    self.start(what, t, g0 + t)

    def take(self, n):
        base = self.at
        self.at += n
        return base

    def slot(self, base, i):
        return (base + i) % self.depth

    def refill(self, base, n, i):
        ahead = base + self.depth
        slot = self.slot(base, i)
        for what, g0, m in self.runs:
            lo, hi = max(g0, ahead), min(g0 + m, ahead + n)
            if lo < hi:
                if isinstance(i, int):
                    if lo - ahead <= i < hi - ahead:
                        self.start(what, ahead - g0 + i, slot)
                else:
                    @pl.when((i >= lo - ahead) & (i < hi - ahead))
                    def _():
                        self.start(what, ahead - g0 + i, slot)


def loop(n, body):
    def step(i, carry):
        body(i, None)
        return carry

    lax.fori_loop(0, n, step, 0)


def sum_blocks(body):
    return lax.fori_loop(0, NBLK, body, jnp.zeros((PIECE, COLS), F32))


def row_sum(v):
    return jnp.sum(v, axis=-1, keepdims=True)


def row_max(v):
    return jnp.max(v, axis=-1, keepdims=True)


def run_ticks(i, ticks):
    for when, fn in ticks.items():
        if isinstance(i, int):
            if i == when:
                fn()
        else:
            pl.when(i == when)(fn)


def later(ticks, n):
    return {i - n: fn for i, fn in ticks.items()}


def mega(x_ref, norm_ref, bout_ref, bo_ref, bd_ref, by_ref, bx_ref, cw_ref, cb_ref, ba_ref, bi_ref, ap_ref, b1_ref, b2_ref,
         conv_ref, lru_ref, wa_ref, wi_ref, pos_ref, slot_ref, scale_ref,
         w_y, w_x, w_out, w_1, w_2, w_d, w_q, w_k, w_v, w_o, k_cache, v_cache,
         xo_ref, convo_ref, lruo_ref, ko_ref, vo_ref,
         nbuf, part, sibr, town, tbuf, dgr, xyr, xres, hbuf, qbuf, obuf, kvbuf, cring, rring,
         gain, bias, rvec, mvec, conv0, convf, poscol, posrow, costab, sintab,
         ag_s, ag_r, rs_s, rs_r, csem, rsem, kvsem):
    me = lax.axis_index('tp')
    core = lax.rem(me, 2)
    xpos = lax.rem(me // 2, 2)
    ypos = me // 4
    sib = me + 1 - 2 * core
    xn = me + 2 - 4 * xpos
    yn = me + 4 - 8 * ypos
    dg = xn + 4 - 8 * ypos

    def start_c(what, t, slot):
        kind, l = what
        cols = pl.ds(t * WID if isinstance(t, int) else pl.multiple_of(t * WID, WID), WID)
        if kind == REC:
            srcs = w_y.at[l, :, cols], w_x.at[l, :, cols]
        elif kind == MLP:
            srcs = w_1.at[l, :, cols], w_2.at[l, :, cols]
        elif kind == 'q':
            srcs = w_q.at[:, pl.ds(0, WID)], w_q.at[:, pl.ds(WID, WID)]
        else:
            srcs = w_k, w_v
        for e, src in enumerate(srcs):
            pltpu.make_async_copy(src, cring.at[slot, e], csem.at[slot, e]).start()

    def wait_c(slot):
        for e, src in enumerate((w_k, w_v)):
            pltpu.make_async_copy(src, cring.at[slot, e], csem.at[slot, e]).wait()

    def start_r(what, t, slot):
        kind, l = what
        if kind == MLP:
            cols = pl.ds(t * COLS if isinstance(t, int) else pl.multiple_of(t * COLS, COLS), COLS)
            for e in range(3):
                pltpu.make_async_copy(w_d.at[l, pl.ds(e * 512, 512), cols], rring.at[slot, e], rsem.at[slot, e]).start()
        else:
            for e in range(4):
                c0 = t * 4 * COLS + e * COLS
                cols = pl.ds(c0 if isinstance(t, int) else pl.multiple_of(c0, COLS), COLS)
                src = w_out.at[l, :, cols] if kind == REC else w_o.at[:, cols]
                pltpu.make_async_copy(src, rring.at[slot, e], rsem.at[slot, e]).start()

    def wait_r(slot, n):
        for e in range(n):
            pltpu.make_async_copy(w_o.at[:, pl.ds(0, COLS)], rring.at[slot, e], rsem.at[slot, e]).wait()

    c_order, r_order = [], []
    for kind, l in SUBLAYERS:
        for _ in range(2):
            if kind == REC:
                c_order.append(((REC, l), 2))
                r_order.append(((REC, l), 2))
            elif kind == MLP:
                c_order.append(((MLP, l), 6))
                r_order.append(((MLP, l), 8))
            else:
                c_order += [(('q', 0), 1), (('kv', 0), 1)]
                r_order.append(((ATT, 0), 2))
    cw = Ring(NC, c_order, start_c)
    rw = Ring(NR, r_order, start_r)

    def kv_copies(seq, slot):
        return (pltpu.make_async_copy(k_cache.at[seq], kvbuf.at[slot, 0], kvsem.at[slot, 0]),
                pltpu.make_async_copy(v_cache.at[seq], kvbuf.at[slot, 1], kvsem.at[slot, 1]))

    def await_bytes(ref, sem):
        pltpu.make_async_copy(ref, ref, sem).wait()

    def rows_of(dev, p=None):
        if p is None:
            return pl.ds(pl.multiple_of(SHARD * dev, SHARD), SHARD)
        return pl.ds(pl.multiple_of(SHARD * dev + PIECE * p, PIECE), PIECE)

    def ag(h, what, r, part=None):
        origin = {'x': me, 'y': me, 'so': me, 'dy': xn, 'dx': yn, 'sx': xn, 'sy': yn, 'sd': dg}[what]
        target = sib if what[0] == 's' else xn if what[-1] == 'x' else yn
        sem = 6 if part is None else 4 + r if what[0] == 'd' else 2 * r + (part if what == 'x' else 1 - part)
        ref = nbuf.at[h, rows_of(origin, r), :] if part is None else nbuf.at[h, rows_of(origin, r), pl.ds(part * D // 2, D // 2)]
        pltpu.make_async_remote_copy(src_ref=ref, dst_ref=ref, send_sem=ag_s.at[h], recv_sem=ag_r.at[h, sem],
                                     device_id={'tp': target}, device_id_type=pl.DeviceIdType.MESH).start()

    def ag_own(h, r):
        ag(h, 'x', r, 0)
        ag(h, 'y', r, 1)
        ag(h, 'x', r, 1)
        ag(h, 'y', r, 0)
        ag(h, 'so', r)

    def ag_step(h, i, r):
        sem = (2 * r, 2 * r + 1, 4 + r, 6)[i - 1]
        await_bytes(nbuf.at[h, pl.ds(0, 8 * PIECE if i == 4 else PIECE), :], ag_r.at[h, sem])
        if i == 1:
            ag(h, 'dy', r, 0)
            ag(h, 'dx', r, 1)
        elif i == 2:
            ag(h, 'sx', r)
            ag(h, 'sy', r)
        elif i == 3:
            ag(h, 'sd', r)
        else:
            await_bytes(nbuf.at[h, pl.ds(0, ROWS - SHARD), :], ag_s.at[h])

    chip_rows = (me, xn, yn, dg)
    other_rows = (sib, xn + 1 - 2 * core, yn + 1 - 2 * core, dg + 1 - 2 * core)

    def remote(h, src, dst, sem, target):
        pltpu.make_async_remote_copy(src_ref=src, dst_ref=dst, send_sem=rs_s.at[h], recv_sem=rs_r.at[h, sem],
                                     device_id={'tp': target}, device_id_type=pl.DeviceIdType.MESH).start()

    def half_blks(c):
        return pl.ds(c * HALF_BLK, HALF_BLK)

    def rs(h, what, r, c):
        cb = half_blks(c)
        if what == 'd':
            remote(h, tbuf.at[h, 2, r, cb], dgr.at[h, r, cb], 2 + r, yn if c else xn)
        else:
            to = 0 if what == 'x' else 1
            remote(h, tbuf.at[h, to, r, cb], xyr.at[h, to, r, cb], 4 + r, yn if to else xn)

    def rs0(h, c):
        cb = half_blks(c)
        for p in (3, 1, 2, 0):
            remote(h, part.at[h, cb, rows_of(other_rows[p]), :], sibr.at[h, p, cb], 6 + c if p == 3 else c, sib)

    def rs1(h, c):
        cb = half_blks(c)

        def add_up(kinds):
            def body(i, _):
                j = c * HALF_BLK + i
                for p in kinds:
                    v = part[h, j, rows_of(chip_rows[p]), :].astype(F32) + sibr[h, p, j].astype(F32)
                    if p == 0:
                        town[h, j] = v
                    else:
                        v = v.astype(BF16)
                        tbuf[h, p - 1, 0, j] = v[:PIECE]
                        tbuf[h, p - 1, 1, j] = v[PIECE:]

            loop(HALF_BLK, body)

        await_bytes(sibr.at[h, 3, cb], rs_r.at[h, 6 + c])
        add_up((3,))
        if c == 1:
            rs(h, 'd', 0, 0)
            rs(h, 'd', 0, 1)
        await_bytes(sibr.at[h, pl.ds(0, 3), cb], rs_r.at[h, c])
        add_up((1, 2, 0))
        if c == 1:
            rs(h, 'x', 0, 0)
            rs(h, 'y', 0, 1)
            rs(h, 'd', 1, 0)
            rs(h, 'd', 1, 1)

    def rs2(h, r):
        await_bytes(dgr.at[h, r], rs_r.at[h, 2 + r])

        def body(i, _):
            for to, j in ((1, i), (0, HALF_BLK + i)):
                tbuf[h, to, r, j] = (tbuf[h, to, r, j].astype(F32) + dgr[h, r, j].astype(F32)).astype(BF16)

        loop(HALF_BLK, body)
        rs(h, 'x', r, 1)
        rs(h, 'y', r, 0)
        if r == 0:
            rs(h, 'x', 1, 0)
            rs(h, 'y', 1, 1)

    def blk(j):
        return pl.ds(pl.multiple_of(j * COLS, COLS), COLS)

    def normalise(h, k, r, square_sum):
        inv = lax.rsqrt(row_sum(square_sum) * (1.0 / D) + 1e-6)

        def body(j, _):
            nbuf[h, rows_of(me, r), blk(j)] = (xres[h, r, j].astype(F32) * inv * gain[k:k + 1, blk(j)]).astype(BF16)

        loop(NBLK, body)
        ag_own(h, r)

    def first(h):
        for r in range(2):
            def body(j, acc):
                row = h * SHARD + r * PIECE
                v = x_ref[row:row + PIECE, blk(j)]
                xres[h, r, j] = v
                v = v.astype(F32)
                return acc + v * v

            normalise(h, 0, r, sum_blocks(body))

    def rs3(h, k, r):
        await_bytes(xyr.at[h, :, r], rs_r.at[h, 4 + r])
        last = k == len(SUBLAYERS) - 1
        here = slice(r * PIECE, (r + 1) * PIECE)

        def body(j, acc):
            got = xyr[h, 0, r, j].astype(F32) + xyr[h, 1, r, j].astype(F32)
            v = xres[h, r, j].astype(F32) + (town[h, j, here] + got) + bias[k:k + 1, blk(j)]
            v = v.astype(BF16)
            if last:
                row = h * SHARD + r * PIECE
                xo_ref[row:row + PIECE, blk(j)] = v
                return acc
            xres[h, r, j] = v
            v = v.astype(F32)
            return acc + v * v

        square_sum = sum_blocks(body)
        if r == 1:
            await_bytes(part.at[h, :, pl.ds(0, ROWS - SHARD), :], rs_s.at[h])
        if not last:
            normalise(h, k + 1, r, square_sum)

    def setup():
        for k, (ref, l) in enumerate(((bout_ref, 0), (bd_ref, 0), (bout_ref, 1), (bd_ref, 1), (bo_ref, None), (bd_ref, 2))):
            v = ref[...].astype(F32)
            bias[k:k + 1, :] = v.reshape(1, D) if l is None else v[l:l + 1]
        rows = [(by_ref[...], 1), (bx_ref[...], 1)] + [(cw_ref[:, i], 1) for i in range(4)]
        rows += [(cb_ref[...], 1), (ba_ref[...], 1), (bi_ref[...], 1), (jax.nn.softplus(ap_ref[...]), -8.0)]
        for r, (v, scale) in enumerate(rows):
            v = v.astype(F32) * scale
            for l in range(LAYERS):
                for t in range(2):
                    rvec[l, t, r:r + 1, :] = v[l:l + 1, t * WID:(t + 1) * WID]
        for r, ref in enumerate((b1_ref, b2_ref)):
            v = ref[...].astype(F32)
            for m in range(3):
                for t in range(6):
                    mvec[m, t, r:r + 1, :] = v[m:m + 1, t * WID:(t + 1) * WID]
        conv0[...] = jnp.zeros_like(conv0)
        for l in range(LAYERS):
            for i in range(3):
                v = conv_ref[l, i].astype(F32)
                for q in range(SEQS):
                    conv0[l, q, 5 + i:6 + i, :] = v[q:q + 1]
        p = pos_ref[...]
        cols = jnp.concatenate([p, p], axis=1).T
        for q in range(SEQS):
            col = cols[:, q:q + 1]
            poscol[q] = col[:TOKENS]
            posrow[q // HALF_SEQ, :, q % HALF_SEQ] = col[:TOKENS].reshape(8, TOK, 1)
        lane = lax.broadcasted_iota(jnp.int32, (1, ROPE_DIM), 1)
        for h in range(HALVES):
            angle = posrow[h].reshape(ROWS, 1).astype(F32) / scale_ref[...]
            costab[h] = jnp.cos(angle)
            sine = jnp.sin(angle)
            sintab[h] = jnp.where(lane < ROPE_DIM // 2, -sine, sine)

    def dot(a, b):
        return jnp.dot(a, b, preferred_element_type=F32)

    def store_part(h, j, v):
        part[h, j] = v.astype(BF16)

    def out_small(h, ticks):
        base = rw.take(2)

        def body(i, _):
            slot = rw.slot(base, i)
            wait_r(slot, 4)
            for e in range(4):
                store_part(h, i * 4 + e, dot(hbuf[:, 0:512], rring[slot, e]))
            rw.refill(base, 2, i)
            run_ticks(i, ticks)

        loop(2, body)

    def comp_rec(h, l, ticks):
        base = cw.take(2)

        def body(t, _):
            slot = cw.slot(base, t)
            wait_c(slot)
            vec = rvec[l, t]
            lanes = pl.ds(pl.multiple_of(t * WID, WID), WID)

            def row(r):
                return vec[r:r + 1, :]

            n = nbuf[h]
            gate_y = jax.nn.gelu(dot(n, cring[slot, 0]) + row(0), approximate=True).astype(BF16).astype(F32)
            u = (dot(n, cring[slot, 1]) + row(1)).astype(BF16).astype(F32)
            cw.refill(base, 2, t)
            u3 = u.reshape(SHARD, TOK, WID)
            for q in range(HALF_SEQ):
                for i in range(3):
                    convf[l, i, h * HALF_SEQ + q:h * HALF_SEQ + q + 1, lanes] = u3[SHARD - HALF_SEQ + q, 5 + i:6 + i, :]
            before = jnp.concatenate([conv0[l, h * HALF_SEQ:(h + 1) * HALF_SEQ, :, lanes], u3[:SHARD - HALF_SEQ]], axis=0)
            jj = lax.broadcasted_iota(jnp.int32, (SHARD, TOK, WID), 1)
            conv = u3 * row(5)
            for back in (1, 2, 3):
                shifted = jnp.where(jj >= back, pltpu.roll(u3, back, 1), pltpu.roll(before, back, 1))
                conv = conv + shifted * row(5 - back)
            conv = (conv + row(6)).reshape(ROWS, WID).astype(BF16)
            gate_r = jax.nn.sigmoid(dot(conv, wa_ref[l, t]) + row(7))
            gate_i = jax.nn.sigmoid(dot(conv, wi_ref[l, t]) + row(8))
            decay = jnp.exp(gate_r * row(9))
            fresh = posrow[h].reshape(ROWS, 1) == 0
            mult = jnp.where(fresh, 1.0, jnp.sqrt(1.0 - decay * decay))
            decay = jnp.where(fresh, 0.0, decay)
            drive = conv.astype(F32) * gate_i * mult
            a3 = decay.reshape(SHARD, TOK, WID)
            b3 = drive.reshape(SHARD, TOK, WID)
            for back in (1, 2, 4):
                b3 = b3 + a3 * jnp.where(jj >= back, pltpu.roll(b3, back, 1), 0.0)
                a3 = a3 * jnp.where(jj >= back, pltpu.roll(a3, back, 1), 1.0)
            held = lru_ref[l, :, lanes]
            carry = jnp.concatenate([held[q:q + 1].reshape(1, 1, WID) for q in range(h * HALF_SEQ, (h + 1) * HALF_SEQ)], axis=0)
            out = []
            for d in range(8):
                here = slice(d * HALF_SEQ, (d + 1) * HALF_SEQ)
                hs = b3[here] + a3[here] * carry
                carry = hs[:, TOK - 1:TOK, :]
                out.append(hs)
            for q in range(HALF_SEQ):
                lruo_ref[l, h * HALF_SEQ + q:h * HALF_SEQ + q + 1, lanes] = carry[q]
            hs = jnp.concatenate(out, axis=0).reshape(ROWS, WID)
            hbuf[:, lanes] = (hs * gate_y).astype(BF16)
            run_ticks(t, ticks)

        loop(2, body)
        out_small(h, later(ticks, 2))

    def comp_mlp(h, m, ticks):
        base = cw.take(6)

        def body(t, _):
            slot = cw.slot(base, t)
            wait_c(slot)
            n = nbuf[h]
            gate = jax.nn.gelu(dot(n, cring[slot, 0]) + mvec[m, t, 0:1, :], approximate=True)
            up = dot(n, cring[slot, 1]) + mvec[m, t, 1:2, :]
            hbuf[:, pl.ds(pl.multiple_of(t * WID, WID), WID)] = (gate * up).astype(BF16)
            cw.refill(base, 6, t)
            run_ticks(t, ticks)

        loop(6, body)
        base_r = rw.take(8)

        def body_r(i, _):
            for e in range(2):
                wait_r(rw.slot(base_r, 2 * i + e), 3)
            for e in range(2):
                slot = rw.slot(base_r, 2 * i + e)
                store_part(h, 2 * i + e, dot(hbuf[:, 0:512], rring[slot, 0]) + dot(hbuf[:, 512:1024], rring[slot, 1])
                           + dot(hbuf[:, 1024:1536], rring[slot, 2]))
            for e in range(2):
                rw.refill(base_r, 8, 2 * i + e)
            run_ticks(i, later(ticks, 6))

        loop(4, body_r)

    def comp_att(h, l, ticks):
        for c in kv_copies(h * HALF_SEQ, 0):
            c.start()
        cos, sin = costab[h], sintab[h]

        def rope(v):
            r = v[:, :ROPE_DIM]
            return jnp.concatenate([r * cos + pltpu.roll(r, ROPE_DIM // 2, 1) * sin, v[:, ROPE_DIM:]], axis=1)

        def by_seq(v):
            v = v.reshape(8, HALF_SEQ, TOK, WID)
            return [v[:, s].reshape(TOKENS, WID).astype(BF16) for s in range(HALF_SEQ)]

        n = nbuf[h]
        base = cw.take(1)
        slot = cw.slot(base, 0)
        wait_c(slot)
        for e in range(2):
            for s, v in enumerate(by_seq(rope(dot(n, cring[slot, e])) * 0.0625)):
                qbuf[s, e * TOKENS:(e + 1) * TOKENS, :] = v
        cw.refill(base, 1, 0)
        run_ticks(0, ticks)
        base = cw.take(1)
        slot = cw.slot(base, 0)
        wait_c(slot)
        for s, v in enumerate(by_seq(rope(dot(n, cring[slot, 0])))):
            ko_ref[h * HALF_SEQ + s] = v
        for s, v in enumerate(by_seq(dot(n, cring[slot, 1]))):
            vo_ref[h * HALF_SEQ + s] = v
        cw.refill(base, 1, 0)
        run_ticks(0, later(ticks, 1))

        def body(s, _):
            seq = h * HALF_SEQ + s
            slot = lax.rem(s, 2)
            for c in kv_copies(seq, slot):
                c.wait()

            @pl.when(s + 1 < HALF_SEQ)
            def _():
                for c in kv_copies(seq + 1, 1 - slot):
                    c.start()

            q = qbuf[s]
            trans = (((1,), (1,)), ((), ()))
            s_old = lax.dot_general(q, kvbuf[slot, 0], trans, preferred_element_type=F32)
            s_new = lax.dot_general(q, ko_ref[seq], trans, preferred_element_type=F32)
            held = slot_ref[pl.ds(seq, 1), :]
            held = jnp.where(held >= 0, held, BIG)
            pos = poscol[seq]
            index = lax.broadcasted_iota(jnp.int32, (TOKENS, 1), 0)
            last = jnp.where(pos > index, pos, -1)
            seen = (held <= last) & (held > pos - WINDOW)
            s_old = jnp.where(seen[None], s_old.reshape(2, TOKENS, WINDOW), NEG).reshape(128, WINDOW)
            other = lax.broadcasted_iota(jnp.int32, (TOKENS, TOKENS), 1)
            seen = (other <= index) & (other >= index - pos)
            s_new = jnp.where(seen[None], s_new.reshape(2, TOKENS, TOKENS), NEG).reshape(128, TOKENS)
            top = jnp.maximum(row_max(s_old), row_max(s_new))
            e_old = jnp.exp(s_old - top)
            e_new = jnp.exp(s_new - top)
            inv = 1.0 / (row_sum(e_old) + row_sum(e_new))
            o = dot((e_old * inv).astype(BF16), kvbuf[slot, 1]) + dot((e_new * inv).astype(BF16), vo_ref[seq])
            o = o.reshape(2, 8, TOK, WID)
            obuf[:, s, :, 0:WID] = o[0]
            obuf[:, s, :, WID:512] = o[1]
            run_ticks(s, later(ticks, 2))

        loop(HALF_SEQ, body)
        hbuf[:, 0:512] = obuf[...].reshape(ROWS, 512).astype(BF16)
        out_small(h, later(ticks, 6))

    comp = {REC: comp_rec, MLP: comp_mlp, ATT: comp_att}

    cw.prime()
    rw.prime()
    barrier = pltpu.get_barrier_semaphore()
    for other in (sib, xn, yn):
        pl.semaphore_signal(barrier, inc=1, device_id={'tp': other}, device_id_type=pl.DeviceIdType.MESH)
    pl.semaphore_wait(barrier, 3)

    gain[...] = 1.0 + norm_ref[...].astype(F32)
    first(0)
    setup()

    def act(name):
        kind, i, c, h, k = name
        if kind == 'start':
            first(h)
        elif kind == 'ag':
            ag_step(h, i, c)
        elif i == 3:
            rs3(h, k, c)
        else:
            (rs0, rs1, rs2)[i](h, c)

    def act_all(names):
        for name in names:
            act(name)

    after, unit = {-1: []}, -1
    for event in plan():
        if event is None:
            unit += 1
            after[unit] = []
        else:
            after[unit].append(event)
    act_all(after[-1])
    base = 0
    for k, (kind, l) in enumerate(SUBLAYERS):
        for h in range(HALVES):
            last = base + UNITS[kind] - 1
            ticks = {u - base: (lambda names=after[u]: act_all(names)) for u in range(base, last) if after[u]}
            comp[kind](h, l, ticks)
            act_all(after[last])
            base = last + 1
    convo_ref[...] = convf[...].astype(BF16)


def finish(pos_s, pos_ref, slot_ref, k_cache, v_cache, kn_ref, vn_ref, x_ref, conv_ref, lru_ref,
           ko, vo, so_ref, xo_ref, convo_ref, lruo_ref, buf, xbuf, cbuf, lbuf, in_sem, out_sem, small_in, small_out):
    pairs = [(e, q) for q in range(SEQS) for e in range(2)]

    def copy_in(e, q):
        return pltpu.make_async_copy((k_cache, v_cache)[e].at[q], buf.at[e, q], in_sem.at[e, q])

    def copy_out(e, q):
        return pltpu.make_async_copy(buf.at[e, q], (ko, vo)[e].at[q], out_sem.at[e, q])

    for e, q in pairs:
        copy_in(e, q).start()
    small = ((x_ref, xbuf, xo_ref), (conv_ref, cbuf, convo_ref), (lru_ref, lbuf, lruo_ref))
    for i, (src, mid, _) in enumerate(small):
        pltpu.make_async_copy(src, mid, small_in.at[i]).start()
    begin, last = pos_ref[:, 0:1], pos_ref[:, 63:TOKENS]
    count = jnp.where(last < 63, 63 - last, TOKENS)
    slot = lax.broadcasted_iota(jnp.int32, (SEQS, WINDOW), 1)
    ahead = (slot - begin) & (WINDOW - 1)
    so_ref[...] = jnp.where(ahead < count, begin + ahead, jnp.where(slot < TOKENS - count, slot, slot_ref[...]))
    for i, (src, mid, dst) in enumerate(small):
        pltpu.make_async_copy(src, mid, small_in.at[i]).wait()
        pltpu.make_async_copy(mid, dst, small_out.at[i]).start()
    for q in range(SEQS):
        first_row = pl.multiple_of(jnp.minimum((pos_s[q, 0] & (WINDOW - 1)) // PIECE * PIECE, WINDOW - SPAN), PIECE)
        new_slots = pos_ref[q:q + 1, :] & (WINDOW - 1)
        for e in range(2):
            copy_in(e, q).wait()
        for start in (first_row, 0):
            rows = pl.ds(start, SPAN)
            hit = lax.broadcasted_iota(jnp.int32, (SPAN, TOKENS), 0) + start == new_slots
            any_hit = row_sum(hit.astype(F32)) > 0.5
            for e, ref in enumerate((kn_ref, vn_ref)):
                put = jnp.dot(hit.astype(BF16), ref[q], preferred_element_type=F32)
                buf[e, q, rows, :] = jnp.where(any_hit, put, buf[e, q, rows, :].astype(F32)).astype(BF16)
        for e in range(2):
            copy_out(e, q).start()
    for e, q in pairs:
        copy_out(e, q).wait()
    for i, (_, mid, dst) in enumerate(small):
        pltpu.make_async_copy(mid, dst, small_out.at[i]).wait()


def solution(mesh):
    def device_body(x_in, seg_pos, conv_state, lru_state, k_cache, v_cache, slot_pos, norm_scale, w_x, b_x, w_y, b_y, conv_w, conv_b, w_a, b_a, w_i, b_i, a_param, w_out, b_out, w_q, w_k, w_v, w_o, b_o, w_1, b_1, w_2, b_2, w_d, b_d):
        half_dim = ROPE_DIM // 2
        timescale = 10000.0 ** (2.0 * (jnp.arange(ROPE_DIM) % half_dim).astype(F32) / ROPE_DIM)

        vmem = pl.BlockSpec(memory_space=pltpu.VMEM)
        hbm = pl.BlockSpec(memory_space=pl.ANY)
        sds = jax.ShapeDtypeStruct
        fresh = sds((SEQS, TOKENS, WID), BF16)
        x_out, conv_out, lru_out, k_new, v_new = pl.pallas_call(
            mega,
            out_shape=(sds((TOKENS, D), BF16), sds((LAYERS, 3, SEQS, 512), BF16), sds((LAYERS, SEQS, 512), F32), fresh, fresh),
            in_specs=[vmem] * 21 + [hbm] * 12,
            out_specs=[vmem] * 5,
            scratch_shapes=[
                pltpu.VMEM((HALVES, ROWS, D), BF16),
                pltpu.VMEM((HALVES, NBLK, ROWS, COLS), BF16),
                pltpu.VMEM((HALVES, 4, NBLK, SHARD, COLS), BF16),
                pltpu.VMEM((HALVES, NBLK, SHARD, COLS), F32),
                pltpu.VMEM((HALVES, 3, 2, NBLK, PIECE, COLS), BF16),
                pltpu.VMEM((HALVES, 2, NBLK, PIECE, COLS), BF16),
                pltpu.VMEM((HALVES, 2, 2, NBLK, PIECE, COLS), BF16),
                pltpu.VMEM((HALVES, 2, NBLK, PIECE, COLS), BF16),
                pltpu.VMEM((ROWS, 1536), BF16),
                pltpu.VMEM((HALF_SEQ, 128, WID), BF16),
                pltpu.VMEM((8, HALF_SEQ, TOK, 512), F32),
                pltpu.VMEM((HALVES, 2, WINDOW, WID), BF16),
                pltpu.VMEM((NC, 2, D, WID), BF16),
                pltpu.VMEM((NR, 4, 512, COLS), BF16),
                pltpu.VMEM((6, D), F32),
                pltpu.VMEM((6, D), F32),
                pltpu.VMEM((LAYERS, 2, 16, WID), F32),
                pltpu.VMEM((3, 6, 8, WID), F32),
                pltpu.VMEM((LAYERS, SEQS, TOK, 512), F32),
                pltpu.VMEM((LAYERS, 3, SEQS, 512), F32),
                pltpu.VMEM((SEQS, TOKENS, 1), jnp.int32),
                pltpu.VMEM((HALVES, 8, HALF_SEQ, TOK, 1), jnp.int32),
                pltpu.VMEM((HALVES, ROWS, ROPE_DIM), F32),
                pltpu.VMEM((HALVES, ROWS, ROPE_DIM), F32),
                pltpu.SemaphoreType.DMA((HALVES,)),
                pltpu.SemaphoreType.DMA((HALVES, 7)),
                pltpu.SemaphoreType.DMA((HALVES,)),
                pltpu.SemaphoreType.DMA((HALVES, 8)),
                pltpu.SemaphoreType.DMA((NC, 2)),
                pltpu.SemaphoreType.DMA((NR, 4)),
                pltpu.SemaphoreType.DMA((HALVES, 2)),
            ],
            compiler_params=pltpu.CompilerParams(collective_id=0, has_side_effects=True, vmem_limit_bytes=67043328),
            name='layers',
        )(x_in.reshape(TOKENS, D), norm_scale, b_out, b_o, b_d, b_y, b_x, conv_w, conv_b, b_a, b_i, a_param, b_1, b_2,
          conv_state.swapaxes(1, 2), lru_state, w_a, w_i, seg_pos, slot_pos, timescale[None],
          w_y, w_x, w_out, w_1, w_2, w_d, w_q, w_k, w_v, w_o, k_cache, v_cache)

        k_out, v_out, slot_out, x_out, conv_out, lru_out = pl.pallas_call(
            finish,
            out_shape=[sds(v.shape, v.dtype) for v in (k_cache, v_cache, slot_pos, x_out, conv_out, lru_out)],
            in_specs=[pl.BlockSpec(memory_space=pltpu.SMEM), vmem, vmem, hbm, hbm, vmem, vmem] + [hbm] * 3,
            out_specs=[hbm, hbm, vmem] + [hbm] * 3,
            scratch_shapes=[pltpu.VMEM((2, SEQS, WINDOW, WID), BF16)] + [pltpu.VMEM(v.shape, v.dtype) for v in (x_out, conv_out, lru_out)]
            + [pltpu.SemaphoreType.DMA((2, SEQS))] * 2 + [pltpu.SemaphoreType.DMA((3,))] * 2,
            name='caches',
        )(seg_pos, seg_pos, slot_pos, k_cache, v_cache, k_new, v_new, x_out, conv_out, lru_out)
        return x_out.reshape(SEQS, TOK, D), conv_out.swapaxes(1, 2), lru_out, k_out, v_out, slot_out

    col_spec = P(None, None, 'tp')
    vec_spec = P(None, 'tp')
    row_spec = vec_spec
    x_spec, seq_spec, conv_spec, lru_spec = P('dp', 'tp'), P('dp'), P(None, 'dp', None, 'tp'), P(None, 'dp', 'tp')
    arg_specs = (x_spec, seq_spec, conv_spec, lru_spec, seq_spec, seq_spec, seq_spec, P(), col_spec, vec_spec, col_spec, vec_spec, col_spec, vec_spec, row_spec, vec_spec, row_spec, vec_spec, vec_spec, row_spec, P(), vec_spec, P(), P(), P('tp'), P(), col_spec, vec_spec, col_spec, vec_spec, row_spec, P())
    result_specs = (x_spec, conv_spec, lru_spec, seq_spec, seq_spec, seq_spec)
    return jax.shard_map(device_body, mesh=mesh, in_specs=arg_specs, out_specs=result_specs, check_vma=False)
```
